128 devices in a mesh: dp: 16 (over z, y), tp: 8 (over x, core).
Axes of the slice: x: 4, y: 4, z: 4, core: 2. Of those that a mesh axis runs over, the one named last changes fastest.
Arguments:
- x_in: bfloat16 [3, 2, 128, 192, 768], P(None, None, 'dp')
- u_pre: bfloat16 [3, 2, 128, 192, 3072], P(None, None, 'dp', None, 'tp')
- w_up: bfloat16 [3, 768, 3072], P(None, None, 'tp')
- w_down: bfloat16 [3, 3072, 768], P(None, 'tp')
- d_out: bfloat16 [2, 128, 192, 768], P(None, 'dp')
- noise_up: float32 [3, 768, 3072], P(None, 'dp', 'tp')
- noise_down: float32 [3, 3072, 768], P(None, 'tp', 'dp')
- clip_norm: float32 [1], replicated
- noise_mult: float32 [1], replicated
Outputs:
- output 1: float32 [3, 768, 3072], P(None, 'dp', 'tp')
- output 2: float32 [3, 3072, 768], P(None, 'tp', 'dp')
- output 3: bfloat16 [2, 128, 192, 768], P(None, 'dp')
All inputs are finite; a program needn't handle non-finite values.
Results may differ from the reference program's by a relative error of at most 0.0177694.
Values are sent between devices in bfloat16 or wider.
A program may use at most 1 GiB of HBM per device.

```python
import math
import jax
import jax.numpy as jnp
from jax import lax

LAYERS = 3
MICRO = 2
GLOBAL_BATCH = 128
SEQ_LEN = 192
D_MODEL = 768
D_FF = 3072

EXAMPLES = MICRO * GLOBAL_BATCH


def setup_inputs(seed: int = 0) -> dict:
    base_key = jax.random.key(seed)
    key_list = jax.random.split(base_key, 10)
    act_shape = (LAYERS, MICRO, GLOBAL_BATCH, SEQ_LEN)
    x_in = jax.random.normal(key_list[0], act_shape + (D_MODEL,), jnp.float32).astype(jnp.bfloat16)
    u_pre = jax.random.normal(key_list[1], act_shape + (D_FF,), jnp.float32).astype(jnp.bfloat16)
    w_up = (jax.random.normal(key_list[2], (LAYERS, D_MODEL, D_FF), jnp.float32) * D_MODEL ** -0.5).astype(jnp.bfloat16)
    w_down = (jax.random.normal(key_list[3], (LAYERS, D_FF, D_MODEL), jnp.float32) * D_FF ** -0.5).astype(jnp.bfloat16)
    log_scale = jax.random.uniform(key_list[4], (MICRO, GLOBAL_BATCH, 1, 1), jnp.float32, math.log(0.5), math.log(16.0))
    d_out = (jax.random.normal(key_list[5], (MICRO, GLOBAL_BATCH, SEQ_LEN, D_MODEL), jnp.float32) * jnp.exp(log_scale)).astype(jnp.bfloat16)
    noise_up = jax.random.normal(key_list[6], (LAYERS, D_MODEL, D_FF), jnp.float32)
    noise_down = jax.random.normal(key_list[7], (LAYERS, D_FF, D_MODEL), jnp.float32)
    clip_norm = jax.random.uniform(key_list[8], (1,), jnp.float32, 0.6, 1.0) * math.sqrt(LAYERS * SEQ_LEN * D_MODEL * D_FF)
    noise_mult = jnp.exp(jax.random.uniform(key_list[9], (1,), jnp.float32, math.log(0.08), math.log(0.75))) * math.sqrt(EXAMPLES / (2.0 * LAYERS * D_MODEL * D_FF))
    return {"x_in": x_in, "u_pre": u_pre, "w_up": w_up, "w_down": w_down, "d_out": d_out, "noise_up": noise_up, "noise_down": noise_down, "clip_norm": clip_norm, "noise_mult": noise_mult}


def reference(x_in, u_pre, w_up, w_down, d_out, noise_up, noise_down, clip_norm, noise_mult):
    x_rows = x_in.reshape(LAYERS, EXAMPLES, SEQ_LEN, D_MODEL)
    u_rows = u_pre.reshape(LAYERS, EXAMPLES, SEQ_LEN, D_FF)
    top_cot = d_out.reshape(EXAMPLES, SEQ_LEN, D_MODEL)

    def layer_step(carry_in, layer_in):
        grad_cot, norm_vec = carry_in
        x_layer, u_layer, w_first, w_second = layer_in
        w_first_t = w_first.T
        w_second_t = w_second.T

        def one_example(example):
            x_ex, u_ex, cot_ex = example
            gelu_out, gelu_vjp = jax.vjp(jax.nn.gelu, u_ex.astype(jnp.float32))
            hidden = gelu_out.astype(jnp.bfloat16)
            d_act = jnp.dot(cot_ex, w_second_t, preferred_element_type=jnp.float32)
            d_hid = gelu_vjp(d_act)[0].astype(jnp.bfloat16)
            back_prop = jnp.dot(d_hid, w_first_t, preferred_element_type=jnp.float32)
            new_cot = (cot_ex.astype(jnp.float32) + back_prop).astype(jnp.bfloat16)
            gram_term = jnp.sum(jnp.dot(hidden, hidden.T, preferred_element_type=jnp.float32) * jnp.dot(cot_ex, cot_ex.T, preferred_element_type=jnp.float32))
            gram_term = gram_term + jnp.sum(jnp.dot(x_ex, x_ex.T, preferred_element_type=jnp.float32) * jnp.dot(d_hid, d_hid.T, preferred_element_type=jnp.float32))
            return new_cot, gram_term, hidden, d_hid

        new_cot, gram_add, hid_layer, dhid_layer = lax.map(one_example, (x_layer, u_layer, grad_cot))
        return (new_cot, norm_vec + gram_add), (hid_layer, dhid_layer, grad_cot)

    start_carry = (top_cot, jnp.zeros((EXAMPLES,), jnp.float32))
    (d_in, norm_vec), (hid_all, dhid_all, cot_all) = lax.scan(layer_step, start_carry, (x_rows, u_rows, w_up, w_down), reverse=True)
    clip_fac = jnp.minimum(1.0, clip_norm[0] / jnp.sqrt(norm_vec))
    scale_col = clip_fac[:, None, None]

    def weight_grads(layer_in):
        x_layer, hidden, d_hid, grad_cot = layer_in
        scaled_dh = (d_hid.astype(jnp.float32) * scale_col).astype(jnp.bfloat16)
        scaled_cot = (grad_cot.astype(jnp.float32) * scale_col).astype(jnp.bfloat16)
        up_grad = jnp.dot(x_layer.reshape(-1, D_MODEL).T, scaled_dh.reshape(-1, D_FF), preferred_element_type=jnp.float32)
        down_grad = jnp.dot(hidden.reshape(-1, D_FF).T, scaled_cot.reshape(-1, D_MODEL), preferred_element_type=jnp.float32)
        return up_grad, down_grad

    up_sum, down_sum = lax.map(weight_grads, (x_rows, hid_all, dhid_all, cot_all))
    noise_scale = noise_mult[0] * clip_norm[0]
    grad_up = (up_sum + noise_scale * noise_up) / EXAMPLES
    grad_down = (down_sum + noise_scale * noise_down) / EXAMPLES
    return grad_up, grad_down, d_in.reshape(MICRO, GLOBAL_BATCH, SEQ_LEN, D_MODEL)
```

```python
import math

import jax
import jax.numpy as jnp
from jax import lax
from jax.experimental import pallas as pl
from jax.experimental.pallas import tpu as pltpu
from jax.sharding import PartitionSpec as P

MESH = pl.DeviceIdType.MESH
F32, BF16 = jnp.float32, jnp.bfloat16
N_CHUNK = 4
RING = 4
K_TANH = math.sqrt(2.0 / math.pi)
(D2D, S1L, S1R, SDL, SDR, S2L, S2R, A1L, A1R, A2L, A2R, FO, FR, FL, FA, FB) = range(16)
N_ROLE = 16
NT = (((1,), (1,)), ((), ()))
TN = (((0,), (0,)), ((), ()))


def step_kernel(x_hbm, u_hbm, w1_hbm, w2_hbm, do_hbm, nu_ref, nd_ref, clip_ref, mult_ref,
                gu_ref, gd_ref, din_hbm,
                u_s, dh_s, dz_s, w1_s, w2_s, xs, da_s, p_s, rd2d, r1, rdir, r2, g_s, q1, q2,
                nrm, nsend, nrecv, clip_s,
                ssem, rsem, gsem_s, gsem_r, nsem_s, nsem_r, usem, wsem, dsem, xsem, osem):
    n_layers, n_chunk, rows, hid = u_s.shape
    dim = dz_s.shape[-1]
    n_ex, _, seq = nrm.shape
    ex_per = n_ex // n_chunk
    piece = rows // 16
    n_item = n_layers * n_chunk
    dp, tp = lax.axis_index("dp"), lax.axis_index("tp")
    xi, core = tp // 2, tp % 2
    zi, yi = dp // RING, dp % RING

    def up(i, by=1):
        return (i + by) % RING

    x_l, x_r, x_o = up(xi, 3), up(xi, 1), up(xi, 2)
    partner = (dp, xi * 2 + 1 - core)
    dev_l, dev_r, dev_o = (dp, x_l * 2 + core), (dp, x_r * 2 + core), (dp, x_o * 2 + core)
    dev_yl, dev_yr = (zi * RING + up(yi, 3), tp), (zi * RING + up(yi), tp)
    dev_zl, dev_zr = (up(zi, 3) * RING + yi, tp), (up(zi) * RING + yi, tp)

    def remote(src, dst, send, recv, dev):
        return pltpu.make_async_remote_copy(src_ref=src, dst_ref=dst, send_sem=send, recv_sem=recv,
                                            device_id=dev, device_id_type=MESH)

    def load_u(layer, c):
        return pltpu.make_async_copy(u_hbm.at[layer, c], u_s.at[layer, c], usem.at[layer, c])

    def load_w(which, layer):
        src, dst = ((w1_hbm, w1_s), (w2_hbm, w2_s))[which]
        return pltpu.make_async_copy(src.at[layer], dst.at[layer], wsem.at[which, layer])

    def load_d(c):
        return pltpu.make_async_copy(do_hbm.at[c], dz_s.at[0, c], dsem.at[c])

    def load_x(item):
        layer, c, slot = n_layers - 1 - item // n_chunk, item % n_chunk, item % 2
        return pltpu.make_async_copy(x_hbm.at[layer, c], xs.at[slot], xsem.at[slot])

    top = n_layers - 1
    load_w(1, top).start()
    load_d(0).start()
    load_u(top, 0).start()
    load_w(0, top).start()
    load_x(0).start()
    for c in range(1, n_chunk):
        load_d(c).start()
        load_u(top, c).start()
    for layer in reversed(range(top)):
        load_w(1, layer).start()
        load_w(0, layer).start()
        for c in range(n_chunk):
            load_u(layer, c).start()

    barrier = pltpu.get_barrier_semaphore()
    peers = (partner, dev_l, dev_r, dev_o, dev_yl, dev_yr, dev_zl, dev_zr)
    for dev in peers:
        pl.semaphore_signal(barrier, inc=1, device_id=dev, device_id_type=MESH)
    pl.semaphore_wait(barrier, len(peers))

    nrm[...] = jnp.zeros_like(nrm)

    def at(cc, xx, half=0, n=1):
        return pl.ds(pl.multiple_of(cc * (rows // 2) + xx * (rows // 8) + half * piece, 16), n * piece)

    def tp_copy(role, item):
        li, c, slot = item // n_chunk, item % n_chunk, item % 2
        part, znew = p_s.at[slot], dz_s.at[li + 1, c]
        send, recv = ssem.at[role, c], rsem.at[role, c]
        if role == D2D:
            half = pl.ds(pl.multiple_of((1 - core) * (rows // 2), 16), rows // 2)
            return remote(part.at[half], rd2d.at[c], send, recv, partner)
        if role in (S1L, S1R):
            h = 0 if role == S1L else 1
            return remote(part.at[at(core, x_o, h)], r1.at[c, h], send, recv, (dev_l, dev_r)[h])
        if role == SDL:
            return remote(part.at[at(core, x_l, 1)], rdir.at[c, 0], send, recv, dev_l)
        if role == SDR:
            return remote(part.at[at(core, x_r, 0)], rdir.at[c, 1], send, recv, dev_r)
        if role == S2L:
            return remote(part.at[at(core, x_l, 0)], r2.at[c, 0], send, recv, dev_l)
        if role == S2R:
            return remote(part.at[at(core, x_r, 1)], r2.at[c, 1], send, recv, dev_r)
        where, dev = {
            A1L: (at(core, xi, 0, 2), dev_l),
            A1R: (at(core, xi, 0, 2), dev_r),
            A2L: (at(core, x_r, 0), dev_l),
            A2R: (at(core, x_l, 1), dev_r),
            FO: (at(core, xi, 0, 2), partner),
            FR: (at(core, x_r, 0, 2), partner),
            FL: (at(core, x_l, 0, 2), partner),
            FA: (at(core, x_o, 0), partner),
            FB: (at(core, x_o, 1), partner),
        }[role]
        return remote(znew.at[where], znew.at[where], send, recv, dev)

    def start(item, *roles):
        for role in roles:
            tp_copy(role, item).start()

    def arrived(item, *roles):
        for role in roles:
            tp_copy(role, item).wait_recv()

    def sent(item, *roles):
        for role in roles:
            tp_copy(role, item).wait_send()

    def pair_sum(item):
        c, slot = item % n_chunk, item % 2
        arrived(item, D2D)
        base = core * (rows // 2)
        blk = rows // 8

        def add(b, _):
            mine = pl.ds(pl.multiple_of(base + b * blk, 16), blk)
            theirs = pl.ds(pl.multiple_of(b * blk, 16), blk)
            p_s[slot, mine, :] = (p_s[slot, mine, :].astype(F32) + rd2d[c, theirs, :].astype(F32)).astype(BF16)
            return 0

        lax.fori_loop(0, 4, add, 0)
        start(item, S1L, S1R, SDL, SDR)

    def relay_sum(item):
        c, slot = item % n_chunk, item % 2
        for h, come, go, xx in ((0, S1L, S2L, x_l), (1, S1R, S2R, x_r)):
            arrived(item, come)
            where = at(core, xx, h)
            p_s[slot, where, :] = (p_s[slot, where, :].astype(F32) + r1[c, h].astype(F32)).astype(BF16)
            start(item, go)

    def own_sum(item):
        li, c, slot = item // n_chunk, item % n_chunk, item % 2
        for h, far, near in ((0, S2L, SDR), (1, S2R, SDL)):
            arrived(item, near, far)
            where = at(core, xi, h)
            total = p_s[slot, where, :].astype(F32) + r2[c, h].astype(F32) + rdir[c, 1 - h].astype(F32)
            dz_s[li + 1, c, where, :] = (dz_s[li, c, where, :].astype(F32) + total).astype(BF16)
        start(item, A1L, A1R, FO)

    def gather_relay(item):
        arrived(item, A1L)
        start(item, A2L, FR)
        arrived(item, A1R)
        start(item, A2R, FL)
        sent(item, D2D, S1L, S1R, SDL, SDR, S2L, S2R)

    def gather_cross(item):
        arrived(item, A2L)
        start(item, FA)
        arrived(item, A2R)
        start(item, FB)

    def out_copy(c):
        return pltpu.make_async_copy(dz_s.at[n_layers, c], din_hbm.at[c], osem.at[c])

    def gather_end(item):
        arrived(item, FO, FR, FL, FA, FB)
        sent(item, A1L, A1R, A2L, A2R, FO, FR, FL, FA, FB)

        @pl.when(item >= n_item - n_chunk)
        def _():
            out_copy(item % n_chunk).start()

    def compute_dh(item):
        li, c = item // n_chunk, item % n_chunk
        layer = top - li

        @pl.when(c == 0)
        def _():
            load_w(1, layer).wait()
            load_w(0, layer).wait()

        @pl.when(li == 0)
        def _():
            load_d(c).wait()

        load_u(layer, c).wait()
        da_s[...] = lax.dot_general(dz_s[li, c], w2_s[layer], NT, preferred_element_type=F32)
        blk = 32

        def act(b, _):
            r = pl.ds(pl.multiple_of(b * blk, blk), blk)
            u = u_s[layer, c, r, :].astype(F32)
            u2 = u * u
            th = jnp.tanh(K_TANH * (u + 0.044715 * (u2 * u)))
            cdf = 0.5 * (1.0 + th)
            slope = cdf + (0.5 * u) * (1.0 - th * th) * K_TANH * (1.0 + (3 * 0.044715) * u2)
            u_s[layer, c, r, :] = (u * cdf).astype(BF16)
            dh_s[layer, c, r, :] = (slope * da_s[r, :]).astype(BF16)
            return 0

        lax.fori_loop(0, rows // blk, act, 0)

    def compute_back(item):
        li, c, slot = item // n_chunk, item % n_chunk, item % 2
        layer = top - li
        for part in range(2):
            cc = 1 - core if part == 0 else core
            r = pl.ds(pl.multiple_of(cc * (rows // 2), 16), rows // 2)
            p_s[slot, r, :] = lax.dot_general(dh_s[layer, c, r, :], w1_s[layer], NT,
                                              preferred_element_type=F32).astype(BF16)
            if part == 0:
                start(item, D2D)

    def compute_norm(item):
        li, c = item // n_chunk, item % n_chunk
        layer = top - li
        load_x(item).wait()

        def one(e, _):
            r = pl.ds(pl.multiple_of(e * seq, 16), seq)

            def gram(v):
                return lax.dot_general(v, v, NT, preferred_element_type=F32)

            total = (gram(u_s[layer, c, r, :]) * gram(dz_s[li, c, r, :])
                     + gram(xs[item % 2, r, :]) * gram(dh_s[layer, c, r, :]))
            nrm[c * ex_per + e] += jnp.sum(total.reshape(seq // 8, 8, seq), axis=0)
            return 0

        lax.fori_loop(0, ex_per, one, 0)

    def slot_body(t, _):
        live = t < n_item
        one_back = jnp.logical_and(t >= 1, t - 1 < n_item)
        two_back = t >= 2

        @pl.when(t + 1 < n_item)
        def _():
            load_x(t + 1).start()

        @pl.when(one_back)
        def _():
            pair_sum(t - 1)

        @pl.when(two_back)
        def _():
            gather_relay(t - 2)

        @pl.when(live)
        def _():
            compute_dh(t)

        @pl.when(one_back)
        def _():
            relay_sum(t - 1)

        @pl.when(two_back)
        def _():
            gather_cross(t - 2)

        @pl.when(live)
        def _():
            compute_back(t)

        @pl.when(one_back)
        def _():
            own_sum(t - 1)

        @pl.when(live)
        def _():
            compute_norm(t)

        @pl.when(two_back)
        def _():
            gather_end(t - 2)

        return 0

    lax.fori_loop(0, n_item + 2, slot_body, 0)

    load_x(0).start()
    local = jnp.sum(jnp.sum(nrm[...], axis=1), axis=-1, keepdims=True)
    nsend[0] = jnp.broadcast_to(local, nsend.shape[1:])
    first = remote(nsend.at[0], nrecv.at[0], nsem_s.at[0], nsem_r.at[0], partner)
    first.start()
    first.wait_recv()
    nsend[1] = nsend[0] + nrecv[0]
    rest = [remote(nsend.at[1], nrecv.at[i + 1], nsem_s.at[i + 1], nsem_r.at[i + 1], dev)
            for i, dev in enumerate((dev_l, dev_r, dev_o))]
    for cp in rest:
        cp.start()
    for cp in rest:
        cp.wait_recv()
    norm = nsend[1] + nrecv[1] + nrecv[2] + nrecv[3]
    factor = jnp.minimum(1.0, clip_ref[0] / jnp.sqrt(norm))
    for e in range(n_ex):
        clip_s[e] = jnp.broadcast_to(factor[e:e + 1, :], clip_s.shape[1:])
    first.wait_send()
    for cp in rest:
        cp.wait_send()

    def grad_view(k, kind, phase, j, h):
        if phase == 0:
            n = RING // 2
            if kind == 0:
                return g_s.at[k, pl.ds(h * n, n), j]
            return g_s.at[k, j, pl.ds(h * n, n)]
        n = g_s.shape[3] // 2
        if kind == 0:
            return g_s.at[k, j, yi, pl.ds(h * n, n)]
        return g_s.at[k, zi, j, pl.ds(h * n, n)]

    def ring_of(kind, phase):
        if (kind == 0) == (phase == 0):
            return yi, dev_yl, dev_yr
        return zi, dev_zl, dev_zr

    def grad_copy(k, kind, phase, role):
        me, d_l, d_r = ring_of(kind, phase)
        buf = (q1, q2)[phase]
        j, h = ((up(me, 2), 0), (up(me, 2), 1), (up(me, 3), 1), (up(me, 1), 0), (up(me, 3), 0), (up(me, 1), 1))[role]
        return remote(grad_view(k, kind, phase, j, h), buf.at[k, role], gsem_s.at[phase, role, k],
                      gsem_r.at[phase, role, k], d_r if role % 2 else d_l)

    def ring_start(p, kind, phase):
        k = 2 * p + kind
        for role in range(4):
            grad_copy(k, kind, phase, role).start()

    def ring_relay(p, kind, phase):
        k = 2 * p + kind
        me, _, _ = ring_of(kind, phase)
        buf = (q1, q2)[phase]
        for h in range(2):
            grad_copy(k, kind, phase, h).wait_recv()
            view = grad_view(k, kind, phase, up(me, 1 if h else 3), h)
            view[...] = view[...] + buf[k, h]
            grad_copy(k, kind, phase, 4 + h).start()

    def ring_end(p, kind, phase):
        k = 2 * p + kind
        me, _, _ = ring_of(kind, phase)
        buf = (q1, q2)[phase]
        for h in range(2):
            grad_copy(k, kind, phase, 3 - h).wait_recv()
            grad_copy(k, kind, phase, 4 + h).wait_recv()
            view = grad_view(k, kind, phase, me, h)
            view[...] = view[...] + buf[k, 3 - h] + buf[k, 4 + h]

    def ring_sent(p, kind, phase):
        for role in range(6):
            grad_copy(2 * p + kind, kind, phase, role).wait_send()

    inv = 1.0 / (n_ex * RING * RING)
    scale = mult_ref[0] * clip_ref[0]

    def finish(p, kind):
        k, layer = 2 * p + kind, top - p
        out, noise = ((gu_ref, nu_ref), (gd_ref, nd_ref))[kind]
        out[layer] = (g_s[k, zi, yi] + scale * noise[layer]) * inv

    def weight_grad(p, kind):
        k, layer = 2 * p + kind, top - p

        def one(c, _):
            if kind == 0:
                item = p * n_chunk + c

                @pl.when(item + 1 < n_item)
                def _():
                    load_x(item + 1).start()

                load_x(item).wait()
            for e in range(ex_per):
                f = clip_s[c * ex_per + e][0:1, 0:1]
                r = pl.ds(e * seq, seq)
                if kind == 0:
                    dh_s[layer, c, r, :] = (dh_s[layer, c, r, :].astype(F32) * f).astype(BF16)
                else:
                    dz_s[p, c, r, :] = (dz_s[p, c, r, :].astype(F32) * f).astype(BF16)
            if kind == 0:
                add = lax.dot_general(xs[c % 2], dh_s[layer, c], TN, preferred_element_type=F32)
            else:
                add = lax.dot_general(dz_s[p, c], u_s[layer, c], TN, preferred_element_type=F32)
            add = add.reshape(g_s.shape[1:])

            @pl.when(c == 0)
            def _():
                g_s[k] = add

            @pl.when(c > 0)
            def _():
                g_s[k] += add

            return 0

        lax.fori_loop(0, n_chunk, one, 0)

    def pair_body(p, _):
        def back(n):
            return jnp.logical_and(p >= n, p - n < n_layers)

        @pl.when(back(0))
        def _():
            weight_grad(p, 0)
            ring_start(p, 0, 0)

        @pl.when(back(1))
        def _():
            ring_relay(p - 1, 1, 0)

        @pl.when(back(0))
        def _():
            weight_grad(p, 1)
            ring_start(p, 1, 0)
            ring_relay(p, 0, 0)

        @pl.when(back(2))
        def _():
            ring_relay(p - 2, 0, 1)
            ring_relay(p - 2, 1, 1)

        @pl.when(back(1))
        def _():
            ring_end(p - 1, 0, 0)
            ring_start(p - 1, 0, 1)
            ring_end(p - 1, 1, 0)
            ring_start(p - 1, 1, 1)

        @pl.when(back(2))
        def _():
            for kind in range(2):
                ring_end(p - 2, kind, 1)
                finish(p - 2, kind)
                ring_sent(p - 2, kind, 0)
                ring_sent(p - 2, kind, 1)

        return 0

    lax.fori_loop(0, n_layers + 2, pair_body, 0)
    for c in range(n_chunk):
        out_copy(c).wait()


def solution(mesh):
    n_dp, n_tp = mesh.shape["dp"], mesh.shape["tp"]

    def local(x_in, u_pre, w_up, w_down, d_out, noise_up, noise_down, clip_norm, noise_mult):
        n_layers, micro, batch, seq, dim = x_in.shape
        hid = u_pre.shape[-1]
        n_ex = micro * batch
        rows = n_ex * seq // N_CHUNK
        piece, grad_rows = rows // 16, dim // n_dp
        x4 = x_in.reshape(n_layers, N_CHUNK, rows, dim)
        u4 = u_pre.reshape(n_layers, N_CHUNK, rows, hid)
        d4 = d_out.reshape(N_CHUNK, rows, dim)
        anyspace = pl.BlockSpec(memory_space=pl.ANY)
        vmem = pl.BlockSpec(memory_space=pltpu.VMEM)
        smem = pl.BlockSpec(memory_space=pltpu.SMEM)
        dma = pltpu.SemaphoreType.DMA
        tokens = n_ex * seq
        flops = 2 * n_layers * tokens * hid * dim * 4 + 4 * n_layers * tokens * seq * (hid + dim)
        g_up, g_down, d_in = pl.pallas_call(
            step_kernel,
            out_shape=(
                jax.ShapeDtypeStruct((n_layers, grad_rows, hid), F32),
                jax.ShapeDtypeStruct((n_layers, grad_rows, hid), F32),
                jax.ShapeDtypeStruct((N_CHUNK, rows, dim), BF16),
            ),
            in_specs=[anyspace] * 5 + [vmem, vmem, smem, smem],
            out_specs=(vmem, vmem, anyspace),
            scratch_shapes=[
                pltpu.VMEM((n_layers, N_CHUNK, rows, hid), BF16),
                pltpu.VMEM((n_layers, N_CHUNK, rows, hid), BF16),
                pltpu.VMEM((n_layers + 1, N_CHUNK, rows, dim), BF16),
                pltpu.VMEM((n_layers, dim, hid), BF16),
                pltpu.VMEM((n_layers, hid, dim), BF16),
                pltpu.VMEM((2, rows, dim), BF16),
                pltpu.VMEM((rows, hid), F32),
                pltpu.VMEM((2, rows, dim), BF16),
                pltpu.VMEM((N_CHUNK, rows // 2, dim), BF16),
                pltpu.VMEM((N_CHUNK, 2, piece, dim), BF16),
                pltpu.VMEM((N_CHUNK, 2, piece, dim), BF16),
                pltpu.VMEM((N_CHUNK, 2, piece, dim), BF16),
                pltpu.VMEM((2 * n_layers, RING, RING, grad_rows, hid), F32),
                pltpu.VMEM((2 * n_layers, 6, RING // 2, grad_rows, hid), F32),
                pltpu.VMEM((2 * n_layers, 6, grad_rows // 2, hid), F32),
                pltpu.VMEM((n_ex, 8, seq), F32),
                pltpu.VMEM((2, n_ex, 128), F32),
                pltpu.VMEM((4, n_ex, 128), F32),
                pltpu.VMEM((n_ex, 8, 128), F32),
                dma((N_ROLE, N_CHUNK)),
                dma((N_ROLE, N_CHUNK)),
                dma((2, 6, 2 * n_layers)),
                dma((2, 6, 2 * n_layers)),
                dma((4,)),
                dma((4,)),
                dma((n_layers, N_CHUNK)),
                dma((2, n_layers)),
                dma((N_CHUNK,)),
                dma((2,)),
                dma((N_CHUNK,)),
            ],
            compiler_params=pltpu.CompilerParams(
                collective_id=0, has_side_effects=True, vmem_limit_bytes=67_043_328
            ),
            cost_estimate=pl.CostEstimate(flops=flops, bytes_accessed=50_000_000, transcendentals=n_layers * tokens * hid),
            name="clipped_step",
        )(x4, u4, w_up, w_down, d4, noise_up, jnp.transpose(noise_down, (0, 2, 1)), clip_norm, noise_mult)
        return g_up, jnp.transpose(g_down, (0, 2, 1)), d_in.reshape(d_out.shape)

    in_specs = (P(None, None, "dp", None, None), P(None, None, "dp", None, "tp"), P(None, None, "tp"),
                P(None, "tp", None), P(None, "dp", None, None), P(None, "dp", "tp"), P(None, "tp", "dp"), P(), P())
    out_specs = (P(None, "dp", "tp"), P(None, "tp", "dp"), P(None, "dp", None, None))
    return jax.shard_map(local, mesh=mesh, in_specs=in_specs, out_specs=out_specs, check_vma=False)
```

```python
import math

import jax
import jax.numpy as jnp
from jax import lax
from jax.experimental import pallas as pl
from jax.experimental.pallas import tpu as pltpu
from jax.sharding import PartitionSpec as P

MESH = pl.DeviceIdType.MESH
F32, BF16 = jnp.float32, jnp.bfloat16
N_CHUNK = 4
RING = 4
K_TANH = math.sqrt(2.0 / math.pi)
(D2D, S1L, S1R, SDL, SDR, S2L, S2R, A1L, A1R, A2L, A2R, FO, FR, FL, FA, FB) = range(16)
N_ROLE = 16
NT = (((1,), (1,)), ((), ()))
TN = (((0,), (0,)), ((), ()))


def step_kernel(x_hbm, u_hbm, w1_hbm, w2_hbm, do_hbm, clip_hbm,
                gu_ref, gd_ref, din_hbm,
                u_s, dh_s, dz_s, w1_s, w2_s, xs, da_s, p_s, rd2d, r1, rdir, r2, g_s, q1, q2,
                nrm, nsend, nrecv, clip_s, clip_ref,
                ssem, rsem, gsem_s, gsem_r, nsem_s, nsem_r, usem, wsem, dsem, xsem, osem, csem):
    n_layers, n_chunk, rows, hid = u_s.shape
    dim = dz_s.shape[-1]
    n_ex, _, seq = nrm.shape
    ex_per = n_ex // n_chunk
    piece = rows // 16
    n_item = n_layers * n_chunk
    dp, tp = lax.axis_index("dp"), lax.axis_index("tp")
    xi, core = tp // 2, tp % 2
    zi, yi = dp // RING, dp % RING

    def up(i, by=1):
        return (i + by) % RING

    x_l, x_r, x_o = up(xi, 3), up(xi, 1), up(xi, 2)
    partner = (dp, xi * 2 + 1 - core)
    dev_l, dev_r, dev_o = (dp, x_l * 2 + core), (dp, x_r * 2 + core), (dp, x_o * 2 + core)
    dev_yl, dev_yr = (zi * RING + up(yi, 3), tp), (zi * RING + up(yi), tp)
    dev_zl, dev_zr = (up(zi, 3) * RING + yi, tp), (up(zi) * RING + yi, tp)

    def remote(src, dst, send, recv, dev):
        return pltpu.make_async_remote_copy(src_ref=src, dst_ref=dst, send_sem=send, recv_sem=recv,
                                            device_id=dev, device_id_type=MESH)

    def load_u(layer, c):
        return pltpu.make_async_copy(u_hbm.at[layer, c], u_s.at[layer, c], usem.at[layer, c])

    def load_w(which, layer):
        src, dst = ((w1_hbm, w1_s), (w2_hbm, w2_s))[which]
        return pltpu.make_async_copy(src.at[layer], dst.at[layer], wsem.at[which, layer])

    def load_d(c):
        return pltpu.make_async_copy(do_hbm.at[c], dz_s.at[0, c], dsem.at[c])

    def load_x(item):
        layer, c, slot = n_layers - 1 - item // n_chunk, item % n_chunk, item % 2
        return pltpu.make_async_copy(x_hbm.at[layer, c], xs.at[slot], xsem.at[slot])

    load_c = pltpu.make_async_copy(clip_hbm, clip_ref, csem)
    top = n_layers - 1
    load_w(1, top).start()
    load_d(0).start()
    load_u(top, 0).start()
    load_w(0, top).start()
    load_x(0).start()
    for c in range(1, n_chunk):
        load_d(c).start()
        load_u(top, c).start()
    for layer in reversed(range(top)):
        load_w(1, layer).start()
        load_w(0, layer).start()
        for c in range(n_chunk):
            load_u(layer, c).start()
    load_c.start()

    barrier = pltpu.get_barrier_semaphore()
    peers = (partner, dev_l, dev_r, dev_o, dev_yl, dev_yr, dev_zl, dev_zr)
    for dev in peers:
        pl.semaphore_signal(barrier, inc=1, device_id=dev, device_id_type=MESH)


    def at(cc, xx, half=0, n=1):
        return pl.ds(pl.multiple_of(cc * (rows // 2) + xx * (rows // 8) + half * piece, 16), n * piece)

    def tp_copy(role, item):
        li, c, slot = item // n_chunk, item % n_chunk, item % n_chunk
        part, znew = p_s.at[slot], dz_s.at[li + 1, c]
        send, recv = ssem.at[role, c], rsem.at[role, c]
        if role == D2D:
            half = pl.ds(pl.multiple_of((1 - core) * (rows // 2), 16), rows // 2)
            return remote(part.at[half], rd2d.at[c], send, recv, partner)
        if role in (S1L, S1R):
            h = 0 if role == S1L else 1
            return remote(part.at[at(core, x_o, h)], r1.at[c, h], send, recv, (dev_l, dev_r)[h])
        if role == SDL:
            return remote(part.at[at(core, x_l, 1)], rdir.at[c, 0], send, recv, dev_l)
        if role == SDR:
            return remote(part.at[at(core, x_r, 0)], rdir.at[c, 1], send, recv, dev_r)
        if role == S2L:
            return remote(part.at[at(core, x_l, 0)], r2.at[c, 0], send, recv, dev_l)
        if role == S2R:
            return remote(part.at[at(core, x_r, 1)], r2.at[c, 1], send, recv, dev_r)
        where, dev = {
            A1L: (at(core, xi, 0, 2), dev_l),
            A1R: (at(core, xi, 0, 2), dev_r),
            A2L: (at(core, x_r, 0), dev_l),
            A2R: (at(core, x_l, 1), dev_r),
            FO: (at(core, xi, 0, 2), partner),
            FR: (at(core, x_r, 0, 2), partner),
            FL: (at(core, x_l, 0, 2), partner),
            FA: (at(core, x_o, 0), partner),
            FB: (at(core, x_o, 1), partner),
        }[role]
        return remote(znew.at[where], znew.at[where], send, recv, dev)

    def start(item, *roles):
        for role in roles:
            tp_copy(role, item).start()

    def arrived(item, *roles):
        for role in roles:
            tp_copy(role, item).wait_recv()

    def sent(item, *roles):
        for role in roles:
            tp_copy(role, item).wait_send()

    def pair_sum(item):
        c, slot = item % n_chunk, item % n_chunk
        arrived(item, D2D)
        base = core * (rows // 2)
        blk = rows // 8

        def add(b, _):
            mine = pl.ds(pl.multiple_of(base + b * blk, 16), blk)
            theirs = pl.ds(pl.multiple_of(b * blk, 16), blk)
            p_s[slot, mine, :] = (p_s[slot, mine, :].astype(F32) + rd2d[c, theirs, :].astype(F32)).astype(BF16)
            return 0

        lax.fori_loop(0, 4, add, 0)
        start(item, S1L, S1R)

    def relay_sum(item):
        c, slot = item % n_chunk, item % n_chunk
        for h, come, go, xx in ((0, S1L, S2L, x_l), (1, S1R, S2R, x_r)):
            arrived(item, come)
            where = at(core, xx, h)
            p_s[slot, where, :] = (p_s[slot, where, :].astype(F32) + r1[c, h].astype(F32)).astype(BF16)
            start(item, go)

    def own_sum(item):
        li, c, slot = item // n_chunk, item % n_chunk, item % n_chunk
        for h, far, near in ((0, S2L, SDR), (1, S2R, SDL)):
            arrived(item, near, far)
            where = at(core, xi, h)
            total = p_s[slot, where, :].astype(F32) + r2[c, h].astype(F32) + rdir[c, 1 - h].astype(F32)
            dz_s[li + 1, c, where, :] = (dz_s[li, c, where, :].astype(F32) + total).astype(BF16)
        start(item, A1L, A1R, FO)

    def gather_relay(item):
        arrived(item, A1L)
        start(item, A2L, FR)
        arrived(item, A1R)
        start(item, A2R, FL)
        sent(item, D2D, S1L, S1R, SDL, SDR, S2L, S2R)

    def gather_cross(item):
        arrived(item, A2L)
        start(item, FA)
        arrived(item, A2R)
        start(item, FB)

    def out_copy(c):
        return pltpu.make_async_copy(dz_s.at[n_layers, c], din_hbm.at[c], osem.at[c])

    def gather_end(item):
        arrived(item, FO, FR, FL, FA, FB)
        sent(item, A1L, A1R, A2L, A2R, FO, FR, FL, FA, FB)

        @pl.when(item >= n_item - n_chunk)
        def _():
            out_copy(item % n_chunk).start()

    def compute_dh(item):
        li, c = item // n_chunk, item % n_chunk
        layer = top - li

        @pl.when(c == 0)
        def _():
            load_w(1, layer).wait()
            load_w(0, layer).wait()

        @pl.when(li == 0)
        def _():
            load_d(c).wait()

        load_u(layer, c).wait()
        da_s[...] = lax.dot_general(dz_s[li, c], w2_s[layer], NT, preferred_element_type=F32)
        blk = 32

        def act(b, _):
            r = pl.ds(pl.multiple_of(b * blk, blk), blk)
            u = u_s[layer, c, r, :].astype(F32)
            u2 = u * u
            th = jnp.tanh(K_TANH * (u + 0.044715 * (u2 * u)))
            cdf = 0.5 * (1.0 + th)
            slope = cdf + (0.5 * u) * (1.0 - th * th) * K_TANH * (1.0 + (3 * 0.044715) * u2)
            u_s[layer, c, r, :] = (u * cdf).astype(BF16)
            dh_s[layer, c, r, :] = (slope * da_s[r, :]).astype(BF16)
            return 0

        lax.fori_loop(0, rows // blk, act, 0)

    def compute_back(item):
        li, c, slot = item // n_chunk, item % n_chunk, item % n_chunk
        layer = top - li
        for part in range(2):
            cc = 1 - core if part == 0 else core
            r = pl.ds(pl.multiple_of(cc * (rows // 2), 16), rows // 2)
            p_s[slot, r, :] = lax.dot_general(dh_s[layer, c, r, :], w1_s[layer], NT,
                                              preferred_element_type=F32).astype(BF16)
            if part == 0:
                start(item, D2D)

    def compute_norm(item):
        li, c = item // n_chunk, item % n_chunk
        layer = top - li
        load_x(item).wait()

        def one(e, _):
            r = pl.ds(pl.multiple_of(e * seq, 16), seq)

            def gram(v):
                return lax.dot_general(v, v, NT, preferred_element_type=F32)

            total = (gram(u_s[layer, c, r, :]) * gram(dz_s[li, c, r, :])
                     + gram(xs[item % 2, r, :]) * gram(dh_s[layer, c, r, :]))
            nrm[c * ex_per + e] += jnp.sum(total.reshape(seq // 8, 8, seq), axis=0)
            return 0

        lax.fori_loop(0, ex_per, one, 0)

    def clip_factors():
        load_c.wait()
        local = jnp.sum(jnp.sum(nrm[...], axis=1), axis=-1, keepdims=True)
        nsend[0] = jnp.broadcast_to(local, nsend.shape[1:])
        first = remote(nsend.at[0], nrecv.at[0], nsem_s.at[0], nsem_r.at[0], partner)
        first.start()
        first.wait_recv()
        nsend[1] = nsend[0] + nrecv[0]
        rest = [remote(nsend.at[1], nrecv.at[i + 1], nsem_s.at[i + 1], nsem_r.at[i + 1], dev)
                for i, dev in enumerate((dev_l, dev_r, dev_o))]
        for cp in rest:
            cp.start()
        for cp in rest:
            cp.wait_recv()
        norm = nsend[1] + nrecv[1] + nrecv[2] + nrecv[3]
        factor = jnp.minimum(1.0, clip_ref[0] / jnp.sqrt(norm))
        for e in range(n_ex):
            clip_s[e] = jnp.broadcast_to(factor[e:e + 1, :], clip_s.shape[1:])
        first.wait_send()
        for cp in rest:
            cp.wait_send()

    def grad_view(k, kind, phase, j, h):
        if phase == 0:
            n = RING // 2
            if kind == 0:
                return g_s.at[k, pl.ds(h * n, n), j]
            return g_s.at[k, j, pl.ds(h * n, n)]
        n = g_s.shape[3] // 2
        if kind == 0:
            return g_s.at[k, j, yi, pl.ds(h * n, n)]
        return g_s.at[k, zi, j, pl.ds(h * n, n)]

    def ring_of(kind, phase):
        if (kind == 0) == (phase == 0):
            return yi, dev_yl, dev_yr
        return zi, dev_zl, dev_zr

    def grad_copy(k, kind, phase, role):
        me, d_l, d_r = ring_of(kind, phase)
        buf = (q1, q2)[phase]
        j, h = ((up(me, 2), 0), (up(me, 2), 1), (up(me, 3), 1), (up(me, 1), 0), (up(me, 3), 0), (up(me, 1), 1))[role]
        return remote(grad_view(k, kind, phase, j, h), buf.at[k, role], gsem_s.at[phase, role, k],
                      gsem_r.at[phase, role, k], d_r if role % 2 else d_l)

    def ring_start(p, kind, phase):
        k = 2 * p + kind
        for role in range(4):
            grad_copy(k, kind, phase, role).start()

    def ring_relay(p, kind, phase):
        k = 2 * p + kind
        me, _, _ = ring_of(kind, phase)
        buf = (q1, q2)[phase]
        for h in range(2):
            grad_copy(k, kind, phase, h).wait_recv()
            view = grad_view(k, kind, phase, up(me, 1 if h else 3), h)
            view[...] = view[...] + buf[k, h]
            grad_copy(k, kind, phase, 4 + h).start()

    def ring_end(p, kind, phase):
        k = 2 * p + kind
        me, _, _ = ring_of(kind, phase)
        buf = (q1, q2)[phase]
        for h in range(2):
            grad_copy(k, kind, phase, 3 - h).wait_recv()
            grad_copy(k, kind, phase, 4 + h).wait_recv()
            view = grad_view(k, kind, phase, me, h)
            view[...] = view[...] + buf[k, 3 - h] + buf[k, 4 + h]

    def ring_sent(p, kind, phase):
        for role in range(6):
            grad_copy(2 * p + kind, kind, phase, role).wait_send()

    def finish(p, kind):
        (gu_ref, gd_ref)[kind][top - p] = g_s[2 * p + kind, zi, yi]

    def weight_grad(p, kind):
        k, layer = 2 * p + kind, top - p

        def one(c, _):
            if kind == 0:
                item = p * n_chunk + c

                @pl.when(item + 1 < n_item)
                def _():
                    load_x(item + 1).start()

                load_x(item).wait()
            for e in range(ex_per):
                f = clip_s[c * ex_per + e][0:1, 0:1]
                r = pl.ds(e * seq, seq)
                if kind == 0:
                    dh_s[layer, c, r, :] = (dh_s[layer, c, r, :].astype(F32) * f).astype(BF16)
                else:
                    xs[1, r, :] = (dz_s[p, c, r, :].astype(F32) * f).astype(BF16)
            if kind == 0:
                add = lax.dot_general(xs[c % 2], dh_s[layer, c], TN, preferred_element_type=F32)
            else:
                add = lax.dot_general(xs[1], u_s[layer, c], TN, preferred_element_type=F32)
            add = add.reshape(g_s.shape[1:])

            @pl.when(c == 0)
            def _():
                g_s[k] = add

            @pl.when(c > 0)
            def _():
                g_s[k] += add

            return 0

        lax.fori_loop(0, n_chunk, one, 0)

    late = n_item - n_chunk

    def slot_body(t, _):
        i_s = t - 1 - 2 * (t // (late + 3))
        i_a = t - 2 - 2 * (t // (late + 4))
        i_e = t - 3 - 2 * (t // (late + 5))

        def span(lo, n):
            return jnp.logical_and(t >= lo, t < lo + n)

        on_s = jnp.logical_or(span(1, late), span(late + 3, n_chunk))
        on_a = jnp.logical_or(span(2, late), span(late + 4, n_chunk))
        on_e = jnp.logical_or(span(3, late), span(late + 5, n_chunk))
        live = t < n_item
        p = t - n_item

        @pl.when(live)
        def _():
            load_x((t + 1) % n_item).start()

        @pl.when(on_s)
        def _():
            pair_sum(i_s)

        @pl.when(on_a)
        def _():
            own_sum(i_a)

        @pl.when(on_s)
        def _():
            start(i_s, SDL, SDR)

        @pl.when(jnp.logical_and(live, t > 0))
        def _():
            compute_dh(t)

        @pl.when(t == n_item)
        def _():
            clip_factors()

        @pl.when(span(n_item, n_layers))
        def _():
            weight_grad(p, 0)
            ring_start(p, 0, 0)

        @pl.when(on_e)
        def _():
            gather_cross(i_e)

        @pl.when(live)
        def _():
            compute_back(t)

        @pl.when(span(n_item + 1, n_layers))
        def _():
            ring_relay(p - 1, 1, 0)

        @pl.when(on_s)
        def _():
            relay_sum(i_s)

        @pl.when(live)
        def _():
            compute_norm(t)

        @pl.when(span(n_item, n_layers))
        def _():
            weight_grad(p, 1)
            ring_start(p, 1, 0)
            ring_relay(p, 0, 0)

        @pl.when(on_a)
        def _():
            gather_relay(i_a)

        @pl.when(span(n_item + 2, n_layers))
        def _():
            ring_relay(p - 2, 0, 1)
            ring_relay(p - 2, 1, 1)

        @pl.when(span(n_item + 1, n_layers))
        def _():
            ring_end(p - 1, 0, 0)
            ring_start(p - 1, 0, 1)
            ring_end(p - 1, 1, 0)
            ring_start(p - 1, 1, 1)

        @pl.when(on_e)
        def _():
            gather_end(i_e)

        return 0

    nrm[...] = jnp.zeros_like(nrm)
    compute_dh(0)
    pl.semaphore_wait(barrier, len(peers))
    lax.fori_loop(0, n_item + n_layers + 2, slot_body, 0)
    for p in range(n_layers):
        for kind in range(2):
            ring_end(p, kind, 1)
            finish(p, kind)
            ring_sent(p, kind, 0)
            ring_sent(p, kind, 1)
    for c in range(n_chunk):
        out_copy(c).wait()


def solution(mesh):
    n_dp, n_tp = mesh.shape["dp"], mesh.shape["tp"]

    def local(x_in, u_pre, w_up, w_down, d_out, noise_up, noise_down, clip_norm, noise_mult):
        n_layers, micro, batch, seq, dim = x_in.shape
        hid = u_pre.shape[-1]
        n_ex = micro * batch
        rows = n_ex * seq // N_CHUNK
        piece, grad_rows = rows // 16, dim // n_dp
        x4 = x_in.reshape(n_layers, N_CHUNK, rows, dim)
        u4 = u_pre.reshape(n_layers, N_CHUNK, rows, hid)
        d4 = d_out.reshape(N_CHUNK, rows, dim)
        anyspace = pl.BlockSpec(memory_space=pl.ANY)
        vmem = pl.BlockSpec(memory_space=pltpu.VMEM)
        dma = pltpu.SemaphoreType.DMA
        tokens = n_ex * seq
        flops = 2 * n_layers * tokens * hid * dim * 4 + 4 * n_layers * tokens * seq * (hid + dim)
        g_up, g_down, d_in = pl.pallas_call(
            step_kernel,
            out_shape=(
                jax.ShapeDtypeStruct((n_layers, grad_rows, hid), F32),
                jax.ShapeDtypeStruct((n_layers, grad_rows, hid), F32),
                jax.ShapeDtypeStruct((N_CHUNK, rows, dim), BF16),
            ),
            in_specs=[anyspace] * 6,
            out_specs=(vmem, vmem, anyspace),
            scratch_shapes=[
                pltpu.VMEM((n_layers, N_CHUNK, rows, hid), BF16),
                pltpu.VMEM((n_layers, N_CHUNK, rows, hid), BF16),
                pltpu.VMEM((n_layers + 1, N_CHUNK, rows, dim), BF16),
                pltpu.VMEM((n_layers, dim, hid), BF16),
                pltpu.VMEM((n_layers, hid, dim), BF16),
                pltpu.VMEM((2, rows, dim), BF16),
                pltpu.VMEM((rows, hid), F32),
                pltpu.VMEM((N_CHUNK, rows, dim), BF16),
                pltpu.VMEM((N_CHUNK, rows // 2, dim), BF16),
                pltpu.VMEM((N_CHUNK, 2, piece, dim), BF16),
                pltpu.VMEM((N_CHUNK, 2, piece, dim), BF16),
                pltpu.VMEM((N_CHUNK, 2, piece, dim), BF16),
                pltpu.VMEM((2 * n_layers, RING, RING, grad_rows, hid), F32),
                pltpu.VMEM((2 * n_layers, 6, RING // 2, grad_rows, hid), F32),
                pltpu.VMEM((2 * n_layers, 6, grad_rows // 2, hid), F32),
                pltpu.VMEM((n_ex, 8, seq), F32),
                pltpu.VMEM((2, n_ex, 128), F32),
                pltpu.VMEM((4, n_ex, 128), F32),
                pltpu.VMEM((n_ex, 8, 128), F32),
                pltpu.SMEM((1,), F32),
                dma((N_ROLE, N_CHUNK)),
                dma((N_ROLE, N_CHUNK)),
                dma((2, 6, 2 * n_layers)),
                dma((2, 6, 2 * n_layers)),
                dma((4,)),
                dma((4,)),
                dma((n_layers, N_CHUNK)),
                dma((2, n_layers)),
                dma((N_CHUNK,)),
                dma((2,)),
                dma((N_CHUNK,)),
                dma,
            ],
            compiler_params=pltpu.CompilerParams(
                collective_id=0, has_side_effects=True, vmem_limit_bytes=67_043_328
            ),
            cost_estimate=pl.CostEstimate(flops=flops, bytes_accessed=50_000_000, transcendentals=n_layers * tokens * hid),
            name="clipped_step",
        )(x4, u4, w_up, w_down, d4, clip_norm)
        inv = 1.0 / (n_ex * n_dp)
        scale = noise_mult[0] * clip_norm[0]
        g_up = (g_up + scale * noise_up) * inv
        g_down = (jnp.transpose(g_down, (0, 2, 1)) + scale * noise_down) * inv
        return g_up, g_down, d_in.reshape(d_out.shape)

    in_specs = (P(None, None, "dp", None, None), P(None, None, "dp", None, "tp"), P(None, None, "tp"),
                P(None, "tp", None), P(None, "dp", None, None), P(None, "dp", "tp"), P(None, "tp", "dp"), P(), P())
    out_specs = (P(None, "dp", "tp"), P(None, "tp", "dp"), P(None, "dp", None, None))
    return jax.shard_map(local, mesh=mesh, in_specs=in_specs, out_specs=out_specs, check_vma=False)
```

```python
import math

import jax
import jax.numpy as jnp
from jax import lax
from jax.experimental import pallas as pl
from jax.experimental.pallas import tpu as pltpu
from jax.sharding import PartitionSpec as P

MESH = pl.DeviceIdType.MESH
F32, BF16 = jnp.float32, jnp.bfloat16
N_CHUNK = 4
RING = 4
K_TANH = math.sqrt(2.0 / math.pi)
(D2D, S1L, S1R, SDL, SDR, S2L, S2R, A1L, A1R, A2L, A2R, FO, FR, FL, FA, FB) = range(16)
N_ROLE = 16
NT = (((1,), (1,)), ((), ()))
TN = (((0,), (0,)), ((), ()))


def scoped(f):
    def g(*a):
        with jax.named_scope(f.__name__):
            return f(*a)
    return g


def step_kernel(x_hbm, u_hbm, w1_hbm, w2_hbm, do_hbm, nu_hbm, nd_hbm, clip_hbm, mult_hbm,
                gu_ref, gd_ref, din_hbm,
                u_s, dh_s, dz_s, w1_s, w2_s, xs, da_s, p_s, rd2d, r1, rdir, r2, g_s, q1, q2,
                nrm, nsend, nrecv, clip_s, nz_s, clip_ref, mult_ref,
                ssem, rsem, gsem_s, gsem_r, nsem_s, nsem_r, usem, wsem, dsem, xsem, osem, csem):
    n_layers, n_chunk, rows, hid = u_s.shape
    dim = dz_s.shape[-1]
    n_ex, _, seq = nrm.shape
    ex_per = n_ex // n_chunk
    piece = rows // 16
    n_item = n_layers * n_chunk
    dp, tp = lax.axis_index("dp"), lax.axis_index("tp")
    xi, core = tp // 2, tp % 2
    zi, yi = dp // RING, dp % RING

    def up(i, by=1):
        return (i + by) % RING

    x_l, x_r, x_o = up(xi, 3), up(xi, 1), up(xi, 2)
    partner = (dp, xi * 2 + 1 - core)
    dev_l, dev_r = (dp, x_l * 2 + core), (dp, x_r * 2 + core)
    dev_yl, dev_yr = (zi * RING + up(yi, 3), tp), (zi * RING + up(yi), tp)
    dev_zl, dev_zr = (up(zi, 3) * RING + yi, tp), (up(zi) * RING + yi, tp)

    def remote(src, dst, send, recv, dev):
        return pltpu.make_async_remote_copy(src_ref=src, dst_ref=dst, send_sem=send, recv_sem=recv,
                                            device_id=dev, device_id_type=MESH)

    def load_u(layer, c):
        return pltpu.make_async_copy(u_hbm.at[layer, c], u_s.at[layer, c], usem.at[layer, c])

    def load_w(which, layer):
        src, dst = ((w1_hbm, w1_s), (w2_hbm, w2_s))[which]
        return pltpu.make_async_copy(src.at[layer], dst.at[layer], wsem.at[which, layer])

    def load_d(c):
        return pltpu.make_async_copy(do_hbm.at[c], dz_s.at[0, c], dsem.at[c])

    def load_x(item):
        layer, c, slot = n_layers - 1 - item // n_chunk, item % n_chunk, item % 2
        return pltpu.make_async_copy(x_hbm.at[layer, c], xs.at[slot], xsem.at[slot])

    load_small = [pltpu.make_async_copy(src, dst, csem.at[i]) for i, (src, dst) in enumerate(
        ((clip_hbm, clip_ref), (mult_hbm, mult_ref), (nu_hbm, nz_s.at[0]), (nd_hbm, nz_s.at[1])))]
    top = n_layers - 1
    load_w(1, top).start()
    load_d(0).start()
    load_u(top, 0).start()

    def load_rest():
        load_w(0, top).start()
        load_x(0).start()
        for c in range(1, n_chunk):
            load_d(c).start()
            load_u(top, c).start()
        for layer in reversed(range(top)):
            load_w(1, layer).start()
            load_w(0, layer).start()
            for c in range(n_chunk):
                load_u(layer, c).start()
        for cp in load_small:
            cp.start()

    barrier = pltpu.get_barrier_semaphore()
    tp_peers = [(dp, (tp + 1 + r) % (2 * RING)) for r in range(2 * RING - 1)]
    peers = tp_peers + [dev_yl, dev_yr, dev_zl, dev_zr]
    for dev in peers:
        pl.semaphore_signal(barrier, inc=1, device_id=dev, device_id_type=MESH)


    def at(cc, xx, half=0, n=1):
        return pl.ds(pl.multiple_of(cc * (rows // 2) + xx * (rows // 8) + half * piece, 16), n * piece)

    def tp_copy(role, item):
        li, c, slot = item // n_chunk, item % n_chunk, item % n_chunk
        part, znew = p_s.at[slot], dz_s.at[li + 1, c]
        send, recv = ssem.at[role, c], rsem.at[role, c]
        if role == D2D:
            half = pl.ds(pl.multiple_of((1 - core) * (rows // 2), 16), rows // 2)
            return remote(part.at[half], rd2d.at[c], send, recv, partner)
        if role in (S1L, S1R):
            h = 0 if role == S1L else 1
            return remote(part.at[at(core, x_o, h)], r1.at[c, h], send, recv, (dev_l, dev_r)[h])
        if role == SDL:
            return remote(part.at[at(core, x_l, 1)], rdir.at[c, 0], send, recv, dev_l)
        if role == SDR:
            return remote(part.at[at(core, x_r, 0)], rdir.at[c, 1], send, recv, dev_r)
        if role == S2L:
            return remote(part.at[at(core, x_l, 0)], r2.at[c, 0], send, recv, dev_l)
        if role == S2R:
            return remote(part.at[at(core, x_r, 1)], r2.at[c, 1], send, recv, dev_r)
        where, dev = {
            A1L: (at(core, xi, 0, 2), dev_l),
            A1R: (at(core, xi, 0, 2), dev_r),
            A2L: (at(core, x_r, 0), dev_l),
            A2R: (at(core, x_l, 1), dev_r),
            FO: (at(core, xi, 0, 2), partner),
            FR: (at(core, x_r, 0, 2), partner),
            FL: (at(core, x_l, 0, 2), partner),
            FA: (at(core, x_o, 0), partner),
            FB: (at(core, x_o, 1), partner),
        }[role]
        return remote(znew.at[where], znew.at[where], send, recv, dev)

    def start(item, *roles):
        for role in roles:
            tp_copy(role, item).start()

    def arrived(item, *roles):
        for role in roles:
            tp_copy(role, item).wait_recv()

    def sent(item, *roles):
        for role in roles:
            tp_copy(role, item).wait_send()

    @scoped
    def pair_sum(item):
        c, slot = item % n_chunk, item % n_chunk
        arrived(item, D2D)
        base = core * (rows // 2)
        blk = rows // 8

        def add(b, _):
            mine = pl.ds(pl.multiple_of(base + b * blk, 16), blk)
            theirs = pl.ds(pl.multiple_of(b * blk, 16), blk)
            p_s[slot, mine, :] = (p_s[slot, mine, :].astype(F32) + rd2d[c, theirs, :].astype(F32)).astype(BF16)
            return 0

        lax.fori_loop(0, 4, add, 0)
        start(item, S1L, S1R)

    @scoped
    def relay_sum(item):
        c, slot = item % n_chunk, item % n_chunk
        for h, come, go, xx in ((0, S1L, S2L, x_l), (1, S1R, S2R, x_r)):
            arrived(item, come)
            where = at(core, xx, h)
            p_s[slot, where, :] = (p_s[slot, where, :].astype(F32) + r1[c, h].astype(F32)).astype(BF16)
            start(item, go)

    @scoped
    def own_sum(item):
        li, c, slot = item // n_chunk, item % n_chunk, item % n_chunk
        for h, far, near in ((0, S2L, SDR), (1, S2R, SDL)):
            arrived(item, near, far)
            where = at(core, xi, h)
            total = p_s[slot, where, :].astype(F32) + r2[c, h].astype(F32) + rdir[c, 1 - h].astype(F32)
            dz_s[li + 1, c, where, :] = (dz_s[li, c, where, :].astype(F32) + total).astype(BF16)
        start(item, A1L, A1R, FO)

    @scoped
    def gather_relay(item):
        arrived(item, A1L)
        start(item, A2L, FR)
        arrived(item, A1R)
        start(item, A2R, FL)
        sent(item, D2D, S1L, S1R, SDL, SDR, S2L, S2R)

    @scoped
    def gather_cross(item):
        arrived(item, A2L)
        start(item, FA)
        arrived(item, A2R)
        start(item, FB)

    def out_copy(c):
        return pltpu.make_async_copy(dz_s.at[n_layers, c], din_hbm.at[c], osem.at[c])

    @scoped
    def gather_end(item):
        arrived(item, FO, FR, FL, FA, FB)
        sent(item, A1L, A1R, A2L, A2R, FO, FR, FL, FA, FB)

        @pl.when(item >= n_item - n_chunk)
        def _():
            out_copy(item % n_chunk).start()

    @scoped
    def compute_dh(item, then=None):
        li, c = item // n_chunk, item % n_chunk
        layer = top - li

        @pl.when(c == 0)
        def _():
            load_w(1, layer).wait()

        @pl.when(li == 0)
        def _():
            load_d(c).wait()

        load_u(layer, c).wait()
        if then is not None:
            then()
        da_s[...] = lax.dot_general(dz_s[li, c], w2_s[layer], NT, preferred_element_type=F32)
        blk = 32

        def act(b, _):
            r = pl.ds(pl.multiple_of(b * blk, blk), blk)
            u = u_s[layer, c, r, :].astype(F32)
            u2 = u * u
            th = jnp.tanh(K_TANH * (u + 0.044715 * (u2 * u)))
            cdf = 0.5 * (1.0 + th)
            slope = cdf + (0.5 * u) * (1.0 - th * th) * K_TANH * (1.0 + (3 * 0.044715) * u2)
            u_s[layer, c, r, :] = (u * cdf).astype(BF16)
            dh_s[layer, c, r, :] = (slope * da_s[r, :]).astype(BF16)
            return 0

        lax.fori_loop(0, rows // blk, act, 0)

    @scoped
    def compute_back(item):
        li, c, slot = item // n_chunk, item % n_chunk, item % n_chunk
        layer = top - li

        @pl.when(c == 0)
        def _():
            load_w(0, layer).wait()

        for part in range(2):
            cc = 1 - core if part == 0 else core
            r = pl.ds(pl.multiple_of(cc * (rows // 2), 16), rows // 2)
            p_s[slot, r, :] = lax.dot_general(dh_s[layer, c, r, :], w1_s[layer], NT,
                                              preferred_element_type=F32).astype(BF16)
            if part == 0:
                start(item, D2D)

    @scoped
    def compute_norm(item):
        li, c = item // n_chunk, item % n_chunk
        layer = top - li
        load_x(item).wait()

        def one(e, _):
            r = pl.ds(pl.multiple_of(e * seq, 16), seq)

            def gram(v):
                return lax.dot_general(v, v, NT, preferred_element_type=F32)

            total = (gram(u_s[layer, c, r, :]) * gram(dz_s[li, c, r, :])
                     + gram(xs[item % 2, r, :]) * gram(dh_s[layer, c, r, :]))
            nrm[c * ex_per + e] += jnp.sum(total.reshape(seq // 8, 8, seq), axis=0)
            return 0

        lax.fori_loop(0, ex_per, one, 0)

    def norm_copies(c):
        return [remote(nsend.at[c], nrecv.at[c, r], nsem_s.at[c, r], nsem_r.at[c, r], dev)
                for r, dev in enumerate(tp_peers)]

    def norm_start(c):
        part = jnp.sum(nrm[pl.ds(c * ex_per, ex_per)], axis=1)
        part = jnp.broadcast_to(jnp.sum(part, axis=-1, keepdims=True), (ex_per, nsend.shape[-1]))
        nsend[c] = jnp.concatenate([part] * (nsend.shape[1] // ex_per), axis=0)
        for cp in norm_copies(c):
            cp.start()

    @scoped
    def clip_factors(c):
        total = nsend[c]
        for r, cp in enumerate(norm_copies(c)):
            cp.wait_recv()
            total = total + nrecv[c, r]
        factor = jnp.minimum(1.0, clip_ref[0] / jnp.sqrt(total))
        for e in range(ex_per):
            clip_s[c * ex_per + e] = jnp.broadcast_to(factor[e:e + 1, :], clip_s.shape[1:])
        for cp in norm_copies(c):
            cp.wait_send()

    def grad_view(k, kind, phase, j, h):
        if phase == 0:
            n = RING // 2
            if kind == 0:
                return g_s.at[k, pl.ds(h * n, n), j]
            return g_s.at[k, j, pl.ds(h * n, n)]
        n = g_s.shape[3] // 2
        if kind == 0:
            return g_s.at[k, j, yi, pl.ds(h * n, n)]
        return g_s.at[k, zi, j, pl.ds(h * n, n)]

    def ring_of(kind, phase):
        if (kind == 0) == (phase == 0):
            return yi, dev_yl, dev_yr
        return zi, dev_zl, dev_zr

    def grad_copy(k, kind, phase, role):
        me, d_l, d_r = ring_of(kind, phase)
        buf = (q1, q2)[phase]
        j, h = ((up(me, 2), 0), (up(me, 2), 1), (up(me, 3), 1), (up(me, 1), 0), (up(me, 3), 0), (up(me, 1), 1))[role]
        return remote(grad_view(k, kind, phase, j, h), buf.at[k, role], gsem_s.at[phase, role, k],
                      gsem_r.at[phase, role, k], d_r if role % 2 else d_l)

    @scoped
    def ring_start(p, kind, phase):
        k = 2 * p + kind
        for role in range(4):
            grad_copy(k, kind, phase, role).start()

    @scoped
    def ring_relay(p, kind, phase):
        k = 2 * p + kind
        me, _, _ = ring_of(kind, phase)
        buf = (q1, q2)[phase]
        for h in range(2):
            grad_copy(k, kind, phase, h).wait_recv()
            view = grad_view(k, kind, phase, up(me, 1 if h else 3), h)
            view[...] = view[...] + buf[k, h]
            grad_copy(k, kind, phase, 4 + h).start()

    @scoped
    def ring_end(p, kind, phase):
        k = 2 * p + kind
        me, _, _ = ring_of(kind, phase)
        buf = (q1, q2)[phase]
        for h in range(2):
            grad_copy(k, kind, phase, 3 - h).wait_recv()
            grad_copy(k, kind, phase, 4 + h).wait_recv()
            view = grad_view(k, kind, phase, me, h)
            view[...] = view[...] + buf[k, 3 - h] + buf[k, 4 + h]

    @scoped
    def ring_sent(p, kind, phase):
        for role in range(6):
            grad_copy(2 * p + kind, kind, phase, role).wait_send()

    inv = 1.0 / (n_ex * RING * RING)

    @scoped
    def finish(p, kind):
        layer, scale = top - p, mult_ref[0] * clip_ref[0]
        (gu_ref, gd_ref)[kind][layer] = (g_s[2 * p + kind, zi, yi] + scale * nz_s[kind, layer]) * inv

    @scoped
    def weight_grad(p, kind, lo, hi):
        k, layer = 2 * p + kind, top - p

        def one(c, _):
            if kind == 0:
                item = p * n_chunk + c

                @pl.when(item + 1 < n_item)
                def _():
                    load_x(item + 1).start()

                load_x(item).wait()
            for e in range(ex_per):
                f = clip_s[c * ex_per + e][0:1, 0:1]
                r = pl.ds(e * seq, seq)
                if kind == 0:
                    dh_s[layer, c, r, :] = (dh_s[layer, c, r, :].astype(F32) * f).astype(BF16)
                else:
                    xs[1, r, :] = (dz_s[p, c, r, :].astype(F32) * f).astype(BF16)
            if kind == 0:
                add = lax.dot_general(xs[c % 2], dh_s[layer, c], TN, preferred_element_type=F32)
            else:
                add = lax.dot_general(xs[1], u_s[layer, c], TN, preferred_element_type=F32)
            add = add.reshape(g_s.shape[1:])

            @pl.when(c == 0)
            def _():
                g_s[k] = add

            @pl.when(c > 0)
            def _():
                g_s[k] += add

            return 0

        lax.fori_loop(lo, hi, one, 0)

    late = n_item - n_chunk

    def slot_body(t, _):
        i_s = t - 1 - 2 * (t // (late + 3))

        def span(lo, n):
            return jnp.logical_and(t >= lo, t < lo + n)

        on_s = jnp.logical_or(span(1, late), t == late + 3)
        on_a = span(2, late)
        on_e = span(3, late)
        early = t < late
        load_x((t + 1) % n_item).start()

        @pl.when(on_s)
        def _():
            pair_sum(i_s)

        @pl.when(on_a)
        def _():
            own_sum(t - 2)

        @pl.when(on_s)
        def _():
            start(i_s, SDL, SDR)

        @pl.when(t > 0)
        def _():
            compute_dh(t)

        @pl.when(early)
        def _():
            @pl.when(on_e)
            def _():
                gather_cross(t - 3)

            compute_back(t)

        @pl.when(on_s)
        def _():
            relay_sum(i_s)

        compute_norm(t)

        @pl.when(jnp.logical_not(early))
        def _():
            norm_start(t - late)

            @pl.when(on_e)
            def _():
                gather_cross(t - 3)

            compute_back(t)

        @pl.when(on_a)
        def _():
            gather_relay(t - 2)

        @pl.when(on_e)
        def _():
            gather_end(t - 3)

        return 0

    nrm[...] = jnp.zeros_like(nrm)
    compute_dh(0, load_rest)
    pl.semaphore_wait(barrier, len(peers))
    lax.fori_loop(0, n_item, slot_body, 0)

    for cp in load_small:
        cp.wait()
    clip_factors(0)
    clip_factors(1)
    half = n_chunk // 2

    def grad_body(p, _):
        after = p >= 1
        weight_grad(p, 0, 0, half)

        @pl.when(after)
        def _():
            ring_relay(p - 1, 0, 0)

        pair_sum(late + 1 + p)
        own_sum(late + p)
        start(late + 1 + p, SDL, SDR)

        @pl.when(p == 0)
        def _():
            clip_factors(2)
            weight_grad(0, 0, half, n_chunk - 1)
            clip_factors(3)
            weight_grad(0, 0, n_chunk - 1, n_chunk)

        @pl.when(after)
        def _():
            weight_grad(p, 0, half, n_chunk)

        ring_start(p, 0, 0)

        @pl.when(p == 2)
        def _():
            ring_end(0, 1, 0)
            ring_start(0, 1, 1)

        @pl.when(after)
        def _():
            gather_cross(late + p - 1)

        weight_grad(p, 1, 0, half)

        @pl.when(after)
        def _():
            ring_relay(p - 1, 1, 0)

        relay_sum(late + 1 + p)
        weight_grad(p, 1, half, n_chunk)
        ring_start(p, 1, 0)
        gather_relay(late + p)

        @pl.when(after)
        def _():
            gather_end(late + p - 1)
            ring_end(p - 1, 0, 0)
            ring_start(p - 1, 0, 1)

        return 0

    lax.fori_loop(0, n_layers, grad_body, 0)
    last = n_item - 1
    own_sum(last)
    gather_cross(last - 1)
    ring_relay(0, 0, 1)
    gather_end(last - 1)
    ring_relay(0, 1, 1)
    ring_relay(2, 0, 0)
    gather_relay(last)
    ring_end(1, 1, 0)
    ring_start(1, 1, 1)
    ring_relay(1, 0, 1)
    ring_relay(2, 1, 0)
    gather_cross(last)
    ring_end(2, 0, 0)
    ring_start(2, 0, 1)
    gather_end(last)
    ring_relay(1, 1, 1)
    ring_end(2, 1, 0)
    ring_start(2, 1, 1)
    ring_relay(2, 0, 1)
    ring_relay(2, 1, 1)
    for p in range(n_layers):
        for kind in range(2):
            ring_end(p, kind, 1)
            finish(p, kind)
            ring_sent(p, kind, 0)
            ring_sent(p, kind, 1)
    for c in range(n_chunk):
        out_copy(c).wait()


def pass_on(gu_in, gd_in, din_in, gu_out, gd_out, din_out, g_buf, d_buf, isem, osem):
    views = [(din_in.at[c], d_buf.at[c], din_out.at[c]) for c in range(N_CHUNK)]
    views += [(gu_in, g_buf.at[0], gu_out), (gd_in, g_buf.at[1], gd_out)]
    for i, (src, buf, _) in enumerate(views):
        pltpu.make_async_copy(src, buf, isem.at[i]).start()
    for i, (src, buf, dst) in enumerate(views):
        pltpu.make_async_copy(src, buf, isem.at[i]).wait()
        pltpu.make_async_copy(buf, dst, osem.at[i]).start()
    for i, (_, buf, dst) in enumerate(views):
        pltpu.make_async_copy(buf, dst, osem.at[i]).wait()


def solution(mesh):
    n_dp, n_tp = mesh.shape["dp"], mesh.shape["tp"]

    def local(x_in, u_pre, w_up, w_down, d_out, noise_up, noise_down, clip_norm, noise_mult):
        n_layers, micro, batch, seq, dim = x_in.shape
        hid = u_pre.shape[-1]
        n_ex = micro * batch
        rows = n_ex * seq // N_CHUNK
        piece, grad_rows = rows // 16, dim // n_dp
        x4 = x_in.reshape(n_layers, N_CHUNK, rows, dim)
        u4 = u_pre.reshape(n_layers, N_CHUNK, rows, hid)
        d4 = d_out.reshape(N_CHUNK, rows, dim)
        anyspace = pl.BlockSpec(memory_space=pl.ANY)
        vmem = pl.BlockSpec(memory_space=pltpu.VMEM)
        dma = pltpu.SemaphoreType.DMA
        tokens = n_ex * seq
        flops = 2 * n_layers * tokens * hid * dim * 4 + 4 * n_layers * tokens * seq * (hid + dim)
        g_up, g_down, d_in = pl.pallas_call(
            step_kernel,
            out_shape=(
                jax.ShapeDtypeStruct((n_layers, grad_rows, hid), F32),
                jax.ShapeDtypeStruct((n_layers, grad_rows, hid), F32),
                jax.ShapeDtypeStruct((N_CHUNK, rows, dim), BF16),
            ),
            in_specs=[anyspace] * 9,
            out_specs=(vmem, vmem, anyspace),
            scratch_shapes=[
                pltpu.VMEM((n_layers, N_CHUNK, rows, hid), BF16),
                pltpu.VMEM((n_layers, N_CHUNK, rows, hid), BF16),
                pltpu.VMEM((n_layers + 1, N_CHUNK, rows, dim), BF16),
                pltpu.VMEM((n_layers, dim, hid), BF16),
                pltpu.VMEM((n_layers, hid, dim), BF16),
                pltpu.VMEM((2, rows, dim), BF16),
                pltpu.VMEM((rows, hid), F32),
                pltpu.VMEM((N_CHUNK, rows, dim), BF16),
                pltpu.VMEM((N_CHUNK, rows // 2, dim), BF16),
                pltpu.VMEM((N_CHUNK, 2, piece, dim), BF16),
                pltpu.VMEM((N_CHUNK, 2, piece, dim), BF16),
                pltpu.VMEM((N_CHUNK, 2, piece, dim), BF16),
                pltpu.VMEM((2 * n_layers, RING, RING, grad_rows, hid), F32),
                pltpu.VMEM((2 * n_layers, 6, RING // 2, grad_rows, hid), F32),
                pltpu.VMEM((2 * n_layers, 6, grad_rows // 2, hid), F32),
                pltpu.VMEM((n_ex, 8, seq), F32),
                pltpu.VMEM((N_CHUNK, 8, 128), F32),
                pltpu.VMEM((N_CHUNK, 2 * RING - 1, 8, 128), F32),
                pltpu.VMEM((n_ex, 8, 128), F32),
                pltpu.VMEM((2, n_layers, grad_rows, hid), F32),
                pltpu.SMEM((1,), F32),
                pltpu.SMEM((1,), F32),
                dma((N_ROLE, N_CHUNK)),
                dma((N_ROLE, N_CHUNK)),
                dma((2, 6, 2 * n_layers)),
                dma((2, 6, 2 * n_layers)),
                dma((N_CHUNK, 2 * RING - 1)),
                dma((N_CHUNK, 2 * RING - 1)),
                dma((n_layers, N_CHUNK)),
                dma((2, n_layers)),
                dma((N_CHUNK,)),
                dma((2,)),
                dma((N_CHUNK,)),
                dma((4,)),
            ],
            compiler_params=pltpu.CompilerParams(
                collective_id=0, has_side_effects=True, vmem_limit_bytes=67_043_328
            ),
            cost_estimate=pl.CostEstimate(flops=flops, bytes_accessed=50_000_000, transcendentals=n_layers * tokens * hid),
            name="clipped_step",
        )(x4, u4, w_up, w_down, d4, noise_up, jnp.transpose(noise_down, (0, 2, 1)), clip_norm, noise_mult)
        shapes = [jax.ShapeDtypeStruct(v.shape, v.dtype) for v in (g_up, g_down, d_in)]
        g_up, g_down, d_in = pl.pallas_call(
            pass_on,
            out_shape=shapes,
            in_specs=[anyspace] * 3,
            out_specs=[anyspace] * 3,
            scratch_shapes=[
                pltpu.VMEM((2,) + g_up.shape, F32),
                pltpu.VMEM(d_in.shape, BF16),
                dma((N_CHUNK + 2,)),
                dma((N_CHUNK + 2,)),
            ],
            name="pass_on",
        )(g_up, g_down, d_in)
        return g_up, jnp.transpose(g_down, (0, 2, 1)), d_in.reshape(d_out.shape)

    in_specs = (P(None, None, "dp", None, None), P(None, None, "dp", None, "tp"), P(None, None, "tp"),
                P(None, "tp", None), P(None, "dp", None, None), P(None, "dp", "tp"), P(None, "tp", "dp"), P(), P())
    out_specs = (P(None, "dp", "tp"), P(None, "tp", "dp"), P(None, "dp", None, None))
    return jax.shard_map(local, mesh=mesh, in_specs=in_specs, out_specs=out_specs, check_vma=False)
```

```python
import math

import jax
import jax.numpy as jnp
from jax import lax
from jax.experimental import pallas as pl
from jax.experimental.pallas import tpu as pltpu
from jax.sharding import PartitionSpec as P

MESH = pl.DeviceIdType.MESH
F32, BF16 = jnp.float32, jnp.bfloat16
N_CHUNK = 4
RING = 4
K_TANH = math.sqrt(2.0 / math.pi)
(D2D, S1L, S1R, SDL, SDR, S2L, S2R, A1L, A1R, A2L, A2R, FO, FR, FL, FA, FB) = range(16)
N_ROLE = 16
NT = (((1,), (1,)), ((), ()))
TN = (((0,), (0,)), ((), ()))


def scoped(f):
    def g(*a):
        with jax.named_scope(f.__name__):
            return f(*a)
    return g


def step_kernel(x_hbm, u_hbm, w1_hbm, w2_hbm, do_hbm, nu_hbm, nd_hbm, clip_hbm, mult_hbm,
                gu_ref, gd_ref, din_ref,
                u_s, dh_s, dz_s, w1_s, w2_s, xs, sc_s, da_s, p_s, rd2d, r1, rdir, r2, g_s, q1, q2,
                nrm, nsend, nrecv, clip_s, nz_s, clip_ref, mult_ref,
                ssem, rsem, gsem_s, gsem_r, nsem_s, nsem_r, usem, wsem, dsem, xsem, csem):
    n_layers, n_chunk, rows, hid = u_s.shape
    dim = dz_s.shape[-1]
    n_ex, _, seq = nrm.shape
    ex_per = n_ex // n_chunk
    piece = rows // 16
    n_item = n_layers * n_chunk
    dp, tp = lax.axis_index("dp"), lax.axis_index("tp")
    xi, core = tp // 2, tp % 2
    zi, yi = dp // RING, dp % RING

    def up(i, by=1):
        return (i + by) % RING

    x_l, x_r, x_o = up(xi, 3), up(xi, 1), up(xi, 2)
    partner = (dp, xi * 2 + 1 - core)
    dev_l, dev_r = (dp, x_l * 2 + core), (dp, x_r * 2 + core)
    dev_yl, dev_yr = (zi * RING + up(yi, 3), tp), (zi * RING + up(yi), tp)
    dev_zl, dev_zr = (up(zi, 3) * RING + yi, tp), (up(zi) * RING + yi, tp)

    def remote(src, dst, send, recv, dev):
        return pltpu.make_async_remote_copy(src_ref=src, dst_ref=dst, send_sem=send, recv_sem=recv,
                                            device_id=dev, device_id_type=MESH)

    def load_u(layer, c):
        return pltpu.make_async_copy(u_hbm.at[layer, c], u_s.at[layer, c], usem.at[layer, c])

    def load_w(which, layer):
        src, dst = ((w1_hbm, w1_s), (w2_hbm, w2_s))[which]
        return pltpu.make_async_copy(src.at[layer], dst.at[layer], wsem.at[which, layer])

    def load_d(c):
        return pltpu.make_async_copy(do_hbm.at[c], dz_s.at[0, c], dsem.at[c])

    def load_x(n):
        layer, c, slot = n_layers - 1 - n % n_item // n_chunk, n % n_chunk, n % 2
        return pltpu.make_async_copy(x_hbm.at[layer, c], xs.at[slot], xsem.at[slot])

    load_small = [pltpu.make_async_copy(src, dst, csem.at[i]) for i, (src, dst) in enumerate(
        ((clip_hbm, clip_ref), (mult_hbm, mult_ref), (nu_hbm, nz_s.at[0]), (nd_hbm, nz_s.at[1])))]
    top = n_layers - 1
    load_w(1, top).start()
    load_d(0).start()
    load_u(top, 0).start()

    def load_rest():
        load_w(0, top).start()
        load_x(0).start()
        load_x(1).start()
        for c in range(1, n_chunk):
            load_d(c).start()
            load_u(top, c).start()
        for layer in reversed(range(top)):
            load_w(1, layer).start()
            load_w(0, layer).start()
            for c in range(n_chunk):
                load_u(layer, c).start()
        for cp in load_small:
            cp.start()

    barrier = pltpu.get_barrier_semaphore()
    tp_peers = [(dp, (tp + 1 + r) % (2 * RING)) for r in range(2 * RING - 1)]
    peers = tp_peers + [dev_yl, dev_yr, dev_zl, dev_zr]
    for dev in peers:
        pl.semaphore_signal(barrier, inc=1, device_id=dev, device_id_type=MESH)


    def at(cc, xx, half=0, n=1):
        return pl.ds(pl.multiple_of(cc * (rows // 2) + xx * (rows // 8) + half * piece, 16), n * piece)

    def tp_copy(role, item):
        li, c, slot = item // n_chunk, item % n_chunk, item % n_chunk
        part, znew = p_s.at[slot], (din_ref.at[c] if li + 1 == n_layers else dz_s.at[li + 1, c])
        send, recv = ssem.at[role, c], rsem.at[role, c]
        if role == D2D:
            half = pl.ds(pl.multiple_of((1 - core) * (rows // 2), 16), rows // 2)
            return remote(part.at[half], rd2d.at[c], send, recv, partner)
        if role in (S1L, S1R):
            h = 0 if role == S1L else 1
            return remote(part.at[at(core, x_o, h)], r1.at[c, h], send, recv, (dev_l, dev_r)[h])
        if role == SDL:
            return remote(part.at[at(core, x_l, 1)], rdir.at[c, 0], send, recv, dev_l)
        if role == SDR:
            return remote(part.at[at(core, x_r, 0)], rdir.at[c, 1], send, recv, dev_r)
        if role == S2L:
            return remote(part.at[at(core, x_l, 0)], r2.at[c, 0], send, recv, dev_l)
        if role == S2R:
            return remote(part.at[at(core, x_r, 1)], r2.at[c, 1], send, recv, dev_r)
        where, dev = {
            A1L: (at(core, xi, 0, 2), dev_l),
            A1R: (at(core, xi, 0, 2), dev_r),
            A2L: (at(core, x_r, 0), dev_l),
            A2R: (at(core, x_l, 1), dev_r),
            FO: (at(core, xi, 0, 2), partner),
            FR: (at(core, x_r, 0, 2), partner),
            FL: (at(core, x_l, 0, 2), partner),
            FA: (at(core, x_o, 0), partner),
            FB: (at(core, x_o, 1), partner),
        }[role]
        return remote(znew.at[where], znew.at[where], send, recv, dev)

    def start(item, *roles):
        for role in roles:
            tp_copy(role, item).start()

    def arrived(item, *roles):
        for role in roles:
            tp_copy(role, item).wait_recv()

    def sent(item, *roles):
        for role in roles:
            tp_copy(role, item).wait_send()

    @scoped
    def pair_sum(item):
        c, slot = item % n_chunk, item % n_chunk
        arrived(item, D2D)
        base = core * (rows // 2)
        blk = rows // 8

        def add(b, _):
            mine = pl.ds(pl.multiple_of(base + b * blk, 16), blk)
            theirs = pl.ds(pl.multiple_of(b * blk, 16), blk)
            p_s[slot, mine, :] = (p_s[slot, mine, :].astype(F32) + rd2d[c, theirs, :].astype(F32)).astype(BF16)
            return 0

        lax.fori_loop(0, 4, add, 0)
        start(item, S1L, S1R)

    @scoped
    def relay_sum(item):
        c, slot = item % n_chunk, item % n_chunk
        for h, come, go, xx in ((0, S1L, S2L, x_l), (1, S1R, S2R, x_r)):
            arrived(item, come)
            where = at(core, xx, h)
            p_s[slot, where, :] = (p_s[slot, where, :].astype(F32) + r1[c, h].astype(F32)).astype(BF16)
            start(item, go)

    @scoped
    def own_sum(item):
        li, c, slot = item // n_chunk, item % n_chunk, item % n_chunk
        for h, far, near in ((0, S2L, SDR), (1, S2R, SDL)):
            arrived(item, near, far)
            where = at(core, xi, h)
            total = p_s[slot, where, :].astype(F32) + r2[c, h].astype(F32) + rdir[c, 1 - h].astype(F32)
            total = (dz_s[li, c, where, :].astype(F32) + total).astype(BF16)
            if li + 1 == n_layers:
                din_ref[c, where, :] = total
            else:
                dz_s[li + 1, c, where, :] = total
        start(item, A1L, A1R, FO)

    @scoped
    def gather_relay(item):
        arrived(item, A1L)
        start(item, A2L, FR)
        arrived(item, A1R)
        start(item, A2R, FL)
        sent(item, D2D, S1L, S1R, SDL, SDR, S2L, S2R)

    @scoped
    def gather_cross(item):
        arrived(item, A2L)
        start(item, FA)
        arrived(item, A2R)
        start(item, FB)

    @scoped
    def gather_end(item):
        arrived(item, FO, FR, FL, FA, FB)
        sent(item, A1L, A1R, A2L, A2R, FO, FR, FL, FA, FB)

    @scoped
    def compute_dh(item, then=None):
        li, c = item // n_chunk, item % n_chunk
        layer = top - li

        if c == 0:
            load_w(1, layer).wait()
            if li > 0:
                load_w(0, layer).wait()
        if li == 0:
            load_d(c).wait()
        load_u(layer, c).wait()
        if then is not None:
            then()
        da_s[...] = lax.dot_general(dz_s[li, c], w2_s[layer], NT, preferred_element_type=F32)
        blk = 32

        def act(b, _):
            r = pl.ds(pl.multiple_of(b * blk, blk), blk)
            u = u_s[layer, c, r, :].astype(F32)
            u2 = u * u
            th = jnp.tanh(K_TANH * (u + 0.044715 * (u2 * u)))
            cdf = 0.5 * (1.0 + th)
            slope = cdf + (0.5 * u) * (1.0 - th * th) * K_TANH * (1.0 + (3 * 0.044715) * u2)
            u_s[layer, c, r, :] = (u * cdf).astype(BF16)
            dh_s[layer, c, r, :] = (slope * da_s[r, :]).astype(BF16)
            return 0

        lax.fori_loop(0, rows // blk, act, 0)

    @scoped
    def compute_back(item):
        li, c, slot = item // n_chunk, item % n_chunk, item % n_chunk
        layer = top - li
        if item == 0:
            load_w(0, layer).wait()
        def part(n, _):
            cc = (core + 1 + n) % 2
            r = pl.ds(pl.multiple_of(cc * (rows // 2), 16), rows // 2)
            p_s[slot, r, :] = lax.dot_general(dh_s[layer, c, r, :], w1_s[layer], NT,
                                              preferred_element_type=F32).astype(BF16)

            @pl.when(n == 0)
            def _():
                start(item, D2D)

            return 0

        lax.fori_loop(0, 2, part, 0)

    @scoped
    def compute_norm(item):
        li, c = item // n_chunk, item % n_chunk
        layer = top - li
        load_x(item).wait()

        def one(e, _):
            r = pl.ds(pl.multiple_of(e * seq, 16), seq)

            def gram(v):
                return lax.dot_general(v, v, NT, preferred_element_type=F32)

            total = (gram(u_s[layer, c, r, :]) * gram(dz_s[li, c, r, :])
                     + gram(xs[item % 2, r, :]) * gram(dh_s[layer, c, r, :]))
            nrm[c * ex_per + e] += jnp.sum(total.reshape(seq // 8, 8, seq), axis=0)
            return 0

        lax.fori_loop(0, ex_per, one, 0)
        load_x(item + 2).start()
        if li == top:
            norm_start(c)

    def norm_copies(c):
        return [remote(nsend.at[c], nrecv.at[c, r], nsem_s.at[c, r], nsem_r.at[c, r], dev)
                for r, dev in enumerate(tp_peers)]

    @scoped
    def norm_start(c):
        part = jnp.sum(nrm[pl.ds(c * ex_per, ex_per)], axis=1)
        part = jnp.broadcast_to(jnp.sum(part, axis=-1, keepdims=True), (ex_per, nsend.shape[-1]))
        nsend[c] = jnp.concatenate([part] * (nsend.shape[1] // ex_per), axis=0)
        for cp in norm_copies(c):
            cp.start()

    @scoped
    def clip_factors(c):
        total = nsend[c]
        for r, cp in enumerate(norm_copies(c)):
            cp.wait_recv()
            total = total + nrecv[c, r]
        factor = jnp.minimum(1.0, clip_ref[0] / jnp.sqrt(total))
        for e in range(ex_per):
            clip_s[c * ex_per + e] = jnp.broadcast_to(factor[e:e + 1, :], clip_s.shape[1:])
        for cp in norm_copies(c):
            cp.wait_send()

    def grad_view(k, kind, phase, j, h):
        if phase == 0:
            n = RING // 2
            if kind == 0:
                return g_s.at[k, pl.ds(h * n, n), j]
            return g_s.at[k, j, pl.ds(h * n, n)]
        n = g_s.shape[3] // 2
        if kind == 0:
            return g_s.at[k, j, yi, pl.ds(h * n, n)]
        return g_s.at[k, zi, j, pl.ds(h * n, n)]

    def ring_of(kind, phase):
        if (kind == 0) == (phase == 0):
            return yi, dev_yl, dev_yr
        return zi, dev_zl, dev_zr

    def grad_copy(k, kind, phase, role):
        me, d_l, d_r = ring_of(kind, phase)
        buf = (q1, q2)[phase]
        j, h = ((up(me, 2), 0), (up(me, 2), 1), (up(me, 3), 1), (up(me, 1), 0), (up(me, 3), 0), (up(me, 1), 1))[role]
        return remote(grad_view(k, kind, phase, j, h), buf.at[k, role], gsem_s.at[phase, role, k],
                      gsem_r.at[phase, role, k], d_r if role % 2 else d_l)

    @scoped
    def ring_start(p, kind, phase):
        k = 2 * p + kind
        for role in range(4):
            grad_copy(k, kind, phase, role).start()

    @scoped
    def ring_relay(p, kind, phase):
        k = 2 * p + kind
        me, _, _ = ring_of(kind, phase)
        buf = (q1, q2)[phase]
        for h in range(2):
            grad_copy(k, kind, phase, h).wait_recv()
            view = grad_view(k, kind, phase, up(me, 1 if h else 3), h)
            view[...] = view[...] + buf[k, h]
            grad_copy(k, kind, phase, 4 + h).start()

    @scoped
    def ring_end(p, kind, phase):
        k = 2 * p + kind
        me, _, _ = ring_of(kind, phase)
        buf = (q1, q2)[phase]
        for h in range(2):
            grad_copy(k, kind, phase, 3 - h).wait_recv()
            grad_copy(k, kind, phase, 4 + h).wait_recv()
            view = grad_view(k, kind, phase, me, h)
            view[...] = view[...] + buf[k, 3 - h] + buf[k, 4 + h]

    @scoped
    def ring_sent(p, kind, phase):
        for role in range(6):
            grad_copy(2 * p + kind, kind, phase, role).wait_send()

    inv = 1.0 / (n_ex * RING * RING)

    @scoped
    def finish(p, kind):
        layer, scale = top - p, mult_ref[0] * clip_ref[0]
        (gu_ref, gd_ref)[kind][layer] = (g_s[2 * p + kind, zi, yi] + scale * nz_s[kind, layer]) * inv

    @scoped
    def weight_grad(p, kind, c):
        k, layer, n = 2 * p + kind, top - p, p * n_chunk + c

        def scaled(e, _):
            r = pl.ds(pl.multiple_of(e * seq, 16), seq)
            f = clip_s[c * ex_per + e][0:1, 0:1]
            if kind == 0:
                dh_s[layer, c, r, :] = (dh_s[layer, c, r, :].astype(F32) * f).astype(BF16)
            else:
                sc_s[r, :] = (dz_s[p, c, r, :].astype(F32) * f).astype(BF16)
            return 0

        lax.fori_loop(0, ex_per, scaled, 0)
        if kind == 0:
            load_x(n_item + n).wait()
        cols = dim // 2

        def part(h, _):
            w = pl.ds(pl.multiple_of(h * cols, 128), cols)
            if kind == 0:
                add = lax.dot_general(xs[n % 2, :, w], dh_s[layer, c], TN, preferred_element_type=F32)
            else:
                add = lax.dot_general(sc_s[:, w], u_s[layer, c], TN, preferred_element_type=F32)
            add = add.reshape((RING // 2,) + g_s.shape[2:])
            z = pl.ds(h * (RING // 2), RING // 2)
            if c == 0:
                g_s[k, z] = add
            else:
                g_s[k, z] += add
            return 0

        lax.fori_loop(0, 2, part, 0)
        if kind == 0 and n + 2 < n_item:
            load_x(n_item + n + 2).start()

    nrm[...] = jnp.zeros_like(nrm)
    compute_dh(0, load_rest)
    pl.semaphore_wait(barrier, len(peers))
    compute_back(0)
    compute_dh(1)
    pair_sum(0)
    compute_back(1)
    start(0, SDL, SDR)
    pair_sum(1)
    start(1, SDL, SDR)
    compute_dh(2)
    compute_back(2)
    relay_sum(0)
    relay_sum(1)
    compute_dh(3)
    pair_sum(2)
    start(2, SDL, SDR)
    compute_back(3)
    own_sum(0)
    compute_norm(0)
    own_sum(1)
    compute_norm(1)
    gather_relay(0)
    relay_sum(2)
    pair_sum(3)
    gather_relay(1)
    gather_cross(0)
    compute_norm(2)
    gather_end(0)
    own_sum(2)
    compute_dh(4)
    start(3, SDL, SDR)
    gather_cross(1)
    relay_sum(3)
    compute_norm(3)
    gather_end(1)
    compute_back(4)
    gather_relay(2)
    pair_sum(4)
    start(4, SDL, SDR)
    compute_dh(5)
    compute_back(5)
    own_sum(3)
    gather_cross(2)
    compute_norm(4)
    relay_sum(4)
    gather_end(2)
    pair_sum(5)
    start(5, SDL, SDR)
    compute_norm(5)
    gather_relay(3)
    compute_dh(6)
    relay_sum(5)
    own_sum(4)
    compute_back(6)
    gather_cross(3)
    own_sum(5)
    gather_end(3)
    compute_dh(7)
    gather_relay(4)
    pair_sum(6)
    compute_norm(6)
    compute_back(7)
    gather_relay(5)
    pair_sum(7)
    gather_cross(4)
    compute_norm(7)
    relay_sum(6)
    gather_end(4)
    start(6, SDL, SDR)
    start(7, SDL, SDR)
    compute_dh(8)
    gather_cross(5)
    compute_norm(8)
    relay_sum(7)
    gather_end(5)
    compute_dh(9)
    own_sum(6)
    compute_norm(9)
    compute_back(9)
    own_sum(7)
    for cp in load_small:
        cp.wait()
    clip_factors(0)
    weight_grad(1, 1, 0)
    weight_grad(2, 1, 0)
    weight_grad(0, 1, 0)
    gather_relay(6)
    clip_factors(1)
    pair_sum(9)
    compute_back(8)
    weight_grad(0, 1, 1)
    gather_relay(7)
    weight_grad(2, 1, 1)
    pair_sum(8)
    start(8, SDL, SDR)
    gather_cross(6)
    weight_grad(1, 1, 1)
    start(9, SDL, SDR)
    gather_end(6)
    compute_dh(10)
    gather_cross(7)
    compute_norm(10)
    gather_end(7)
    compute_dh(11)
    compute_norm(11)
    weight_grad(0, 0, 0)
    clip_factors(2)
    weight_grad(0, 0, 1)
    weight_grad(0, 1, 2)
    clip_factors(3)
    weight_grad(0, 0, 2)
    weight_grad(0, 1, 3)
    ring_start(0, 1, 0)
    weight_grad(0, 0, 3)
    ring_start(0, 0, 0)
    relay_sum(9)
    relay_sum(8)
    weight_grad(1, 0, 0)
    compute_back(10)
    weight_grad(1, 1, 2)
    pair_sum(10)
    weight_grad(1, 1, 3)
    ring_relay(0, 1, 0)
    own_sum(9)
    start(10, SDL, SDR)
    ring_relay(0, 0, 0)
    weight_grad(1, 0, 1)
    ring_start(1, 1, 0)
    weight_grad(1, 0, 2)
    weight_grad(1, 0, 3)
    ring_start(1, 0, 0)
    own_sum(8)
    weight_grad(2, 1, 2)
    compute_back(11)
    weight_grad(2, 0, 0)
    weight_grad(2, 1, 3)
    ring_start(2, 1, 0)
    gather_relay(9)
    pair_sum(11)
    relay_sum(10)
    weight_grad(2, 0, 1)
    ring_relay(1, 0, 0)
    weight_grad(2, 0, 2)
    weight_grad(2, 0, 3)
    ring_start(2, 0, 0)
    gather_relay(8)
    relay_sum(11)
    gather_cross(9)
    start(11, SDL, SDR)
    ring_relay(2, 1, 0)
    gather_end(9)
    ring_relay(1, 1, 0)
    own_sum(10)
    ring_relay(2, 0, 0)
    gather_cross(8)
    ring_end(1, 0, 0)
    ring_start(1, 0, 1)
    own_sum(11)
    gather_end(8)
    ring_end(2, 1, 0)
    ring_start(2, 1, 1)
    ring_end(0, 0, 0)
    ring_start(0, 0, 1)
    ring_end(0, 1, 0)
    ring_start(0, 1, 1)
    gather_relay(10)
    ring_end(2, 0, 0)
    ring_start(2, 0, 1)
    ring_end(1, 1, 0)
    ring_start(1, 1, 1)
    gather_relay(11)
    ring_relay(1, 0, 1)
    ring_relay(2, 1, 1)
    ring_relay(0, 0, 1)
    ring_relay(0, 1, 1)
    gather_cross(10)
    ring_relay(2, 0, 1)
    ring_relay(1, 1, 1)
    gather_cross(11)
    gather_end(10)
    gather_end(11)
    ring_end(2, 0, 1)
    finish(2, 0)
    ring_end(2, 1, 1)
    finish(2, 1)
    ring_end(1, 0, 1)
    finish(1, 0)
    ring_end(0, 0, 1)
    finish(0, 0)
    ring_end(0, 1, 1)
    finish(0, 1)
    ring_end(1, 1, 1)
    finish(1, 1)
    for p in range(n_layers):
        for kind in range(2):
            ring_sent(p, kind, 0)
            ring_sent(p, kind, 1)


def solution(mesh):
    n_dp, n_tp = mesh.shape["dp"], mesh.shape["tp"]

    def local(x_in, u_pre, w_up, w_down, d_out, noise_up, noise_down, clip_norm, noise_mult):
        n_layers, micro, batch, seq, dim = x_in.shape
        hid = u_pre.shape[-1]
        n_ex = micro * batch
        rows = n_ex * seq // N_CHUNK
        piece, grad_rows = rows // 16, dim // n_dp
        x4 = x_in.reshape(n_layers, N_CHUNK, rows, dim)
        u4 = u_pre.reshape(n_layers, N_CHUNK, rows, hid)
        d4 = d_out.reshape(N_CHUNK, rows, dim)
        anyspace = pl.BlockSpec(memory_space=pl.ANY)
        vmem = pl.BlockSpec(memory_space=pltpu.VMEM)
        dma = pltpu.SemaphoreType.DMA
        tokens = n_ex * seq
        flops = 2 * n_layers * tokens * hid * dim * 4 + 4 * n_layers * tokens * seq * (hid + dim)
        g_up, g_down, d_in = pl.pallas_call(
            step_kernel,
            out_shape=(
                pltpu.VMEM((n_layers, grad_rows, hid), F32),
                pltpu.VMEM((n_layers, grad_rows, hid), F32),
                pltpu.VMEM((N_CHUNK, rows, dim), BF16),
            ),
            in_specs=[anyspace] * 9,
            out_specs=(vmem, vmem, vmem),
            scratch_shapes=[
                pltpu.VMEM((n_layers, N_CHUNK, rows, hid), BF16),
                pltpu.VMEM((n_layers, N_CHUNK, rows, hid), BF16),
                pltpu.VMEM((n_layers, N_CHUNK, rows, dim), BF16),
                pltpu.VMEM((n_layers, dim, hid), BF16),
                pltpu.VMEM((n_layers, hid, dim), BF16),
                pltpu.VMEM((2, rows, dim), BF16),
                pltpu.VMEM((rows, dim), BF16),
                pltpu.VMEM((rows, hid), F32),
                pltpu.VMEM((N_CHUNK, rows, dim), BF16),
                pltpu.VMEM((N_CHUNK, rows // 2, dim), BF16),
                pltpu.VMEM((N_CHUNK, 2, piece, dim), BF16),
                pltpu.VMEM((N_CHUNK, 2, piece, dim), BF16),
                pltpu.VMEM((N_CHUNK, 2, piece, dim), BF16),
                pltpu.VMEM((2 * n_layers, RING, RING, grad_rows, hid), F32),
                pltpu.VMEM((2 * n_layers, 6, RING // 2, grad_rows, hid), F32),
                pltpu.VMEM((2 * n_layers, 6, grad_rows // 2, hid), F32),
                pltpu.VMEM((n_ex, 8, seq), F32),
                pltpu.VMEM((N_CHUNK, 8, 128), F32),
                pltpu.VMEM((N_CHUNK, 2 * RING - 1, 8, 128), F32),
                pltpu.VMEM((n_ex, 8, 128), F32),
                pltpu.VMEM((2, n_layers, grad_rows, hid), F32),
                pltpu.SMEM((1,), F32),
                pltpu.SMEM((1,), F32),
                dma((N_ROLE, N_CHUNK)),
                dma((N_ROLE, N_CHUNK)),
                dma((2, 6, 2 * n_layers)),
                dma((2, 6, 2 * n_layers)),
                dma((N_CHUNK, 2 * RING - 1)),
                dma((N_CHUNK, 2 * RING - 1)),
                dma((n_layers, N_CHUNK)),
                dma((2, n_layers)),
                dma((N_CHUNK,)),
                dma((2,)),
                dma((4,)),
            ],
            compiler_params=pltpu.CompilerParams(
                collective_id=0, has_side_effects=True, vmem_limit_bytes=61_700_000
            ),
            cost_estimate=pl.CostEstimate(flops=flops, bytes_accessed=50_000_000, transcendentals=n_layers * tokens * hid),
            name="clipped_step",
        )(x4, u4, w_up, w_down, d4, noise_up, jnp.transpose(noise_down, (0, 2, 1)), clip_norm, noise_mult)
        return g_up, jnp.transpose(g_down, (0, 2, 1)), d_in.reshape(d_out.shape)

    in_specs = (P(None, None, "dp", None, None), P(None, None, "dp", None, "tp"), P(None, None, "tp"),
                P(None, "tp", None), P(None, "dp", None, None), P(None, "dp", "tp"), P(None, "tp", "dp"), P(), P())
    out_specs = (P(None, "dp", "tp"), P(None, "tp", "dp"), P(None, "dp", None, None))
    return jax.shard_map(local, mesh=mesh, in_specs=in_specs, out_specs=out_specs, check_vma=False)
```

```python
import functools
import math

import jax
import jax.numpy as jnp
from jax import lax
from jax.experimental import pallas as pl
from jax.experimental.pallas import tpu as pltpu
from jax.sharding import PartitionSpec as P

MESH = pl.DeviceIdType.MESH
F32, BF16 = jnp.float32, jnp.bfloat16
N_CHUNK = 4
RING = 4
K_TANH = math.sqrt(2.0 / math.pi)
(D2D, S1L, S1R, SDL, SDR, S2L, S2R, A1L, A1R, A2L, A2R, FO, FR, FL, FA, FB) = range(16)
GROUP = [0, 1, 1, 2, 2, 2, 2, 3, 3, 4, 4, 5, 5, 5, 5, 5]
GROUP_PIECES = [8, 2, 4, 4, 2, 8]
NT = (((1,), (1,)), ((), ()))
TN = (((0,), (0,)), ((), ()))


def scoped(f):
    def g(*a):
        with jax.named_scope(f.__name__):
            return f(*a)
    return g


def step_kernel(x_hbm, u_hbm, w1_hbm, w2_hbm, do_hbm, nu_hbm, nd_hbm, clip_hbm, mult_hbm,
                gu_ref, gd_ref, din_ref,
                u_s, dh_s, dz_s, w1_s, w2_s, xs, sc_s, da_s, p_s, rd2d, r1, rdir, r2, g_s, q1, q2,
                nrm, nsend, nrecv, clip_s, nz_s, clip_ref, mult_ref,
                ssem, rsem, gsem_s, gsem_r, nsem_s, nsem_r, usem, wsem, dsem, xsem, csem):
    n_layers, n_chunk, rows, hid = u_s.shape
    dim = dz_s.shape[-1]
    n_ex, _, seq = nrm.shape
    ex_per = n_ex // n_chunk
    piece = rows // 16
    n_item = n_layers * n_chunk
    dp, tp = lax.axis_index("dp"), lax.axis_index("tp")
    xi, core = tp // 2, tp % 2
    zi, yi = dp // RING, dp % RING

    def up(i, by=1):
        return (i + by) % RING

    x_l, x_r, x_o = up(xi, 3), up(xi, 1), up(xi, 2)
    partner = (dp, xi * 2 + 1 - core)
    dev_l, dev_r = (dp, x_l * 2 + core), (dp, x_r * 2 + core)
    dev_yl, dev_yr = (zi * RING + up(yi, 3), tp), (zi * RING + up(yi), tp)
    dev_zl, dev_zr = (up(zi, 3) * RING + yi, tp), (up(zi) * RING + yi, tp)

    def remote(src, dst, send, recv, dev):
        return pltpu.make_async_remote_copy(src_ref=src, dst_ref=dst, send_sem=send, recv_sem=recv,
                                            device_id=dev, device_id_type=MESH)

    def load_u(layer, c):
        return pltpu.make_async_copy(u_hbm.at[layer, c], u_s.at[layer, c], usem.at[layer, c])

    def load_w(which, layer):
        src, dst = ((w1_hbm, w1_s), (w2_hbm, w2_s))[which]
        return pltpu.make_async_copy(src.at[layer], dst.at[layer], wsem.at[which, layer])

    def load_d(c):
        return pltpu.make_async_copy(do_hbm.at[c], dz_s.at[0, c], dsem.at[c])

    def load_x(n):
        layer, c, slot = n_layers - 1 - n % n_item // n_chunk, n % n_chunk, n % 2
        return pltpu.make_async_copy(x_hbm.at[layer, c], xs.at[slot], xsem.at[slot])

    load_small = [pltpu.make_async_copy(src, dst, csem.at[i]) for i, (src, dst) in enumerate(
        ((clip_hbm, clip_ref), (mult_hbm, mult_ref), (nu_hbm, nz_s.at[0]), (nd_hbm, nz_s.at[1])))]
    top = n_layers - 1
    load_w(1, top).start()
    load_d(0).start()
    load_u(top, 0).start()

    def load_rest():
        load_w(0, top).start()
        load_x(0).start()
        load_x(1).start()
        for c in range(1, n_chunk):
            load_d(c).start()
            load_u(top, c).start()
        for layer in reversed(range(top)):
            load_w(1, layer).start()
            load_w(0, layer).start()
            for c in range(n_chunk):
                load_u(layer, c).start()
        for cp in load_small:
            cp.start()

    barrier = pltpu.get_barrier_semaphore()
    tp_peers = [(dp, (tp + 1 + r) % (2 * RING)) for r in range(2 * RING - 1)]
    peers = tp_peers + [dev_yl, dev_yr, dev_zl, dev_zr]
    for dev in peers:
        pl.semaphore_signal(barrier, inc=1, device_id=dev, device_id_type=MESH)

    def at(cc, xx, half=0, n=1):
        return pl.ds(pl.multiple_of(cc * (rows // 2) + xx * (rows // 8) + half * piece, 16), n * piece)

    def tp_copy(role, item):
        li, c, slot = item // n_chunk, item % n_chunk, item % n_chunk
        part, znew = p_s.at[slot], (din_ref.at[c] if li + 1 == n_layers else dz_s.at[li + 1, c])
        send, recv = ssem.at[int(role >= A1L), c], rsem.at[GROUP[role], c]
        if role == D2D:
            half = pl.ds(pl.multiple_of((1 - core) * (rows // 2), 16), rows // 2)
            return remote(part.at[half], rd2d.at[c], send, recv, partner)
        if role in (S1L, S1R):
            h = 0 if role == S1L else 1
            return remote(part.at[at(core, x_o, h)], r1.at[c, h], send, recv, (dev_l, dev_r)[h])
        if role == SDL:
            return remote(part.at[at(core, x_l, 1)], rdir.at[c, 0], send, recv, dev_l)
        if role == SDR:
            return remote(part.at[at(core, x_r, 0)], rdir.at[c, 1], send, recv, dev_r)
        if role == S2L:
            return remote(part.at[at(core, x_l, 0)], r2.at[c, 0], send, recv, dev_l)
        if role == S2R:
            return remote(part.at[at(core, x_r, 1)], r2.at[c, 1], send, recv, dev_r)
        where, dev = {
            A1L: (at(core, xi, 0, 2), dev_l),
            A1R: (at(core, xi, 0, 2), dev_r),
            A2L: (at(core, x_r, 0), dev_l),
            A2R: (at(core, x_l, 1), dev_r),
            FO: (at(core, xi, 0, 2), partner),
            FR: (at(core, x_r, 0, 2), partner),
            FL: (at(core, x_l, 0, 2), partner),
            FA: (at(core, x_o, 0), partner),
            FB: (at(core, x_o, 1), partner),
        }[role]
        return remote(znew.at[where], znew.at[where], send, recv, dev)

    def start(item, *roles):
        for role in roles:
            tp_copy(role, item).start()

    def pieces(item, n, send, recv):
        view = p_s.at[item % n_chunk, pl.ds(0, n * piece)]
        return remote(view, view, ssem.at[send, item % n_chunk], rsem.at[recv, item % n_chunk], partner)

    def arrived(item, group):
        pieces(item, GROUP_PIECES[group], 0, group).wait_recv()

    def sent(item, half):
        pieces(item, sum(GROUP_PIECES) // 2, half, 0).wait_send()

    @scoped
    def send_direct(item):
        start(item, SDL, SDR)

    @scoped
    def pair_sum(item):
        c, slot = item % n_chunk, item % n_chunk
        arrived(item, 0)
        base = core * (rows // 2)
        blk = rows // 8

        def add(b, _):
            mine = pl.ds(pl.multiple_of(base + b * blk, 16), blk)
            theirs = pl.ds(pl.multiple_of(b * blk, 16), blk)
            p_s[slot, mine, :] = (p_s[slot, mine, :].astype(F32) + rd2d[c, theirs, :].astype(F32)).astype(BF16)
            return 0

        lax.fori_loop(0, 4, add, 0)
        start(item, S1L, S1R)

    @scoped
    def relay_sum(item):
        c, slot = item % n_chunk, item % n_chunk
        arrived(item, 1)
        for h, go, xx in ((0, S2L, x_l), (1, S2R, x_r)):
            where = at(core, xx, h)
            p_s[slot, where, :] = (p_s[slot, where, :].astype(F32) + r1[c, h].astype(F32)).astype(BF16)
            start(item, go)

    @scoped
    def own_sum(item):
        li, c, slot = item // n_chunk, item % n_chunk, item % n_chunk
        arrived(item, 2)
        for h in range(2):
            where = at(core, xi, h)
            total = p_s[slot, where, :].astype(F32) + r2[c, h].astype(F32) + rdir[c, 1 - h].astype(F32)
            total = (dz_s[li, c, where, :].astype(F32) + total).astype(BF16)
            if li + 1 == n_layers:
                din_ref[c, where, :] = total
            else:
                dz_s[li + 1, c, where, :] = total
        start(item, A1L, A1R, FO)

    @scoped
    def gather_relay(item):
        arrived(item, 3)
        start(item, A2L, A2R, FR, FL)
        sent(item, 0)

    @scoped
    def gather_cross(item):
        arrived(item, 4)
        start(item, FA, FB)

    @scoped
    def gather_end(item):
        arrived(item, 5)
        sent(item, 1)

    @scoped
    def compute_dh(item):
        li, c = item // n_chunk, item % n_chunk
        layer = top - li

        if c == 0:
            load_w(1, layer).wait()
            if li > 0:
                load_w(0, layer).wait()
        if li == 0:
            load_d(c).wait()
        load_u(layer, c).wait()
        if item == 0:
            load_rest()
        da_s[...] = lax.dot_general(dz_s[li, c], w2_s[layer], NT, preferred_element_type=F32)
        blk = 32

        def act(b, _):
            r = pl.ds(pl.multiple_of(b * blk, blk), blk)
            u = u_s[layer, c, r, :].astype(F32)
            u2 = u * u
            th = jnp.tanh(K_TANH * (u + 0.044715 * (u2 * u)))
            cdf = 0.5 * (1.0 + th)
            slope = cdf + (0.5 * u) * (1.0 - th * th) * K_TANH * (1.0 + (3 * 0.044715) * u2)
            u_s[layer, c, r, :] = (u * cdf).astype(BF16)
            dh_s[layer, c, r, :] = (slope * da_s[r, :]).astype(BF16)
            return 0

        lax.fori_loop(0, rows // blk, act, 0)

    @scoped
    def compute_back(item):
        li, c, slot = item // n_chunk, item % n_chunk, item % n_chunk
        layer = top - li
        if item == 0:
            load_w(0, layer).wait()
            pl.semaphore_wait(barrier, len(peers))
        def part(n, _):
            cc = (core + 1 + n) % 2
            r = pl.ds(pl.multiple_of(cc * (rows // 2), 16), rows // 2)
            p_s[slot, r, :] = lax.dot_general(dh_s[layer, c, r, :], w1_s[layer], NT,
                                              preferred_element_type=F32).astype(BF16)

            @pl.when(n == 0)
            def _():
                start(item, D2D)

            return 0

        lax.fori_loop(0, 2, part, 0)

    @scoped
    def compute_norm(item):
        li, c = item // n_chunk, item % n_chunk
        layer = top - li
        load_x(item).wait()

        def one(e, _):
            r = pl.ds(pl.multiple_of(e * seq, 16), seq)

            def gram(v):
                return lax.dot_general(v, v, NT, preferred_element_type=F32)

            total = (gram(u_s[layer, c, r, :]) * gram(dz_s[li, c, r, :])
                     + gram(xs[item % 2, r, :]) * gram(dh_s[layer, c, r, :]))
            nrm[c * ex_per + e] += jnp.sum(total.reshape(seq // 8, 8, seq), axis=0)
            return 0

        lax.fori_loop(0, ex_per, one, 0)
        load_x(item + 2).start()
        if li == top:
            norm_start(c)

    def norm_copies(c):
        return [remote(nsend.at[c], nrecv.at[c, r], nsem_s.at[c], nsem_r.at[c], dev)
                for r, dev in enumerate(tp_peers)]

    @scoped
    def norm_start(c):
        part = jnp.sum(nrm[pl.ds(c * ex_per, ex_per)], axis=1)
        part = jnp.broadcast_to(jnp.sum(part, axis=-1, keepdims=True), (ex_per, nsend.shape[-1]))
        nsend[c] = jnp.concatenate([part] * (nsend.shape[1] // ex_per), axis=0)
        for cp in norm_copies(c):
            cp.start()

    @scoped
    def clip_factors(c):
        if c == 0:
            for cp in load_small:
                cp.wait()
        every = remote(nrecv.at[c], nrecv.at[c], nsem_s.at[c], nsem_r.at[c], partner)
        every.wait_recv()
        total = nsend[c]
        for r in range(len(tp_peers)):
            total = total + nrecv[c, r]
        factor = jnp.minimum(1.0, clip_ref[0] / jnp.sqrt(total))
        for e in range(ex_per):
            clip_s[c * ex_per + e] = jnp.broadcast_to(factor[e:e + 1, :], clip_s.shape[1:])
        every.wait_send()

    def grad_view(k, kind, phase, j, h):
        if phase == 0:
            n = RING // 2
            if kind == 0:
                return g_s.at[k, pl.ds(h * n, n), j]
            return g_s.at[k, j, pl.ds(h * n, n)]
        n = g_s.shape[3] // 2
        if kind == 0:
            return g_s.at[k, j, yi, pl.ds(h * n, n)]
        return g_s.at[k, zi, j, pl.ds(h * n, n)]

    def ring_of(kind, phase):
        if (kind == 0) == (phase == 0):
            return yi, dev_yl, dev_yr
        return zi, dev_zl, dev_zr

    def grad_copy(k, kind, phase, role):
        me, d_l, d_r = ring_of(kind, phase)
        buf = (q1, q2)[phase]
        j, h = ((up(me, 2), 0), (up(me, 2), 1), (up(me, 3), 1), (up(me, 1), 0), (up(me, 3), 0), (up(me, 1), 1))[role]
        return remote(grad_view(k, kind, phase, j, h), buf.at[k, role], gsem_s.at[phase],
                      gsem_r.at[phase, int(role >= 2), k], d_r if role % 2 else d_l)

    @scoped
    def ring_start(p, kind, phase):
        k = 2 * p + kind
        for role in range(4):
            grad_copy(k, kind, phase, role).start()

    def ring_arrived(k, phase, lo, n):
        view = (q1, q2)[phase].at[k, pl.ds(lo, n)]
        remote(view, view, gsem_s.at[phase], gsem_r.at[phase, int(lo > 0), k], partner).wait_recv()

    @scoped
    def ring_relay(p, kind, phase):
        k = 2 * p + kind
        me, _, _ = ring_of(kind, phase)
        buf = (q1, q2)[phase]
        ring_arrived(k, phase, 0, 2)
        for h in range(2):
            view = grad_view(k, kind, phase, up(me, 1 if h else 3), h)
            view[...] = view[...] + buf[k, h]
            grad_copy(k, kind, phase, 4 + h).start()

    @scoped
    def ring_end(p, kind, phase):
        k = 2 * p + kind
        me, _, _ = ring_of(kind, phase)
        buf = (q1, q2)[phase]
        ring_arrived(k, phase, 2, 4)
        for h in range(2):
            view = grad_view(k, kind, phase, me, h)
            view[...] = view[...] + buf[k, 3 - h] + buf[k, 4 + h]

    @scoped
    def ring_turn(p, kind):
        ring_end(p, kind, 0)
        ring_start(p, kind, 1)

    @scoped
    def ring_last(p, kind):
        ring_end(p, kind, 1)
        finish(p, kind)

    @scoped
    def ring_sent():
        for phase, buf in enumerate((q1, q2)):
            remote(buf, buf, gsem_s.at[phase], gsem_r.at[phase, 0, 0], partner).wait_send()

    inv = 1.0 / (n_ex * RING * RING)

    @scoped
    def finish(p, kind):
        layer, scale = top - p, mult_ref[0] * clip_ref[0]
        (gu_ref, gd_ref)[kind][layer] = (g_s[2 * p + kind, zi, yi] + scale * nz_s[kind, layer]) * inv

    @scoped
    def weight_grad(p, kind, c):
        k, layer, n = 2 * p + kind, top - p, p * n_chunk + c

        def scaled(e, _):
            r = pl.ds(pl.multiple_of(e * seq, 16), seq)
            f = clip_s[c * ex_per + e][0:1, 0:1]
            if kind == 0:
                dh_s[layer, c, r, :] = (dh_s[layer, c, r, :].astype(F32) * f).astype(BF16)
            else:
                sc_s[r, :] = (dz_s[p, c, r, :].astype(F32) * f).astype(BF16)
            return 0

        lax.fori_loop(0, ex_per, scaled, 0)
        if kind == 0:
            load_x(n_item + n).wait()
            add = lax.dot_general(xs[n % 2], dh_s[layer, c], TN, preferred_element_type=F32)
        else:
            add = lax.dot_general(sc_s[...], u_s[layer, c], TN, preferred_element_type=F32)
        add = add.reshape(g_s.shape[1:])
        if c == 0:
            g_s[k] = add
        else:
            g_s[k] += add
        if kind == 0 and n + 2 < n_item:
            load_x(n_item + n + 2).start()

    def each(stage):
        return [functools.partial(stage, i) for i in range(n_item)]

    def ring(stage, kind, *phase):
        return [functools.partial(stage, p, kind, *phase) for p in range(n_layers)]

    def units(kind):
        return [functools.partial(weight_grad, p, kind, c) for p in range(n_layers) for c in range(n_chunk)]

    dh0, dh1, dh2, dh3, dh4, dh5, dh6, dh7, dh8, dh9, dh10, dh11 = each(compute_dh)
    back0, back1, back2, back3, back4, back5, back6, back7, back8, back9, back10, back11 = each(compute_back)
    norm0, norm1, norm2, norm3, norm4, norm5, norm6, norm7, norm8, norm9, norm10, norm11 = each(compute_norm)
    pair0, pair1, pair2, pair3, pair4, pair5, pair6, pair7, pair8, pair9, pair10, pair11 = each(pair_sum)
    sd0, sd1, sd2, sd3, sd4, sd5, sd6, sd7, sd8, sd9, sd10, sd11 = each(send_direct)
    (
        relay0, relay1, relay2, relay3, relay4, relay5, relay6, relay7, relay8, relay9, relay10, relay11,
    ) = each(relay_sum)
    own0, own1, own2, own3, own4, own5, own6, own7, own8, own9, own10, own11 = each(own_sum)
    gr0, gr1, gr2, gr3, gr4, gr5, gr6, gr7, gr8, gr9, gr10, gr11 = each(gather_relay)
    (
        cross0, cross1, cross2, cross3, cross4, cross5, cross6, cross7, cross8, cross9, cross10, cross11,
    ) = each(gather_cross)
    end0, end1, end2, end3, end4, end5, end6, end7, end8, end9, end10, end11 = each(gather_end)
    clip0, clip1, clip2, clip3 = [functools.partial(clip_factors, c) for c in range(n_chunk)]
    uA0c0, uA0c1, uA0c2, uA0c3, uA1c0, uA1c1, uA1c2, uA1c3, uA2c0, uA2c1, uA2c2, uA2c3 = units(0)
    stA0, stA1, stA2 = ring(ring_start, 0, 0)
    rlA0, rlA1, rlA2 = ring(ring_relay, 0, 0)
    enA0, enA1, enA2 = ring(ring_turn, 0)
    r2A0, r2A1, r2A2 = ring(ring_relay, 0, 1)
    e2A0, e2A1, e2A2 = ring(ring_last, 0)
    uB0c0, uB0c1, uB0c2, uB0c3, uB1c0, uB1c1, uB1c2, uB1c3, uB2c0, uB2c1, uB2c2, uB2c3 = units(1)
    stB0, stB1, stB2 = ring(ring_start, 1, 0)
    rlB0, rlB1, rlB2 = ring(ring_relay, 1, 0)
    enB0, enB1, enB2 = ring(ring_turn, 1)
    r2B0, r2B1, r2B2 = ring(ring_relay, 1, 1)
    e2B0, e2B1, e2B2 = ring(ring_last, 1)

    nrm[...] = jnp.zeros_like(nrm)
    dh0()
    back0()
    dh1()
    pair0()
    back1()
    sd0()
    pair1()
    sd1()
    dh2()
    back2()
    relay0()
    relay1()
    dh3()
    pair2()
    sd2()
    back3()
    own0()
    norm0()
    own1()
    norm1()
    gr0()
    relay2()
    pair3()
    gr1()
    cross0()
    norm2()
    end0()
    own2()
    dh4()
    sd3()
    cross1()
    relay3()
    norm3()
    end1()
    back4()
    gr2()
    pair4()
    sd4()
    dh5()
    back5()
    own3()
    cross2()
    norm4()
    relay4()
    end2()
    pair5()
    sd5()
    norm5()
    gr3()
    dh6()
    relay5()
    own4()
    back6()
    cross3()
    own5()
    end3()
    dh7()
    gr4()
    pair6()
    norm6()
    back7()
    gr5()
    pair7()
    cross4()
    norm7()
    relay6()
    end4()
    sd6()
    sd7()
    dh8()
    cross5()
    norm8()
    relay7()
    end5()
    dh9()
    own6()
    norm9()
    back9()
    own7()
    clip0()
    uB1c0()
    uB2c0()
    uB0c0()
    gr6()
    clip1()
    pair9()
    back8()
    uB0c1()
    gr7()
    uB2c1()
    pair8()
    sd8()
    cross6()
    uB1c1()
    sd9()
    end6()
    dh10()
    cross7()
    norm10()
    end7()
    dh11()
    norm11()
    uA0c0()
    clip2()
    uA0c1()
    uB0c2()
    clip3()
    uA0c2()
    uB0c3()
    stB0()
    uA0c3()
    stA0()
    relay9()
    relay8()
    uA1c0()
    back10()
    uB1c2()
    pair10()
    uB1c3()
    rlB0()
    own9()
    sd10()
    rlA0()
    uA1c1()
    stB1()
    uA1c2()
    uA1c3()
    stA1()
    own8()
    uB2c2()
    back11()
    uA2c0()
    uB2c3()
    stB2()
    gr9()
    pair11()
    relay10()
    uA2c1()
    rlA1()
    uA2c2()
    uA2c3()
    stA2()
    gr8()
    relay11()
    cross9()
    sd11()
    rlB2()
    end9()
    rlB1()
    own10()
    rlA2()
    cross8()
    enA1()
    own11()
    end8()
    enB2()
    enA0()
    enB0()
    gr10()
    enA2()
    enB1()
    gr11()
    r2A1()
    r2B2()
    r2A0()
    r2B0()
    cross10()
    r2A2()
    r2B1()
    cross11()
    end10()
    end11()
    e2A2()
    e2B2()
    e2A1()
    e2A0()
    e2B0()
    e2B1()
    ring_sent()


def solution(mesh):
    n_dp, n_tp = mesh.shape["dp"], mesh.shape["tp"]

    def local(x_in, u_pre, w_up, w_down, d_out, noise_up, noise_down, clip_norm, noise_mult):
        n_layers, micro, batch, seq, dim = x_in.shape
        hid = u_pre.shape[-1]
        n_ex = micro * batch
        rows = n_ex * seq // N_CHUNK
        piece, grad_rows = rows // 16, dim // n_dp
        x4 = x_in.reshape(n_layers, N_CHUNK, rows, dim)
        u4 = u_pre.reshape(n_layers, N_CHUNK, rows, hid)
        d4 = d_out.reshape(N_CHUNK, rows, dim)
        anyspace = pl.BlockSpec(memory_space=pl.ANY)
        vmem = pl.BlockSpec(memory_space=pltpu.VMEM)
        dma = pltpu.SemaphoreType.DMA
        tokens = n_ex * seq
        flops = 2 * n_layers * tokens * hid * dim * 4 + 4 * n_layers * tokens * seq * (hid + dim)
        g_up, g_down, d_in = pl.pallas_call(
            step_kernel,
            out_shape=(
                pltpu.VMEM((n_layers, grad_rows, hid), F32),
                pltpu.VMEM((n_layers, grad_rows, hid), F32),
                pltpu.VMEM((N_CHUNK, rows, dim), BF16),
            ),
            in_specs=[anyspace] * 9,
            out_specs=(vmem, vmem, vmem),
            scratch_shapes=[
                pltpu.VMEM((n_layers, N_CHUNK, rows, hid), BF16),
                pltpu.VMEM((n_layers, N_CHUNK, rows, hid), BF16),
                pltpu.VMEM((n_layers, N_CHUNK, rows, dim), BF16),
                pltpu.VMEM((n_layers, dim, hid), BF16),
                pltpu.VMEM((n_layers, hid, dim), BF16),
                pltpu.VMEM((2, rows, dim), BF16),
                pltpu.VMEM((rows, dim), BF16),
                pltpu.VMEM((rows, hid), F32),
                pltpu.VMEM((N_CHUNK, rows, dim), BF16),
                pltpu.VMEM((N_CHUNK, rows // 2, dim), BF16),
                pltpu.VMEM((N_CHUNK, 2, piece, dim), BF16),
                pltpu.VMEM((N_CHUNK, 2, piece, dim), BF16),
                pltpu.VMEM((N_CHUNK, 2, piece, dim), BF16),
                pltpu.VMEM((2 * n_layers, RING, RING, grad_rows, hid), F32),
                pltpu.VMEM((2 * n_layers, 6, RING // 2, grad_rows, hid), F32),
                pltpu.VMEM((2 * n_layers, 6, grad_rows // 2, hid), F32),
                pltpu.VMEM((n_ex, 8, seq), F32),
                pltpu.VMEM((N_CHUNK, 8, 128), F32),
                pltpu.VMEM((N_CHUNK, 2 * RING - 1, 8, 128), F32),
                pltpu.VMEM((n_ex, 8, 128), F32),
                pltpu.VMEM((2, n_layers, grad_rows, hid), F32),
                pltpu.SMEM((1,), F32),
                pltpu.SMEM((1,), F32),
                dma((2, N_CHUNK)),
                dma((len(GROUP_PIECES), N_CHUNK)),
                dma((2,)),
                dma((2, 2, 2 * n_layers)),
                dma((N_CHUNK,)),
                dma((N_CHUNK,)),
                dma((n_layers, N_CHUNK)),
                dma((2, n_layers)),
                dma((N_CHUNK,)),
                dma((2,)),
                dma((4,)),
            ],
            compiler_params=pltpu.CompilerParams(
                collective_id=0, has_side_effects=True, vmem_limit_bytes=61_700_000
            ),
            cost_estimate=pl.CostEstimate(flops=flops, bytes_accessed=50_000_000, transcendentals=n_layers * tokens * hid),
            name="clipped_step",
        )(x4, u4, w_up, w_down, d4, noise_up, jnp.transpose(noise_down, (0, 2, 1)), clip_norm, noise_mult)
        return g_up, jnp.transpose(g_down, (0, 2, 1)), d_in.reshape(d_out.shape)

    in_specs = (P(None, None, "dp", None, None), P(None, None, "dp", None, "tp"), P(None, None, "tp"),
                P(None, "tp", None), P(None, "dp", None, None), P(None, "dp", "tp"), P(None, "tp", "dp"), P(), P())
    out_specs = (P(None, "dp", "tp"), P(None, "tp", "dp"), P(None, "dp", None, None))
    return jax.shard_map(local, mesh=mesh, in_specs=in_specs, out_specs=out_specs, check_vma=False)
```

```python
import functools
import math

import jax
import jax.numpy as jnp
from jax import lax
from jax.experimental import pallas as pl
from jax.experimental.pallas import tpu as pltpu
from jax.sharding import PartitionSpec as P

MESH = pl.DeviceIdType.MESH
F32, BF16 = jnp.float32, jnp.bfloat16
N_CHUNK = 4
RING = 4
K_TANH = math.sqrt(2.0 / math.pi)
(D2D, S1L, S1R, SDL, SDR, S2L, S2R, A1L, A1R, A2L, A2R, FO, FR, FL, FA, FB) = range(16)
GROUP = [0, 1, 1, 2, 2, 2, 2, 3, 3, 4, 4, 5, 5, 5, 5, 5]
GROUP_PIECES = [8, 2, 4, 4, 2, 8]
NT = (((1,), (1,)), ((), ()))
TN = (((0,), (0,)), ((), ()))


def scoped(f):
    def g(*a):
        with jax.named_scope(f.__name__):
            return f(*a)
    return g


def step_kernel(x_hbm, u_hbm, w1_hbm, w2_hbm, do_hbm, nu_hbm, nd_hbm, clip_hbm, mult_hbm,
                gu_ref, gd_ref, din_ref,
                u_s, dh_s, dz_s, w1_s, w2_s, xs, sc_s, da_s, p_s, rd2d, r1, rdir, r2, g_s, q1, q2,
                nrm, nsend, nrecv, clip_s, nz_s, clip_ref, mult_ref,
                ssem, rsem, gsem_s, gsem_r, nsem_s, nsem_r, usem, wsem, dsem, xsem, csem):
    n_layers, n_chunk, rows, hid = u_s.shape
    dim = dz_s.shape[-1]
    n_ex, _, seq = nrm.shape
    ex_per = n_ex // n_chunk
    piece = rows // 16
    n_item = n_layers * n_chunk
    dp, tp = lax.axis_index("dp"), lax.axis_index("tp")
    xi, core = tp // 2, tp % 2
    zi, yi = dp // RING, dp % RING

    def up(i, by=1):
        return (i + by) % RING

    x_l, x_r, x_o = up(xi, 3), up(xi, 1), up(xi, 2)
    partner = (dp, xi * 2 + 1 - core)
    dev_l, dev_r = (dp, x_l * 2 + core), (dp, x_r * 2 + core)
    dev_yl, dev_yr = (zi * RING + up(yi, 3), tp), (zi * RING + up(yi), tp)
    dev_zl, dev_zr = (up(zi, 3) * RING + yi, tp), (up(zi) * RING + yi, tp)

    def remote(src, dst, send, recv, dev):
        return pltpu.make_async_remote_copy(src_ref=src, dst_ref=dst, send_sem=send, recv_sem=recv,
                                            device_id=dev, device_id_type=MESH)

    def load_u(layer, c):
        return pltpu.make_async_copy(u_hbm.at[layer, c], u_s.at[layer, c], usem.at[layer, c])

    def load_w(which, layer):
        src, dst = ((w1_hbm, w1_s), (w2_hbm, w2_s))[which]
        return pltpu.make_async_copy(src.at[layer], dst.at[layer], wsem.at[which, layer])

    def load_d(c):
        return pltpu.make_async_copy(do_hbm.at[c], dz_s.at[0, c], dsem.at[c])

    def load_x(n):
        layer, c, slot = n_layers - 1 - n % n_item // n_chunk, n % n_chunk, n % 2
        return pltpu.make_async_copy(x_hbm.at[layer, c], xs.at[slot], xsem.at[slot])

    load_small = [pltpu.make_async_copy(src, dst, csem.at[i]) for i, (src, dst) in enumerate(
        ((clip_hbm, clip_ref), (mult_hbm, mult_ref), (nu_hbm, nz_s.at[0]), (nd_hbm, nz_s.at[1])))]
    top = n_layers - 1
    load_w(1, top).start()
    load_d(0).start()
    load_u(top, 0).start()

    def load_rest():
        load_w(0, top).start()
        load_x(0).start()
        load_x(1).start()
        for c in range(1, n_chunk):
            load_d(c).start()
            load_u(top, c).start()
        for layer in reversed(range(top)):
            load_w(1, layer).start()
            load_w(0, layer).start()
            for c in range(n_chunk):
                load_u(layer, c).start()
        for cp in load_small:
            cp.start()

    barrier = pltpu.get_barrier_semaphore()
    tp_peers = [(dp, (tp + 1 + r) % (2 * RING)) for r in range(2 * RING - 1)]
    peers = tp_peers + [dev_yl, dev_yr, dev_zl, dev_zr]
    for dev in peers:
        pl.semaphore_signal(barrier, inc=1, device_id=dev, device_id_type=MESH)

    def at(cc, xx, half=0, n=1):
        return pl.ds(pl.multiple_of(cc * (rows // 2) + xx * (rows // 8) + half * piece, 16), n * piece)

    def tp_copy(role, item):
        li, c, slot = item // n_chunk, item % n_chunk, item % n_chunk
        part, znew = p_s.at[slot], (din_ref.at[c] if li + 1 == n_layers else dz_s.at[li + 1, c])
        send, recv = ssem.at[int(role >= A1L), c], rsem.at[GROUP[role], c]
        if role == D2D:
            half = pl.ds(pl.multiple_of((1 - core) * (rows // 2), 16), rows // 2)
            return remote(part.at[half], rd2d.at[c], send, recv, partner)
        if role in (S1L, S1R):
            h = 0 if role == S1L else 1
            return remote(part.at[at(core, x_o, h)], r1.at[c, h], send, recv, (dev_l, dev_r)[h])
        if role == SDL:
            return remote(part.at[at(core, x_l, 1)], rdir.at[c, 0], send, recv, dev_l)
        if role == SDR:
            return remote(part.at[at(core, x_r, 0)], rdir.at[c, 1], send, recv, dev_r)
        if role == S2L:
            return remote(part.at[at(core, x_l, 0)], r2.at[c, 0], send, recv, dev_l)
        if role == S2R:
            return remote(part.at[at(core, x_r, 1)], r2.at[c, 1], send, recv, dev_r)
        where, dev = {
            A1L: (at(core, xi, 0, 2), dev_l),
            A1R: (at(core, xi, 0, 2), dev_r),
            A2L: (at(core, x_r, 0), dev_l),
            A2R: (at(core, x_l, 1), dev_r),
            FO: (at(core, xi, 0, 2), partner),
            FR: (at(core, x_r, 0, 2), partner),
            FL: (at(core, x_l, 0, 2), partner),
            FA: (at(core, x_o, 0), partner),
            FB: (at(core, x_o, 1), partner),
        }[role]
        return remote(znew.at[where], znew.at[where], send, recv, dev)

    def start(item, *roles):
        for role in roles:
            tp_copy(role, item).start()

    def pieces(item, n, send, recv):
        view = p_s.at[item % n_chunk, pl.ds(0, n * piece)]
        return remote(view, view, ssem.at[send, item % n_chunk], rsem.at[recv, item % n_chunk], partner)

    def arrived(item, group):
        pieces(item, GROUP_PIECES[group], 0, group).wait_recv()

    def sent(item, half):
        pieces(item, sum(GROUP_PIECES) // 2, half, 0).wait_send()

    @scoped
    def send_direct(item):
        start(item, SDL, SDR)

    @scoped
    def pair_sum(item):
        c, slot = item % n_chunk, item % n_chunk
        arrived(item, 0)
        base = core * (rows // 2)
        blk = rows // 8

        def add(b, _):
            mine = pl.ds(pl.multiple_of(base + b * blk, 16), blk)
            theirs = pl.ds(pl.multiple_of(b * blk, 16), blk)
            p_s[slot, mine, :] = (p_s[slot, mine, :].astype(F32) + rd2d[c, theirs, :].astype(F32)).astype(BF16)
            return 0

        lax.fori_loop(0, 4, add, 0)
        start(item, S1L, S1R)

    @scoped
    def relay_sum(item):
        c, slot = item % n_chunk, item % n_chunk
        arrived(item, 1)
        for h, go, xx in ((0, S2L, x_l), (1, S2R, x_r)):
            where = at(core, xx, h)
            p_s[slot, where, :] = (p_s[slot, where, :].astype(F32) + r1[c, h].astype(F32)).astype(BF16)
            start(item, go)

    @scoped
    def own_sum(item):
        li, c, slot = item // n_chunk, item % n_chunk, item % n_chunk
        arrived(item, 2)
        for h in range(2):
            where = at(core, xi, h)
            total = p_s[slot, where, :].astype(F32) + r2[c, h].astype(F32) + rdir[c, 1 - h].astype(F32)
            total = (dz_s[li, c, where, :].astype(F32) + total).astype(BF16)
            if li + 1 == n_layers:
                din_ref[c, where, :] = total
            else:
                dz_s[li + 1, c, where, :] = total
        start(item, A1L, A1R, FO)

    @scoped
    def gather_relay(item):
        arrived(item, 3)
        start(item, A2L, A2R, FR, FL)
        sent(item, 0)

    @scoped
    def gather_cross(item):
        arrived(item, 4)
        start(item, FA, FB)

    @scoped
    def gather_end(item):
        arrived(item, 5)
        sent(item, 1)

    @scoped
    def compute_dh(item):
        li, c = item // n_chunk, item % n_chunk
        layer = top - li

        if c == 0:
            load_w(1, layer).wait()
            if li > 0:
                load_w(0, layer).wait()
        if li == 0:
            load_d(c).wait()
        load_u(layer, c).wait()
        if item == 0:
            load_rest()
        da_s[...] = lax.dot_general(dz_s[li, c], w2_s[layer], NT, preferred_element_type=F32)
        blk = 32

        def act(b, _):
            r = pl.ds(pl.multiple_of(b * blk, blk), blk)
            u = u_s[layer, c, r, :].astype(F32)
            u2 = u * u
            th = jnp.tanh(K_TANH * (u + 0.044715 * (u2 * u)))
            cdf = 0.5 * (1.0 + th)
            slope = cdf + (0.5 * u) * (1.0 - th * th) * K_TANH * (1.0 + (3 * 0.044715) * u2)
            u_s[layer, c, r, :] = (u * cdf).astype(BF16)
            dh_s[layer, c, r, :] = (slope * da_s[r, :]).astype(BF16)
            return 0

        lax.fori_loop(0, rows // blk, act, 0)

    @scoped
    def compute_back(item):
        li, c, slot = item // n_chunk, item % n_chunk, item % n_chunk
        layer = top - li
        if item == 0:
            load_w(0, layer).wait()
        def part(n, _):
            cc = (core + 1 + n) % 2
            r = pl.ds(pl.multiple_of(cc * (rows // 2), 16), rows // 2)
            p_s[slot, r, :] = lax.dot_general(dh_s[layer, c, r, :], w1_s[layer], NT,
                                              preferred_element_type=F32).astype(BF16)

            @pl.when(n == 0)
            def _():
                if item == 0:
                    pl.semaphore_wait(barrier, len(peers))
                start(item, D2D)

            return 0

        lax.fori_loop(0, 2, part, 0)

    @scoped
    def compute_norm(item):
        li, c = item // n_chunk, item % n_chunk
        layer = top - li
        load_x(item).wait()

        def one(e, _):
            r = pl.ds(pl.multiple_of(e * seq, 16), seq)

            def gram(v):
                return lax.dot_general(v, v, NT, preferred_element_type=F32)

            total = (gram(u_s[layer, c, r, :]) * gram(dz_s[li, c, r, :])
                     + gram(xs[item % 2, r, :]) * gram(dh_s[layer, c, r, :]))
            nrm[c * ex_per + e] += jnp.sum(total.reshape(seq // 8, 8, seq), axis=0)
            return 0

        lax.fori_loop(0, ex_per, one, 0)
        load_x(item + 2).start()
        if li == top:
            norm_start(c)

    def norm_copies(c):
        return [remote(nsend.at[c], nrecv.at[c, r], nsem_s.at[c], nsem_r.at[c], dev)
                for r, dev in enumerate(tp_peers)]

    @scoped
    def norm_start(c):
        part = jnp.sum(nrm[pl.ds(c * ex_per, ex_per)], axis=1)
        part = jnp.broadcast_to(jnp.sum(part, axis=-1, keepdims=True), (ex_per, nsend.shape[-1]))
        nsend[c] = jnp.concatenate([part] * (nsend.shape[1] // ex_per), axis=0)
        for cp in norm_copies(c):
            cp.start()

    @scoped
    def clip_factors(c):
        if c == 0:
            for cp in load_small:
                cp.wait()
        every = remote(nrecv.at[c], nrecv.at[c], nsem_s.at[c], nsem_r.at[c], partner)
        every.wait_recv()
        total = nsend[c]
        for r in range(len(tp_peers)):
            total = total + nrecv[c, r]
        factor = jnp.minimum(1.0, clip_ref[0] / jnp.sqrt(total))
        for e in range(ex_per):
            clip_s[c * ex_per + e] = jnp.broadcast_to(factor[e:e + 1, :], clip_s.shape[1:])
        every.wait_send()

    def grad_view(k, kind, phase, j, h):
        if phase == 0:
            n = RING // 2
            if kind == 0:
                return g_s.at[k, pl.ds(h * n, n), j]
            return g_s.at[k, j, pl.ds(h * n, n)]
        n = g_s.shape[3] // 2
        if kind == 0:
            return g_s.at[k, j, yi, pl.ds(h * n, n)]
        return g_s.at[k, zi, j, pl.ds(h * n, n)]

    def ring_of(kind, phase):
        if (kind == 0) == (phase == 0):
            return yi, dev_yl, dev_yr
        return zi, dev_zl, dev_zr

    def grad_copy(k, kind, phase, role):
        me, d_l, d_r = ring_of(kind, phase)
        buf = (q1, q2)[phase]
        j, h = ((up(me, 2), 0), (up(me, 2), 1), (up(me, 3), 1), (up(me, 1), 0), (up(me, 3), 0), (up(me, 1), 1))[role]
        return remote(grad_view(k, kind, phase, j, h), buf.at[k, role], gsem_s.at[phase],
                      gsem_r.at[phase, int(role >= 2), k], d_r if role % 2 else d_l)

    @scoped
    def ring_start(p, kind, phase):
        k = 2 * p + kind
        for role in range(4):
            grad_copy(k, kind, phase, role).start()

    def ring_arrived(k, phase, lo, n):
        view = (q1, q2)[phase].at[k, pl.ds(lo, n)]
        remote(view, view, gsem_s.at[phase], gsem_r.at[phase, int(lo > 0), k], partner).wait_recv()

    @scoped
    def ring_relay(p, kind, phase):
        k = 2 * p + kind
        me, _, _ = ring_of(kind, phase)
        buf = (q1, q2)[phase]
        ring_arrived(k, phase, 0, 2)
        for h in range(2):
            view = grad_view(k, kind, phase, up(me, 1 if h else 3), h)
            view[...] = view[...] + buf[k, h]
            grad_copy(k, kind, phase, 4 + h).start()

    @scoped
    def ring_end(p, kind, phase):
        k = 2 * p + kind
        me, _, _ = ring_of(kind, phase)
        buf = (q1, q2)[phase]
        ring_arrived(k, phase, 2, 4)
        for h in range(2):
            view = grad_view(k, kind, phase, me, h)
            view[...] = view[...] + buf[k, 3 - h] + buf[k, 4 + h]

    @scoped
    def ring_turn(p, kind):
        ring_end(p, kind, 0)
        ring_start(p, kind, 1)

    @scoped
    def ring_last(p, kind):
        ring_end(p, kind, 1)
        finish(p, kind)

    @scoped
    def ring_sent():
        for phase, buf in enumerate((q1, q2)):
            remote(buf, buf, gsem_s.at[phase], gsem_r.at[phase, 0, 0], partner).wait_send()

    inv = 1.0 / (n_ex * RING * RING)

    @scoped
    def finish(p, kind):
        layer, scale = top - p, mult_ref[0] * clip_ref[0]
        (gu_ref, gd_ref)[kind][layer] = (g_s[2 * p + kind, zi, yi] + scale * nz_s[kind, layer]) * inv

    @scoped
    def weight_grad(p, kind, c):
        k, layer, n = 2 * p + kind, top - p, p * n_chunk + c

        def scaled(e, _):
            r = pl.ds(pl.multiple_of(e * seq, 16), seq)
            f = clip_s[c * ex_per + e][0:1, 0:1]
            if kind == 0:
                dh_s[layer, c, r, :] = (dh_s[layer, c, r, :].astype(F32) * f).astype(BF16)
            else:
                sc_s[r, :] = (dz_s[p, c, r, :].astype(F32) * f).astype(BF16)
            return 0

        lax.fori_loop(0, ex_per, scaled, 0)
        if kind == 0:
            load_x(n_item + n).wait()
            add = lax.dot_general(xs[n % 2], dh_s[layer, c], TN, preferred_element_type=F32)
        else:
            add = lax.dot_general(sc_s[...], u_s[layer, c], TN, preferred_element_type=F32)
        add = add.reshape(g_s.shape[1:])
        if c == 0:
            g_s[k] = add
        else:
            g_s[k] += add
        if kind == 0 and n + 2 < n_item:
            load_x(n_item + n + 2).start()

    def each(stage):
        return [functools.partial(stage, i) for i in range(n_item)]

    def ring(stage, kind, *phase):
        return [functools.partial(stage, p, kind, *phase) for p in range(n_layers)]

    def units(kind):
        return [functools.partial(weight_grad, p, kind, c) for p in range(n_layers) for c in range(n_chunk)]

    dh0, dh1, dh2, dh3, dh4, dh5, dh6, dh7, dh8, dh9, dh10, dh11 = each(compute_dh)
    back0, back1, back2, back3, back4, back5, back6, back7, back8, back9, back10, back11 = each(compute_back)
    norm0, norm1, norm2, norm3, norm4, norm5, norm6, norm7, norm8, norm9, norm10, norm11 = each(compute_norm)
    pair0, pair1, pair2, pair3, pair4, pair5, pair6, pair7, pair8, pair9, pair10, pair11 = each(pair_sum)
    sd0, sd1, sd2, sd3, sd4, sd5, sd6, sd7, sd8, sd9, sd10, sd11 = each(send_direct)
    (
        relay0, relay1, relay2, relay3, relay4, relay5, relay6, relay7, relay8, relay9, relay10, relay11,
    ) = each(relay_sum)
    own0, own1, own2, own3, own4, own5, own6, own7, own8, own9, own10, own11 = each(own_sum)
    gr0, gr1, gr2, gr3, gr4, gr5, gr6, gr7, gr8, gr9, gr10, gr11 = each(gather_relay)
    (
        cross0, cross1, cross2, cross3, cross4, cross5, cross6, cross7, cross8, cross9, cross10, cross11,
    ) = each(gather_cross)
    end0, end1, end2, end3, end4, end5, end6, end7, end8, end9, end10, end11 = each(gather_end)
    clip0, clip1, clip2, clip3 = [functools.partial(clip_factors, c) for c in range(n_chunk)]
    uA0c0, uA0c1, uA0c2, uA0c3, uA1c0, uA1c1, uA1c2, uA1c3, uA2c0, uA2c1, uA2c2, uA2c3 = units(0)
    stA0, stA1, stA2 = ring(ring_start, 0, 0)
    rlA0, rlA1, rlA2 = ring(ring_relay, 0, 0)
    enA0, enA1, enA2 = ring(ring_turn, 0)
    r2A0, r2A1, r2A2 = ring(ring_relay, 0, 1)
    e2A0, e2A1, e2A2 = ring(ring_last, 0)
    uB0c0, uB0c1, uB0c2, uB0c3, uB1c0, uB1c1, uB1c2, uB1c3, uB2c0, uB2c1, uB2c2, uB2c3 = units(1)
    stB0, stB1, stB2 = ring(ring_start, 1, 0)
    rlB0, rlB1, rlB2 = ring(ring_relay, 1, 0)
    enB0, enB1, enB2 = ring(ring_turn, 1)
    r2B0, r2B1, r2B2 = ring(ring_relay, 1, 1)
    e2B0, e2B1, e2B2 = ring(ring_last, 1)

    nrm[...] = jnp.zeros_like(nrm)
    dh0()
    back0()
    dh1()
    pair0()
    back1()
    sd0()
    dh2()
    pair1()
    sd1()
    back2()
    dh3()
    relay0()
    pair2()
    norm0()
    sd2()
    relay1()
    norm1()
    back3()
    own0()
    norm2()
    pair3()
    norm3()
    own1()
    gr0()
    relay2()
    relay3()
    sd3()
    gr1()
    cross0()
    own2()
    end0()
    dh4()
    back4()
    own3()
    cross1()
    pair4()
    sd4()
    end1()
    dh5()
    back5()
    gr2()
    pair5()
    norm4()
    relay4()
    gr3()
    sd5()
    norm5()
    cross2()
    end2()
    relay5()
    dh6()
    own4()
    back6()
    norm6()
    pair6()
    cross3()
    own5()
    end3()
    dh7()
    gr4()
    sd6()
    back7()
    pair7()
    gr5()
    cross4()
    relay6()
    sd7()
    norm7()
    end4()
    dh8()
    relay7()
    norm8()
    cross5()
    own6()
    back8()
    end5()
    dh9()
    own7()
    back9()
    norm9()
    clip0()
    gr6()
    pair9()
    uB2c0()
    uB1c0()
    uB0c0()
    gr7()
    clip1()
    sd9()
    uB1c1()
    cross6()
    pair8()
    uB0c1()
    relay9()
    end6()
    dh10()
    cross7()
    norm10()
    end7()
    dh11()
    norm11()
    uA0c0()
    uA0c1()
    clip2()
    uA0c2()
    uB0c2()
    clip3()
    uA0c3()
    stA0()
    uB0c3()
    stB0()
    own9()
    sd8()
    back11()
    back10()
    uB1c2()
    pair11()
    sd11()
    uA1c0()
    uB1c3()
    stB1()
    rlA0()
    relay8()
    uA1c1()
    uA1c2()
    uA1c3()
    stA1()
    pair10()
    sd10()
    uA2c0()
    rlB0()
    relay11()
    uA2c1()
    uA2c2()
    rlB1()
    uA2c3()
    own8()
    stA2()
    uB2c1()
    uB2c2()
    relay10()
    uB2c3()
    stB2()
    own11()
    rlA1()
    gr9()
    own10()
    gr8()
    rlA2()
    enB1()
    rlB2()
    enA1()
    enA0()
    enB0()
    cross9()
    gr10()
    gr11()
    enA2()
    enB2()
    r2B0()
    r2A1()
    r2A0()
    r2B1()
    cross8()
    cross10()
    r2A2()
    r2B2()
    cross11()
    e2B0()
    end10()
    end11()
    end8()
    e2B1()
    e2A0()
    e2A1()
    end9()
    e2A2()
    e2B2()
    ring_sent()


def hand_on(gu_in, gd_in, din_in, gu_out, gd_out, din_out, sem):
    copies = [pltpu.make_async_copy(src, dst, sem.at[i])
              for i, (src, dst) in enumerate(((din_in, din_out), (gu_in, gu_out), (gd_in, gd_out)))]
    for cp in copies:
        cp.start()
    for cp in copies:
        cp.wait()


def solution(mesh):
    n_dp, n_tp = mesh.shape["dp"], mesh.shape["tp"]

    def local(x_in, u_pre, w_up, w_down, d_out, noise_up, noise_down, clip_norm, noise_mult):
        n_layers, micro, batch, seq, dim = x_in.shape
        hid = u_pre.shape[-1]
        n_ex = micro * batch
        rows = n_ex * seq // N_CHUNK
        piece, grad_rows = rows // 16, dim // n_dp
        x4 = x_in.reshape(n_layers, N_CHUNK, rows, dim)
        u4 = u_pre.reshape(n_layers, N_CHUNK, rows, hid)
        d4 = d_out.reshape(N_CHUNK, rows, dim)
        anyspace = pl.BlockSpec(memory_space=pl.ANY)
        vmem = pl.BlockSpec(memory_space=pltpu.VMEM)
        dma = pltpu.SemaphoreType.DMA
        tokens = n_ex * seq
        flops = 2 * n_layers * tokens * hid * dim * 4 + 4 * n_layers * tokens * seq * (hid + dim)
        g_up, g_down, d_in = pl.pallas_call(
            step_kernel,
            out_shape=(
                pltpu.VMEM((n_layers, grad_rows, hid), F32),
                pltpu.VMEM((n_layers, grad_rows, hid), F32),
                pltpu.VMEM((N_CHUNK, rows, dim), BF16),
            ),
            in_specs=[anyspace] * 7 + [pl.BlockSpec(memory_space=pltpu.HBM)] * 2,
            out_specs=(vmem, vmem, vmem),
            scratch_shapes=[
                pltpu.VMEM((n_layers, N_CHUNK, rows, hid), BF16),
                pltpu.VMEM((n_layers, N_CHUNK, rows, hid), BF16),
                pltpu.VMEM((n_layers, N_CHUNK, rows, dim), BF16),
                pltpu.VMEM((n_layers, dim, hid), BF16),
                pltpu.VMEM((n_layers, hid, dim), BF16),
                pltpu.VMEM((2, rows, dim), BF16),
                pltpu.VMEM((rows, dim), BF16),
                pltpu.VMEM((rows, hid), F32),
                pltpu.VMEM((N_CHUNK, rows, dim), BF16),
                pltpu.VMEM((N_CHUNK, rows // 2, dim), BF16),
                pltpu.VMEM((N_CHUNK, 2, piece, dim), BF16),
                pltpu.VMEM((N_CHUNK, 2, piece, dim), BF16),
                pltpu.VMEM((N_CHUNK, 2, piece, dim), BF16),
                pltpu.VMEM((2 * n_layers, RING, RING, grad_rows, hid), F32),
                pltpu.VMEM((2 * n_layers, 6, RING // 2, grad_rows, hid), F32),
                pltpu.VMEM((2 * n_layers, 6, grad_rows // 2, hid), F32),
                pltpu.VMEM((n_ex, 8, seq), F32),
                pltpu.VMEM((N_CHUNK, 8, 128), F32),
                pltpu.VMEM((N_CHUNK, 2 * RING - 1, 8, 128), F32),
                pltpu.VMEM((n_ex, 8, 128), F32),
                pltpu.VMEM((2, n_layers, grad_rows, hid), F32),
                pltpu.SMEM((1,), F32),
                pltpu.SMEM((1,), F32),
                dma((2, N_CHUNK)),
                dma((len(GROUP_PIECES), N_CHUNK)),
                dma((2,)),
                dma((2, 2, 2 * n_layers)),
                dma((N_CHUNK,)),
                dma((N_CHUNK,)),
                dma((n_layers, N_CHUNK)),
                dma((2, n_layers)),
                dma((N_CHUNK,)),
                dma((2,)),
                dma((4,)),
            ],
            compiler_params=pltpu.CompilerParams(
                collective_id=0, has_side_effects=True, vmem_limit_bytes=61_700_000
            ),
            cost_estimate=pl.CostEstimate(flops=flops, bytes_accessed=50_000_000, transcendentals=n_layers * tokens * hid),
            name="clipped_step",
        )(x4, u4, w_up, w_down, d4, noise_up, jnp.transpose(noise_down, (0, 2, 1)), clip_norm, noise_mult)
        results = (g_up, g_down, d_in)
        g_up, g_down, d_in = pl.pallas_call(
            hand_on,
            out_shape=[jax.ShapeDtypeStruct(v.shape, v.dtype) for v in results],
            in_specs=[vmem] * 3,
            out_specs=[pl.BlockSpec(memory_space=pltpu.HBM)] * 3,
            scratch_shapes=[dma((3,))],
            compiler_params=pltpu.CompilerParams(vmem_limit_bytes=1_000_000),
            name="hand_on",
        )(*[pltpu.with_memory_space_constraint(v, pltpu.VMEM) for v in results])
        return g_up, jnp.transpose(g_down, (0, 2, 1)), d_in.reshape(d_out.shape)

    in_specs = (P(None, None, "dp", None, None), P(None, None, "dp", None, "tp"), P(None, None, "tp"),
                P(None, "tp", None), P(None, "dp", None, None), P(None, "dp", "tp"), P(None, "tp", "dp"), P(), P())
    out_specs = (P(None, "dp", "tp"), P(None, "tp", "dp"), P(None, "dp", None, None))
    return jax.shard_map(local, mesh=mesh, in_specs=in_specs, out_specs=out_specs, check_vma=False)
```

```python
import functools
import math

import jax
import jax.numpy as jnp
from jax import lax
from jax.experimental import pallas as pl
from jax.experimental.pallas import tpu as pltpu
from jax.sharding import PartitionSpec as P

MESH = pl.DeviceIdType.MESH
F32, BF16 = jnp.float32, jnp.bfloat16
N_CHUNK = 4
RING = 4
K_TANH = math.sqrt(2.0 / math.pi)
(D2D, S1L, S1R, SDL, SDR, S2L, S2R, A1L, A1R, A2L, A2R, FO, FR, FL, FA, FB) = range(16)
GROUP = [0, 1, 1, 2, 2, 2, 2, 3, 3, 4, 4, 5, 5, 5, 5, 5]
GROUP_PIECES = [8, 2, 4, 4, 2, 8]
NT = (((1,), (1,)), ((), ()))
TN = (((0,), (0,)), ((), ()))


def scoped(f):
    def g(*a):
        with jax.named_scope(f.__name__):
            return f(*a)
    return g


def step_kernel(x_hbm, u_hbm, w1_hbm, w2_hbm, do_hbm, nu_hbm, nd_hbm, clip_hbm, mult_hbm,
                gu_ref, gd_ref, din_ref,
                u_s, dh_s, dz_s, w1_s, w2_s, xs, da_s, p_s, rd2d, r1, rdir, r2, g_s, q1, q2,
                nrm, nsend, nrecv, clip_s, nz_s, clip_ref, mult_ref,
                ssem, rsem, gsem_s, gsem_r, nsem_s, nsem_r, usem, wsem, dsem, xsem, csem):
    n_layers, n_chunk, rows, hid = u_s.shape
    dim = dz_s.shape[-1]
    n_ex, _, seq = nrm.shape
    ex_per = n_ex // n_chunk
    piece = rows // 16
    n_item = n_layers * n_chunk
    dp, tp = lax.axis_index("dp"), lax.axis_index("tp")
    xi, core = tp // 2, tp % 2
    zi, yi = dp // RING, dp % RING

    def up(i, by=1):
        return (i + by) % RING

    x_l, x_r, x_o = up(xi, 3), up(xi, 1), up(xi, 2)
    partner = (dp, xi * 2 + 1 - core)
    dev_l, dev_r = (dp, x_l * 2 + core), (dp, x_r * 2 + core)
    dev_yl, dev_yr = (zi * RING + up(yi, 3), tp), (zi * RING + up(yi), tp)
    dev_zl, dev_zr = (up(zi, 3) * RING + yi, tp), (up(zi) * RING + yi, tp)

    def remote(src, dst, send, recv, dev):
        return pltpu.make_async_remote_copy(src_ref=src, dst_ref=dst, send_sem=send, recv_sem=recv,
                                            device_id=dev, device_id_type=MESH)

    def load_u(layer, c):
        return pltpu.make_async_copy(u_hbm.at[layer, c], u_s.at[layer, c], usem.at[layer, c])

    def load_w(which, layer):
        src, dst = ((w1_hbm, w1_s), (w2_hbm, w2_s))[which]
        return pltpu.make_async_copy(src.at[layer], dst.at[layer], wsem.at[which, layer])

    def load_d(c):
        return pltpu.make_async_copy(do_hbm.at[c], dz_s.at[0, c], dsem.at[c])

    def load_x(n):
        layer, c, slot = n_layers - 1 - n % n_item // n_chunk, n % n_chunk, n % 2
        return pltpu.make_async_copy(x_hbm.at[layer, c], xs.at[slot], xsem.at[slot])

    load_small = [pltpu.make_async_copy(src, dst, csem.at[i]) for i, (src, dst) in enumerate(
        ((clip_hbm, clip_ref), (mult_hbm, mult_ref), (nu_hbm, nz_s.at[0]), (nd_hbm, nz_s.at[1])))]
    top = n_layers - 1
    load_w(1, top).start()
    load_d(0).start()
    load_u(top, 0).start()

    def load_rest():
        load_w(0, top).start()
        load_x(0).start()
        load_x(1).start()
        for c in range(1, n_chunk):
            load_d(c).start()
            load_u(top, c).start()
        for layer in reversed(range(top)):
            load_w(1, layer).start()
            load_w(0, layer).start()
            for c in range(n_chunk):
                load_u(layer, c).start()
        for cp in load_small:
            cp.start()

    barrier = pltpu.get_barrier_semaphore()
    tp_peers = [(dp, (tp + 1 + r) % (2 * RING)) for r in range(2 * RING - 1)]
    peers = tp_peers + [dev_yl, dev_yr, dev_zl, dev_zr]
    for dev in peers:
        pl.semaphore_signal(barrier, inc=1, device_id=dev, device_id_type=MESH)

    def at(cc, xx, half=0, n=1):
        return pl.ds(pl.multiple_of(cc * (rows // 2) + xx * (rows // 8) + half * piece, 16), n * piece)

    def tp_copy(role, item):
        li, c, slot = item // n_chunk, item % n_chunk, item % n_chunk
        part, znew = p_s.at[slot], (din_ref.at[c] if li + 1 == n_layers else dz_s.at[li + 1, c])
        send, recv = ssem.at[int(role >= A1L), c], rsem.at[GROUP[role], c]
        if role == D2D:
            half = pl.ds(pl.multiple_of((1 - core) * (rows // 2), 16), rows // 2)
            return remote(part.at[half], rd2d.at[c], send, recv, partner)
        if role in (S1L, S1R):
            h = 0 if role == S1L else 1
            return remote(part.at[at(core, x_o, h)], r1.at[c, h], send, recv, (dev_l, dev_r)[h])
        if role == SDL:
            return remote(part.at[at(core, x_l, 1)], rdir.at[c, 0], send, recv, dev_l)
        if role == SDR:
            return remote(part.at[at(core, x_r, 0)], rdir.at[c, 1], send, recv, dev_r)
        if role == S2L:
            return remote(part.at[at(core, x_l, 0)], r2.at[c, 0], send, recv, dev_l)
        if role == S2R:
            return remote(part.at[at(core, x_r, 1)], r2.at[c, 1], send, recv, dev_r)
        where, dev = {
            A1L: (at(core, xi, 0, 2), dev_l),
            A1R: (at(core, xi, 0, 2), dev_r),
            A2L: (at(core, x_r, 0), dev_l),
            A2R: (at(core, x_l, 1), dev_r),
            FO: (at(core, xi, 0, 2), partner),
            FR: (at(core, x_r, 0, 2), partner),
            FL: (at(core, x_l, 0, 2), partner),
            FA: (at(core, x_o, 0), partner),
            FB: (at(core, x_o, 1), partner),
        }[role]
        return remote(znew.at[where], znew.at[where], send, recv, dev)

    def start(item, *roles):
        for role in roles:
            tp_copy(role, item).start()

    def pieces(item, n, send, recv):
        view = p_s.at[item % n_chunk, pl.ds(0, n * piece)]
        return remote(view, view, ssem.at[send, item % n_chunk], rsem.at[recv, item % n_chunk], partner)

    def arrived(item, group):
        pieces(item, GROUP_PIECES[group], 0, group).wait_recv()

    def sent(item, half):
        pieces(item, sum(GROUP_PIECES) // 2, half, 0).wait_send()

    @scoped
    def send_direct(item):
        start(item, SDL, SDR)

    @scoped
    def pair_sum(item):
        c, slot = item % n_chunk, item % n_chunk
        arrived(item, 0)
        base = core * (rows // 2)
        blk = rows // 8

        def add(b, _):
            mine = pl.ds(pl.multiple_of(base + b * blk, 16), blk)
            theirs = pl.ds(pl.multiple_of(b * blk, 16), blk)
            p_s[slot, mine, :] = (p_s[slot, mine, :].astype(F32) + rd2d[c, theirs, :].astype(F32)).astype(BF16)
            return 0

        lax.fori_loop(0, 4, add, 0)
        start(item, S1L, S1R)

    @scoped
    def relay_sum(item):
        c, slot = item % n_chunk, item % n_chunk
        arrived(item, 1)
        for h, go, xx in ((0, S2L, x_l), (1, S2R, x_r)):
            where = at(core, xx, h)
            p_s[slot, where, :] = (p_s[slot, where, :].astype(F32) + r1[c, h].astype(F32)).astype(BF16)
            start(item, go)

    @scoped
    def own_sum(item):
        li, c, slot = item // n_chunk, item % n_chunk, item % n_chunk
        arrived(item, 2)
        for h in range(2):
            where = at(core, xi, h)
            total = p_s[slot, where, :].astype(F32) + r2[c, h].astype(F32) + rdir[c, 1 - h].astype(F32)
            total = (dz_s[li, c, where, :].astype(F32) + total).astype(BF16)
            if li + 1 == n_layers:
                din_ref[c, where, :] = total
            else:
                dz_s[li + 1, c, where, :] = total
        start(item, A1L, A1R, FO)

    @scoped
    def gather_relay(item):
        arrived(item, 3)
        start(item, A2L, A2R, FR, FL)
        sent(item, 0)

    @scoped
    def gather_cross(item):
        arrived(item, 4)
        start(item, FA, FB)

    @scoped
    def gather_end(item):
        arrived(item, 5)
        sent(item, 1)

    @scoped
    def compute_dh(item):
        li, c = item // n_chunk, item % n_chunk
        layer = top - li

        if c == 0:
            load_w(1, layer).wait()
            if li > 0:
                load_w(0, layer).wait()
        if li == 0:
            load_d(c).wait()
        load_u(layer, c).wait()
        if item == 0:
            load_rest()
        da_s[...] = lax.dot_general(dz_s[li, c], w2_s[layer], NT, preferred_element_type=F32)
        blk = 32

        def act(b, _):
            r = pl.ds(pl.multiple_of(b * blk, blk), blk)
            u = u_s[layer, c, r, :].astype(F32)
            u2 = u * u
            th = jnp.tanh(K_TANH * (u + 0.044715 * (u2 * u)))
            cdf = 0.5 * (1.0 + th)
            slope = cdf + (0.5 * u) * (1.0 - th * th) * K_TANH * (1.0 + (3 * 0.044715) * u2)
            u_s[layer, c, r, :] = (u * cdf).astype(BF16)
            dh_s[layer, c, r, :] = (slope * da_s[r, :]).astype(BF16)
            return 0

        lax.fori_loop(0, rows // blk, act, 0)

    @scoped
    def compute_back(item):
        li, c, slot = item // n_chunk, item % n_chunk, item % n_chunk
        layer = top - li
        if item == 0:
            load_w(0, layer).wait()
        def part(n, _):
            cc = (core + 1 + n) % 2
            r = pl.ds(pl.multiple_of(cc * (rows // 2), 16), rows // 2)
            p_s[slot, r, :] = lax.dot_general(dh_s[layer, c, r, :], w1_s[layer], NT,
                                              preferred_element_type=F32).astype(BF16)

            @pl.when(n == 0)
            def _():
                if item == 0:
                    pl.semaphore_wait(barrier, len(peers))
                start(item, D2D)

            return 0

        lax.fori_loop(0, 2, part, 0)

    @scoped
    def compute_norm(item):
        li, c = item // n_chunk, item % n_chunk
        layer = top - li
        load_x(item).wait()

        def one(e, _):
            r = pl.ds(pl.multiple_of(e * seq, 16), seq)

            def gram(v):
                return lax.dot_general(v, v, NT, preferred_element_type=F32)

            total = (gram(u_s[layer, c, r, :]) * gram(dz_s[li, c, r, :])
                     + gram(xs[item % 2, r, :]) * gram(dh_s[layer, c, r, :]))
            nrm[c * ex_per + e] += jnp.sum(total.reshape(seq // 8, 8, seq), axis=0)
            return 0

        lax.fori_loop(0, ex_per, one, 0)
        load_x(item + 2).start()
        if li == top:
            norm_start(c)

    def norm_copies(c):
        return [remote(nsend.at[c], nrecv.at[c, r], nsem_s.at[c], nsem_r.at[c], dev)
                for r, dev in enumerate(tp_peers)]

    @scoped
    def norm_start(c):
        part = jnp.sum(nrm[pl.ds(c * ex_per, ex_per)], axis=1)
        part = jnp.broadcast_to(jnp.sum(part, axis=-1, keepdims=True), (ex_per, nsend.shape[-1]))
        nsend[c] = jnp.concatenate([part] * (nsend.shape[1] // ex_per), axis=0)
        for cp in norm_copies(c):
            cp.start()

    @scoped
    def clip_factors(c):
        if c == 0:
            for cp in load_small:
                cp.wait()
        every = remote(nrecv.at[c], nrecv.at[c], nsem_s.at[c], nsem_r.at[c], partner)
        every.wait_recv()
        total = nsend[c]
        for r in range(len(tp_peers)):
            total = total + nrecv[c, r]
        factor = jnp.minimum(1.0, clip_ref[0] / jnp.sqrt(total))
        for e in range(ex_per):
            clip_s[c * ex_per + e] = jnp.broadcast_to(factor[e:e + 1, :], clip_s.shape[1:])
        every.wait_send()

    def grad_view(k, kind, phase, j, h):
        if phase == 0:
            n = RING // 2
            if kind == 0:
                return g_s.at[k, pl.ds(h * n, n), j]
            return g_s.at[k, j, pl.ds(h * n, n)]
        n = g_s.shape[3] // 2
        if kind == 0:
            return g_s.at[k, j, yi, pl.ds(h * n, n)]
        return g_s.at[k, zi, j, pl.ds(h * n, n)]

    def ring_of(kind, phase):
        if (kind == 0) == (phase == 0):
            return yi, dev_yl, dev_yr
        return zi, dev_zl, dev_zr

    def grad_copy(k, kind, phase, role):
        me, d_l, d_r = ring_of(kind, phase)
        buf = (q1, q2)[phase]
        j, h = ((up(me, 2), 0), (up(me, 2), 1), (up(me, 3), 1), (up(me, 1), 0), (up(me, 3), 0), (up(me, 1), 1))[role]
        return remote(grad_view(k, kind, phase, j, h), buf.at[k, role], gsem_s.at[phase],
                      gsem_r.at[phase, int(role >= 2), k], d_r if role % 2 else d_l)

    @scoped
    def ring_start(p, kind, phase):
        k = 2 * p + kind
        for role in range(4):
            grad_copy(k, kind, phase, role).start()

    def ring_arrived(k, phase, lo, n):
        view = (q1, q2)[phase].at[k, pl.ds(lo, n)]
        remote(view, view, gsem_s.at[phase], gsem_r.at[phase, int(lo > 0), k], partner).wait_recv()

    @scoped
    def ring_relay(p, kind, phase):
        k = 2 * p + kind
        me, _, _ = ring_of(kind, phase)
        buf = (q1, q2)[phase]
        ring_arrived(k, phase, 0, 2)
        for h in range(2):
            view = grad_view(k, kind, phase, up(me, 1 if h else 3), h)
            view[...] = view[...] + buf[k, h]
            grad_copy(k, kind, phase, 4 + h).start()

    @scoped
    def ring_end(p, kind, phase):
        k = 2 * p + kind
        me, _, _ = ring_of(kind, phase)
        buf = (q1, q2)[phase]
        ring_arrived(k, phase, 2, 4)
        for h in range(2):
            view = grad_view(k, kind, phase, me, h)
            view[...] = view[...] + buf[k, 3 - h] + buf[k, 4 + h]

    @scoped
    def ring_turn(p, kind):
        ring_end(p, kind, 0)
        ring_start(p, kind, 1)

    @scoped
    def ring_last(p, kind):
        ring_end(p, kind, 1)
        finish(p, kind)

    @scoped
    def ring_sent():
        for phase, buf in enumerate((q1, q2)):
            remote(buf, buf, gsem_s.at[phase], gsem_r.at[phase, 0, 0], partner).wait_send()

    inv = 1.0 / (n_ex * RING * RING)

    @scoped
    def finish(p, kind):
        layer, scale = top - p, mult_ref[0] * clip_ref[0]
        (gu_ref, gd_ref)[kind][layer] = (g_s[2 * p + kind, zi, yi] + scale * nz_s[kind, layer]) * inv

    @scoped
    def weight_grad(p, kind, c):
        k, layer, n = 2 * p + kind, top - p, p * n_chunk + c

        src = dh_s.at[layer, c] if kind == 0 else dz_s.at[p, c]
        scaled = jnp.concatenate([
            (src[pl.ds(e * seq, seq), :].astype(F32) * clip_s[c * ex_per + e][0:1, 0:1]).astype(BF16)
            for e in range(ex_per)])
        if kind == 0:
            load_x(n_item + n).wait()
            add = lax.dot_general(xs[n % 2], scaled, TN, preferred_element_type=F32)
        else:
            add = lax.dot_general(scaled, u_s[layer, c], TN, preferred_element_type=F32)
        add = add.reshape(g_s.shape[1:])
        if c == 0:
            g_s[k] = add
        else:
            g_s[k] += add
        if kind == 0 and n + 2 < n_item:
            load_x(n_item + n + 2).start()

    def each(stage):
        return [functools.partial(stage, i) for i in range(n_item)]

    def ring(stage, kind, *phase):
        return [functools.partial(stage, p, kind, *phase) for p in range(n_layers)]

    def units(kind):
        return [functools.partial(weight_grad, p, kind, c) for p in range(n_layers) for c in range(n_chunk)]

    dh0, dh1, dh2, dh3, dh4, dh5, dh6, dh7, dh8, dh9, dh10, dh11 = each(compute_dh)
    back0, back1, back2, back3, back4, back5, back6, back7, back8, back9, back10, back11 = each(compute_back)
    norm0, norm1, norm2, norm3, norm4, norm5, norm6, norm7, norm8, norm9, norm10, norm11 = each(compute_norm)
    pair0, pair1, pair2, pair3, pair4, pair5, pair6, pair7, pair8, pair9, pair10, pair11 = each(pair_sum)
    sd0, sd1, sd2, sd3, sd4, sd5, sd6, sd7, sd8, sd9, sd10, sd11 = each(send_direct)
    (
        relay0, relay1, relay2, relay3, relay4, relay5, relay6, relay7, relay8, relay9, relay10, relay11,
    ) = each(relay_sum)
    own0, own1, own2, own3, own4, own5, own6, own7, own8, own9, own10, own11 = each(own_sum)
    gr0, gr1, gr2, gr3, gr4, gr5, gr6, gr7, gr8, gr9, gr10, gr11 = each(gather_relay)
    (
        cross0, cross1, cross2, cross3, cross4, cross5, cross6, cross7, cross8, cross9, cross10, cross11,
    ) = each(gather_cross)
    end0, end1, end2, end3, end4, end5, end6, end7, end8, end9, end10, end11 = each(gather_end)
    clip0, clip1, clip2, clip3 = [functools.partial(clip_factors, c) for c in range(n_chunk)]
    uA0c0, uA0c1, uA0c2, uA0c3, uA1c0, uA1c1, uA1c2, uA1c3, uA2c0, uA2c1, uA2c2, uA2c3 = units(0)
    stA0, stA1, stA2 = ring(ring_start, 0, 0)
    rlA0, rlA1, rlA2 = ring(ring_relay, 0, 0)
    enA0, enA1, enA2 = ring(ring_turn, 0)
    r2A0, r2A1, r2A2 = ring(ring_relay, 0, 1)
    e2A0, e2A1, e2A2 = ring(ring_last, 0)
    uB0c0, uB0c1, uB0c2, uB0c3, uB1c0, uB1c1, uB1c2, uB1c3, uB2c0, uB2c1, uB2c2, uB2c3 = units(1)
    stB0, stB1, stB2 = ring(ring_start, 1, 0)
    rlB0, rlB1, rlB2 = ring(ring_relay, 1, 0)
    enB0, enB1, enB2 = ring(ring_turn, 1)
    r2B0, r2B1, r2B2 = ring(ring_relay, 1, 1)
    e2B0, e2B1, e2B2 = ring(ring_last, 1)

    nrm[...] = jnp.zeros_like(nrm)
    dh0()
    back0()
    dh1()
    pair0()
    back1()
    sd0()
    dh2()
    pair1()
    sd1()
    back2()
    dh3()
    relay0()
    pair2()
    norm0()
    sd2()
    relay1()
    norm1()
    back3()
    own0()
    norm2()
    pair3()
    norm3()
    own1()
    gr0()
    relay2()
    relay3()
    sd3()
    gr1()
    cross0()
    own2()
    end0()
    dh4()
    back4()
    own3()
    cross1()
    pair4()
    sd4()
    end1()
    dh5()
    back5()
    gr2()
    pair5()
    norm4()
    relay4()
    gr3()
    sd5()
    norm5()
    cross2()
    end2()
    relay5()
    dh6()
    own4()
    back6()
    norm6()
    pair6()
    cross3()
    own5()
    end3()
    dh7()
    gr4()
    sd6()
    back7()
    pair7()
    gr5()
    cross4()
    relay6()
    sd7()
    norm7()
    end4()
    dh8()
    relay7()
    norm8()
    cross5()
    own6()
    back8()
    end5()
    dh9()
    own7()
    back9()
    norm9()
    clip0()
    gr6()
    pair9()
    uB2c0()
    uB1c0()
    uB0c0()
    gr7()
    clip1()
    sd9()
    uB1c1()
    cross6()
    pair8()
    uB0c1()
    relay9()
    end6()
    dh10()
    cross7()
    norm10()
    end7()
    dh11()
    norm11()
    uA0c0()
    uA0c1()
    clip2()
    uA0c2()
    uB0c2()
    clip3()
    uA0c3()
    stA0()
    uB0c3()
    stB0()
    own9()
    sd8()
    back11()
    back10()
    uB1c2()
    pair11()
    sd11()
    uA1c0()
    uB1c3()
    stB1()
    rlA0()
    relay8()
    uA1c1()
    uA1c2()
    uA1c3()
    stA1()
    pair10()
    sd10()
    uA2c0()
    rlB0()
    relay11()
    uA2c1()
    uA2c2()
    rlB1()
    uA2c3()
    own8()
    stA2()
    uB2c1()
    uB2c2()
    relay10()
    uB2c3()
    stB2()
    own11()
    rlA1()
    gr9()
    own10()
    gr8()
    rlA2()
    enB1()
    rlB2()
    enA1()
    enA0()
    enB0()
    cross9()
    gr10()
    gr11()
    enA2()
    enB2()
    r2B0()
    r2A1()
    r2A0()
    r2B1()
    cross8()
    cross10()
    r2A2()
    r2B2()
    cross11()
    e2B0()
    end10()
    end11()
    end8()
    e2B1()
    e2A0()
    e2A1()
    end9()
    e2A2()
    e2B2()
    ring_sent()


def hand_on(gu_in, gd_in, din_in, gu_out, gd_out, din_out, sem):
    copies = [pltpu.make_async_copy(src, dst, sem.at[i])
              for i, (src, dst) in enumerate(((din_in, din_out), (gu_in, gu_out), (gd_in, gd_out)))]
    for cp in copies:
        cp.start()
    for cp in copies:
        cp.wait()


def solution(mesh):
    n_dp, n_tp = mesh.shape["dp"], mesh.shape["tp"]

    def local(x_in, u_pre, w_up, w_down, d_out, noise_up, noise_down, clip_norm, noise_mult):
        n_layers, micro, batch, seq, dim = x_in.shape
        hid = u_pre.shape[-1]
        n_ex = micro * batch
        rows = n_ex * seq // N_CHUNK
        piece, grad_rows = rows // 16, dim // n_dp
        x4 = x_in.reshape(n_layers, N_CHUNK, rows, dim)
        u4 = u_pre.reshape(n_layers, N_CHUNK, rows, hid)
        d4 = d_out.reshape(N_CHUNK, rows, dim)
        anyspace = pl.BlockSpec(memory_space=pl.ANY)
        vmem = pl.BlockSpec(memory_space=pltpu.VMEM)
        dma = pltpu.SemaphoreType.DMA
        tokens = n_ex * seq
        flops = 2 * n_layers * tokens * hid * dim * 4 + 4 * n_layers * tokens * seq * (hid + dim)
        g_up, g_down, d_in = pl.pallas_call(
            step_kernel,
            out_shape=(
                pltpu.VMEM((n_layers, grad_rows, hid), F32),
                pltpu.VMEM((n_layers, grad_rows, hid), F32),
                pltpu.VMEM((N_CHUNK, rows, dim), BF16),
            ),
            in_specs=[anyspace] * 7 + [pl.BlockSpec(memory_space=pltpu.HBM)] * 2,
            out_specs=(vmem, vmem, vmem),
            scratch_shapes=[
                pltpu.VMEM((n_layers, N_CHUNK, rows, hid), BF16),
                pltpu.VMEM((n_layers, N_CHUNK, rows, hid), BF16),
                pltpu.VMEM((n_layers, N_CHUNK, rows, dim), BF16),
                pltpu.VMEM((n_layers, dim, hid), BF16),
                pltpu.VMEM((n_layers, hid, dim), BF16),
                pltpu.VMEM((2, rows, dim), BF16),
                pltpu.VMEM((rows, hid), F32),
                pltpu.VMEM((N_CHUNK, rows, dim), BF16),
                pltpu.VMEM((N_CHUNK, rows // 2, dim), BF16),
                pltpu.VMEM((N_CHUNK, 2, piece, dim), BF16),
                pltpu.VMEM((N_CHUNK, 2, piece, dim), BF16),
                pltpu.VMEM((N_CHUNK, 2, piece, dim), BF16),
                pltpu.VMEM((2 * n_layers, RING, RING, grad_rows, hid), F32),
                pltpu.VMEM((2 * n_layers, 6, RING // 2, grad_rows, hid), F32),
                pltpu.VMEM((2 * n_layers, 6, grad_rows // 2, hid), F32),
                pltpu.VMEM((n_ex, 8, seq), F32),
                pltpu.VMEM((N_CHUNK, 8, 128), F32),
                pltpu.VMEM((N_CHUNK, 2 * RING - 1, 8, 128), F32),
                pltpu.VMEM((n_ex, 8, 128), F32),
                pltpu.VMEM((2, n_layers, grad_rows, hid), F32),
                pltpu.SMEM((1,), F32),
                pltpu.SMEM((1,), F32),
                dma((2, N_CHUNK)),
                dma((len(GROUP_PIECES), N_CHUNK)),
                dma((2,)),
                dma((2, 2, 2 * n_layers)),
                dma((N_CHUNK,)),
                dma((N_CHUNK,)),
                dma((n_layers, N_CHUNK)),
                dma((2, n_layers)),
                dma((N_CHUNK,)),
                dma((2,)),
                dma((4,)),
            ],
            compiler_params=pltpu.CompilerParams(
                collective_id=0, has_side_effects=True, vmem_limit_bytes=61_700_000
            ),
            cost_estimate=pl.CostEstimate(flops=flops, bytes_accessed=50_000_000, transcendentals=n_layers * tokens * hid),
            name="clipped_step",
        )(x4, u4, w_up, w_down, d4, noise_up, jnp.transpose(noise_down, (0, 2, 1)), clip_norm, noise_mult)
        results = (g_up, g_down, d_in)
        g_up, g_down, d_in = pl.pallas_call(
            hand_on,
            out_shape=[jax.ShapeDtypeStruct(v.shape, v.dtype) for v in results],
            in_specs=[vmem] * 3,
            out_specs=[pl.BlockSpec(memory_space=pltpu.HBM)] * 3,
            scratch_shapes=[dma((3,))],
            compiler_params=pltpu.CompilerParams(vmem_limit_bytes=1_000_000),
            name="hand_on",
        )(*[pltpu.with_memory_space_constraint(v, pltpu.VMEM) for v in results])
        return g_up, jnp.transpose(g_down, (0, 2, 1)), d_in.reshape(d_out.shape)

    in_specs = (P(None, None, "dp", None, None), P(None, None, "dp", None, "tp"), P(None, None, "tp"),
                P(None, "tp", None), P(None, "dp", None, None), P(None, "dp", "tp"), P(None, "tp", "dp"), P(), P())
    out_specs = (P(None, "dp", "tp"), P(None, "tp", "dp"), P(None, "dp", None, None))
    return jax.shard_map(local, mesh=mesh, in_specs=in_specs, out_specs=out_specs, check_vma=False)
```

```python
import functools
import math

import jax
import jax.numpy as jnp
from jax import lax
from jax.experimental import pallas as pl
from jax.experimental.pallas import tpu as pltpu
from jax.sharding import PartitionSpec as P

MESH = pl.DeviceIdType.MESH
F32, BF16 = jnp.float32, jnp.bfloat16
N_CHUNK = 4
RING = 4
K_TANH = math.sqrt(2.0 / math.pi)
(D2D, S1L, S1R, SDL, SDR, S2L, S2R, A1L, A1R, A2L, A2R, FO, FR, FL, FA, FB) = range(16)
GROUP = [0, 1, 1, 2, 2, 2, 2, 3, 3, 4, 4, 5, 5, 5, 5, 5]
GROUP_PIECES = [8, 2, 4, 4, 2, 8]
NT = (((1,), (1,)), ((), ()))
TN = (((0,), (0,)), ((), ()))


def step_kernel(x_hbm, u_hbm, w1_hbm, w2_hbm, do_hbm, nu_hbm, nd_hbm, clip_hbm, mult_hbm,
                gu_ref, gd_ref, din_ref,
                u_s, dh_s, dz_s, w1_s, w2_s, xs, da_s, p_s, rd2d, r1, rdir, r2, g_s, q1, q2,
                nrm, nsend, nrecv, clip_s, nz_s, clip_ref, mult_ref,
                ssem, rsem, gsem_s, gsem_r, nsem_s, nsem_r, usem, wsem, dsem, xsem, csem):
    n_layers, n_chunk, rows, hid = u_s.shape
    dim = dz_s.shape[-1]
    n_ex, _, seq = nrm.shape
    ex_per = n_ex // n_chunk
    piece = rows // 16
    n_item = n_layers * n_chunk
    dp, tp = lax.axis_index("dp"), lax.axis_index("tp")
    xi, core = tp // 2, tp % 2
    zi, yi = dp // RING, dp % RING

    def up(i, by=1):
        return (i + by) % RING

    x_l, x_r, x_o = up(xi, 3), up(xi, 1), up(xi, 2)
    partner = (dp, xi * 2 + 1 - core)
    dev_l, dev_r = (dp, x_l * 2 + core), (dp, x_r * 2 + core)
    dev_yl, dev_yr = (zi * RING + up(yi, 3), tp), (zi * RING + up(yi), tp)
    dev_zl, dev_zr = (up(zi, 3) * RING + yi, tp), (up(zi) * RING + yi, tp)

    def remote(src, dst, send, recv, dev):
        return pltpu.make_async_remote_copy(src_ref=src, dst_ref=dst, send_sem=send, recv_sem=recv,
                                            device_id=dev, device_id_type=MESH)

    def load_u(layer, c):
        return pltpu.make_async_copy(u_hbm.at[layer, c], u_s.at[layer, c], usem.at[layer, c])

    def load_w(which, layer):
        src, dst = ((w1_hbm, w1_s), (w2_hbm, w2_s))[which]
        return pltpu.make_async_copy(src.at[layer], dst.at[layer], wsem.at[which, layer])

    def load_d(c):
        return pltpu.make_async_copy(do_hbm.at[c], dz_s.at[0, c], dsem.at[c])

    def load_x(n):
        layer, c, slot = n_layers - 1 - n % n_item // n_chunk, n % n_chunk, n % 2
        return pltpu.make_async_copy(x_hbm.at[layer, c], xs.at[slot], xsem.at[slot])

    load_small = [pltpu.make_async_copy(src, dst, csem.at[i]) for i, (src, dst) in enumerate(
        ((clip_hbm, clip_ref), (mult_hbm, mult_ref), (nu_hbm, nz_s.at[0]), (nd_hbm, nz_s.at[1])))]
    top = n_layers - 1
    load_w(1, top).start()
    load_d(0).start()
    load_u(top, 0).start()

    def load_rest():
        load_w(0, top).start()
        load_x(0).start()
        load_x(1).start()
        for c in range(1, n_chunk):
            load_d(c).start()
            load_u(top, c).start()
        for layer in reversed(range(top)):
            load_w(1, layer).start()
            load_w(0, layer).start()
            for c in range(n_chunk):
                load_u(layer, c).start()
        for cp in load_small:
            cp.start()

    barrier = pltpu.get_barrier_semaphore()
    tp_peers = [(dp, (tp + 1 + r) % (2 * RING)) for r in range(2 * RING - 1)]
    peers = tp_peers + [dev_yl, dev_yr, dev_zl, dev_zr]
    for dev in peers:
        pl.semaphore_signal(barrier, inc=1, device_id=dev, device_id_type=MESH)

    def at(cc, xx, half=0, n=1):
        return pl.ds(pl.multiple_of(cc * (rows // 2) + xx * (rows // 8) + half * piece, 16), n * piece)

    def tp_copy(role, item):
        li, c, slot = item // n_chunk, item % n_chunk, item % n_chunk
        part, znew = p_s.at[slot], (din_ref.at[c] if li + 1 == n_layers else dz_s.at[li + 1, c])
        send, recv = ssem.at[int(role >= A1L), c], rsem.at[GROUP[role], c]
        if role == D2D:
            half = pl.ds(pl.multiple_of((1 - core) * (rows // 2), 16), rows // 2)
            return remote(part.at[half], rd2d.at[c], send, recv, partner)
        if role in (S1L, S1R):
            h = 0 if role == S1L else 1
            return remote(part.at[at(core, x_o, h)], r1.at[c, h], send, recv, (dev_l, dev_r)[h])
        if role == SDL:
            return remote(part.at[at(core, x_l, 1)], rdir.at[c, 0], send, recv, dev_l)
        if role == SDR:
            return remote(part.at[at(core, x_r, 0)], rdir.at[c, 1], send, recv, dev_r)
        if role == S2L:
            return remote(part.at[at(core, x_l, 0)], r2.at[c, 0], send, recv, dev_l)
        if role == S2R:
            return remote(part.at[at(core, x_r, 1)], r2.at[c, 1], send, recv, dev_r)
        where, dev = {
            A1L: (at(core, xi, 0, 2), dev_l),
            A1R: (at(core, xi, 0, 2), dev_r),
            A2L: (at(core, x_r, 0), dev_l),
            A2R: (at(core, x_l, 1), dev_r),
            FO: (at(core, xi, 0, 2), partner),
            FR: (at(core, x_r, 0, 2), partner),
            FL: (at(core, x_l, 0, 2), partner),
            FA: (at(core, x_o, 0), partner),
            FB: (at(core, x_o, 1), partner),
        }[role]
        return remote(znew.at[where], znew.at[where], send, recv, dev)

    def start(item, *roles):
        for role in roles:
            tp_copy(role, item).start()

    def pieces(item, n, send, recv):
        view = p_s.at[item % n_chunk, pl.ds(0, n * piece)]
        return remote(view, view, ssem.at[send, item % n_chunk], rsem.at[recv, item % n_chunk], partner)

    def arrived(item, group):
        pieces(item, GROUP_PIECES[group], 0, group).wait_recv()

    def sent(item, half):
        pieces(item, sum(GROUP_PIECES) // 2, half, 0).wait_send()

    def send_direct(item):
        start(item, SDL, SDR)

    def pair_sum(item):
        c, slot = item % n_chunk, item % n_chunk
        arrived(item, 0)
        base = core * (rows // 2)
        blk = rows // 8

        def add(b, _):
            mine = pl.ds(pl.multiple_of(base + b * blk, 16), blk)
            theirs = pl.ds(pl.multiple_of(b * blk, 16), blk)
            p_s[slot, mine, :] = (p_s[slot, mine, :].astype(F32) + rd2d[c, theirs, :].astype(F32)).astype(BF16)
            return 0

        lax.fori_loop(0, 4, add, 0)
        start(item, S1L, S1R)

    def relay_sum(item):
        c, slot = item % n_chunk, item % n_chunk
        arrived(item, 1)
        for h, go, xx in ((0, S2L, x_l), (1, S2R, x_r)):
            where = at(core, xx, h)
            p_s[slot, where, :] = (p_s[slot, where, :].astype(F32) + r1[c, h].astype(F32)).astype(BF16)
            start(item, go)

    def own_sum(item):
        li, c, slot = item // n_chunk, item % n_chunk, item % n_chunk
        arrived(item, 2)
        for h in range(2):
            where = at(core, xi, h)
            total = p_s[slot, where, :].astype(F32) + r2[c, h].astype(F32) + rdir[c, 1 - h].astype(F32)
            total = (dz_s[li, c, where, :].astype(F32) + total).astype(BF16)
            if li + 1 == n_layers:
                din_ref[c, where, :] = total
            else:
                dz_s[li + 1, c, where, :] = total
        start(item, A1L, A1R, FO)

    def gather_relay(item):
        arrived(item, 3)
        start(item, A2L, A2R, FR, FL)
        sent(item, 0)

    def gather_cross(item):
        arrived(item, 4)
        start(item, FA, FB)

    def gather_end(item):
        arrived(item, 5)
        sent(item, 1)

    def compute_dh(item):
        li, c = item // n_chunk, item % n_chunk
        layer = top - li

        if c == 0:
            load_w(1, layer).wait()
            if li > 0:
                load_w(0, layer).wait()
        if li == 0:
            load_d(c).wait()
        load_u(layer, c).wait()
        if item == 0:
            load_rest()
        da_s[...] = lax.dot_general(dz_s[li, c], w2_s[layer], NT, preferred_element_type=F32)
        blk = 32

        def act(b, _):
            r = pl.ds(pl.multiple_of(b * blk, blk), blk)
            u = u_s[layer, c, r, :].astype(F32)
            u2 = u * u
            th = jnp.tanh(K_TANH * (u + 0.044715 * (u2 * u)))
            cdf = 0.5 * (1.0 + th)
            slope = cdf + (0.5 * u) * (1.0 - th * th) * K_TANH * (1.0 + (3 * 0.044715) * u2)
            u_s[layer, c, r, :] = (u * cdf).astype(BF16)
            dh_s[layer, c, r, :] = (slope * da_s[r, :]).astype(BF16)
            return 0

        lax.fori_loop(0, rows // blk, act, 0)

    def compute_back(item):
        li, c, slot = item // n_chunk, item % n_chunk, item % n_chunk
        layer = top - li
        if item == 0:
            load_w(0, layer).wait()
        def part(n, _):
            cc = (core + 1 + n) % 2
            r = pl.ds(pl.multiple_of(cc * (rows // 2), 16), rows // 2)
            p_s[slot, r, :] = lax.dot_general(dh_s[layer, c, r, :], w1_s[layer], NT,
                                              preferred_element_type=F32).astype(BF16)

            @pl.when(n == 0)
            def _():
                if item == 0:
                    pl.semaphore_wait(barrier, len(peers))
                start(item, D2D)

            return 0

        lax.fori_loop(0, 2, part, 0)

    def compute_norm(item):
        li, c = item // n_chunk, item % n_chunk
        layer = top - li
        load_x(item).wait()

        def one(e, _):
            r = pl.ds(pl.multiple_of(e * seq, 16), seq)

            def gram(v):
                return lax.dot_general(v, v, NT, preferred_element_type=F32)

            total = (gram(u_s[layer, c, r, :]) * gram(dz_s[li, c, r, :])
                     + gram(xs[item % 2, r, :]) * gram(dh_s[layer, c, r, :]))
            nrm[c * ex_per + e] += jnp.sum(total.reshape(seq // 8, 8, seq), axis=0)
            return 0

        lax.fori_loop(0, ex_per, one, 0)
        load_x(item + 2).start()
        if li == top:
            norm_start(c)

    def norm_copies(c):
        return [remote(nsend.at[c], nrecv.at[c, r], nsem_s.at[c], nsem_r.at[c], dev)
                for r, dev in enumerate(tp_peers)]

    def norm_start(c):
        part = jnp.sum(nrm[pl.ds(c * ex_per, ex_per)], axis=1)
        part = jnp.broadcast_to(jnp.sum(part, axis=-1, keepdims=True), (ex_per, nsend.shape[-1]))
        nsend[c] = jnp.concatenate([part] * (nsend.shape[1] // ex_per), axis=0)
        for cp in norm_copies(c):
            cp.start()

    def clip_factors(c):
        if c == 0:
            for cp in load_small:
                cp.wait()
        every = remote(nrecv.at[c], nrecv.at[c], nsem_s.at[c], nsem_r.at[c], partner)
        every.wait_recv()
        total = nsend[c]
        for r in range(len(tp_peers)):
            total = total + nrecv[c, r]
        factor = jnp.minimum(1.0, clip_ref[0] / jnp.sqrt(total))
        for e in range(ex_per):
            clip_s[c * ex_per + e] = jnp.broadcast_to(factor[e:e + 1, :], clip_s.shape[1:])
        every.wait_send()

    def grad_view(k, kind, phase, j, h):
        if phase == 0:
            n = RING // 2
            if kind == 0:
                return g_s.at[k, pl.ds(h * n, n), j]
            return g_s.at[k, j, pl.ds(h * n, n)]
        n = g_s.shape[3] // 2
        if kind == 0:
            return g_s.at[k, j, yi, pl.ds(h * n, n)]
        return g_s.at[k, zi, j, pl.ds(h * n, n)]

    def ring_of(kind, phase):
        if (kind == 0) == (phase == 0):
            return yi, dev_yl, dev_yr
        return zi, dev_zl, dev_zr

    def grad_copy(k, kind, phase, role):
        me, d_l, d_r = ring_of(kind, phase)
        buf = (q1, q2)[phase]
        j, h = ((up(me, 2), 0), (up(me, 2), 1), (up(me, 3), 1), (up(me, 1), 0), (up(me, 3), 0), (up(me, 1), 1))[role]
        return remote(grad_view(k, kind, phase, j, h), buf.at[k, role], gsem_s.at[phase],
                      gsem_r.at[phase, int(role >= 2), k], d_r if role % 2 else d_l)

    def ring_start(p, kind, phase):
        k = 2 * p + kind
        for role in range(4):
            grad_copy(k, kind, phase, role).start()

    def ring_arrived(k, phase, lo, n):
        view = (q1, q2)[phase].at[k, pl.ds(lo, n)]
        remote(view, view, gsem_s.at[phase], gsem_r.at[phase, int(lo > 0), k], partner).wait_recv()

    def ring_relay(p, kind, phase):
        k = 2 * p + kind
        me, _, _ = ring_of(kind, phase)
        buf = (q1, q2)[phase]
        ring_arrived(k, phase, 0, 2)
        for h in range(2):
            view = grad_view(k, kind, phase, up(me, 1 if h else 3), h)
            view[...] = view[...] + buf[k, h]
            grad_copy(k, kind, phase, 4 + h).start()

    def ring_end(p, kind, phase):
        k = 2 * p + kind
        me, _, _ = ring_of(kind, phase)
        buf = (q1, q2)[phase]
        ring_arrived(k, phase, 2, 4)
        for h in range(2):
            view = grad_view(k, kind, phase, me, h)
            view[...] = view[...] + buf[k, 3 - h] + buf[k, 4 + h]

    def ring_turn(p, kind):
        ring_end(p, kind, 0)
        ring_start(p, kind, 1)

    def ring_last(p, kind):
        ring_end(p, kind, 1)
        finish(p, kind)

    def ring_sent():
        for phase, buf in enumerate((q1, q2)):
            remote(buf, buf, gsem_s.at[phase], gsem_r.at[phase, 0, 0], partner).wait_send()

    inv = 1.0 / (n_ex * RING * RING)

    def finish(p, kind):
        layer, scale = top - p, mult_ref[0] * clip_ref[0]
        (gu_ref, gd_ref)[kind][layer] = (g_s[2 * p + kind, zi, yi] + scale * nz_s[kind, layer]) * inv

    def weight_grad(p, kind, c):
        k, layer, n = 2 * p + kind, top - p, p * n_chunk + c

        src = dh_s.at[layer, c] if kind == 0 else dz_s.at[p, c]
        scaled = jnp.concatenate([
            (src[pl.ds(e * seq, seq), :].astype(F32) * clip_s[c * ex_per + e][0:1, 0:1]).astype(BF16)
            for e in range(ex_per)])
        if kind == 0:
            load_x(n_item + n).wait()
            add = lax.dot_general(xs[n % 2], scaled, TN, preferred_element_type=F32)
        else:
            add = lax.dot_general(scaled, u_s[layer, c], TN, preferred_element_type=F32)
        add = add.reshape(g_s.shape[1:])
        if c == 0:
            g_s[k] = add
        else:
            g_s[k] += add
        if kind == 0 and n + 2 < n_item:
            load_x(n_item + n + 2).start()

    def each(stage):
        return [functools.partial(stage, i) for i in range(n_item)]

    def ring(stage, kind, *phase):
        return [functools.partial(stage, p, kind, *phase) for p in range(n_layers)]

    def units(kind):
        return [functools.partial(weight_grad, p, kind, c) for p in range(n_layers) for c in range(n_chunk)]

    dh0, dh1, dh2, dh3, dh4, dh5, dh6, dh7, dh8, dh9, dh10, dh11 = each(compute_dh)
    back0, back1, back2, back3, back4, back5, back6, back7, back8, back9, back10, back11 = each(compute_back)
    norm0, norm1, norm2, norm3, norm4, norm5, norm6, norm7, norm8, norm9, norm10, norm11 = each(compute_norm)
    pair0, pair1, pair2, pair3, pair4, pair5, pair6, pair7, pair8, pair9, pair10, pair11 = each(pair_sum)
    sd0, sd1, sd2, sd3, sd4, sd5, sd6, sd7, sd8, sd9, sd10, sd11 = each(send_direct)
    (
        relay0, relay1, relay2, relay3, relay4, relay5, relay6, relay7, relay8, relay9, relay10, relay11,
    ) = each(relay_sum)
    own0, own1, own2, own3, own4, own5, own6, own7, own8, own9, own10, own11 = each(own_sum)
    gr0, gr1, gr2, gr3, gr4, gr5, gr6, gr7, gr8, gr9, gr10, gr11 = each(gather_relay)
    (
        cross0, cross1, cross2, cross3, cross4, cross5, cross6, cross7, cross8, cross9, cross10, cross11,
    ) = each(gather_cross)
    end0, end1, end2, end3, end4, end5, end6, end7, end8, end9, end10, end11 = each(gather_end)
    clip0, clip1, clip2, clip3 = [functools.partial(clip_factors, c) for c in range(n_chunk)]
    uA0c0, uA0c1, uA0c2, uA0c3, uA1c0, uA1c1, uA1c2, uA1c3, uA2c0, uA2c1, uA2c2, uA2c3 = units(0)
    stA0, stA1, stA2 = ring(ring_start, 0, 0)
    rlA0, rlA1, rlA2 = ring(ring_relay, 0, 0)
    enA0, enA1, enA2 = ring(ring_turn, 0)
    r2A0, r2A1, r2A2 = ring(ring_relay, 0, 1)
    e2A0, e2A1, e2A2 = ring(ring_last, 0)
    uB0c0, uB0c1, uB0c2, uB0c3, uB1c0, uB1c1, uB1c2, uB1c3, uB2c0, uB2c1, uB2c2, uB2c3 = units(1)
    stB0, stB1, stB2 = ring(ring_start, 1, 0)
    rlB0, rlB1, rlB2 = ring(ring_relay, 1, 0)
    enB0, enB1, enB2 = ring(ring_turn, 1)
    r2B0, r2B1, r2B2 = ring(ring_relay, 1, 1)
    e2B0, e2B1, e2B2 = ring(ring_last, 1)

    nrm[...] = jnp.zeros_like(nrm)
    dh0()
    back0()
    dh1()
    pair0()
    sd0()
    back1()
    dh2()
    pair1()
    sd1()
    back2()
    norm0()
    relay0()
    pair2()
    dh3()
    sd2()
    back3()
    relay1()
    norm1()
    own0()
    pair3()
    own1()
    gr0()
    relay2()
    sd3()
    relay3()
    norm2()
    norm3()
    cross0()
    gr1()
    own2()
    end0()
    dh4()
    back4()
    own3()
    cross1()
    pair4()
    end1()
    sd4()
    dh5()
    back5()
    gr2()
    pair5()
    relay4()
    sd5()
    gr3()
    norm4()
    cross2()
    norm5()
    end2()
    relay5()
    dh6()
    own4()
    back6()
    norm6()
    pair6()
    sd6()
    cross3()
    own5()
    end3()
    dh7()
    gr4()
    back7()
    norm7()
    pair7()
    relay6()
    gr5()
    cross4()
    sd7()
    relay7()
    end4()
    dh8()
    own6()
    back8()
    norm8()
    cross5()
    own7()
    end5()
    dh9()
    back9()
    gr6()
    norm9()
    pair9()
    clip0()
    uB0c0()
    gr7()
    sd9()
    uB2c0()
    pair8()
    cross6()
    sd8()
    clip1()
    uB0c1()
    end6()
    dh10()
    cross7()
    norm10()
    end7()
    dh11()
    norm11()
    uA0c0()
    relay8()
    relay9()
    clip2()
    uA0c1()
    uA0c2()
    uB0c2()
    clip3()
    uB0c3()
    stB0()
    uA0c3()
    stA0()
    uB2c1()
    uA1c0()
    uB2c2()
    own9()
    uB2c3()
    stB2()
    uA1c1()
    uA1c2()
    uA1c3()
    stA1()
    back11()
    own8()
    uB1c0()
    back10()
    uB1c1()
    pair11()
    uB1c2()
    sd11()
    uB1c3()
    stB1()
    rlA0()
    pair10()
    uA2c0()
    uA2c1()
    uA2c2()
    sd10()
    uA2c3()
    stA2()
    rlA1()
    relay11()
    rlB0()
    rlB2()
    gr9()
    rlB1()
    relay10()
    gr8()
    rlA2()
    own11()
    own10()
    enB0()
    enB2()
    enA0()
    cross8()
    enA1()
    enB1()
    gr11()
    enA2()
    r2A0()
    r2B0()
    gr10()
    cross9()
    r2B2()
    end8()
    r2A1()
    r2B1()
    r2A2()
    e2A0()
    cross11()
    e2B0()
    cross10()
    end9()
    e2A1()
    end10()
    end11()
    e2B2()
    e2B1()
    e2A2()
    ring_sent()


def hand_on(gu_in, gd_in, din_in, gu_out, gd_out, din_out, sem):
    copies = [pltpu.make_async_copy(src, dst, sem.at[i])
              for i, (src, dst) in enumerate(((din_in, din_out), (gu_in, gu_out), (gd_in, gd_out)))]
    for cp in copies:
        cp.start()
    for cp in copies:
        cp.wait()


def solution(mesh):
    n_dp, n_tp = mesh.shape["dp"], mesh.shape["tp"]

    def local(x_in, u_pre, w_up, w_down, d_out, noise_up, noise_down, clip_norm, noise_mult):
        n_layers, micro, batch, seq, dim = x_in.shape
        hid = u_pre.shape[-1]
        n_ex = micro * batch
        rows = n_ex * seq // N_CHUNK
        piece, grad_rows = rows // 16, dim // n_dp
        x4 = x_in.reshape(n_layers, N_CHUNK, rows, dim)
        u4 = u_pre.reshape(n_layers, N_CHUNK, rows, hid)
        d4 = d_out.reshape(N_CHUNK, rows, dim)
        anyspace = pl.BlockSpec(memory_space=pl.ANY)
        vmem = pl.BlockSpec(memory_space=pltpu.VMEM)
        dma = pltpu.SemaphoreType.DMA
        tokens = n_ex * seq
        flops = 2 * n_layers * tokens * hid * dim * 4 + 4 * n_layers * tokens * seq * (hid + dim)
        g_up, g_down, d_in = pl.pallas_call(
            step_kernel,
            out_shape=(
                pltpu.VMEM((n_layers, grad_rows, hid), F32),
                pltpu.VMEM((n_layers, grad_rows, hid), F32),
                pltpu.VMEM((N_CHUNK, rows, dim), BF16),
            ),
            in_specs=[anyspace] * 7 + [pl.BlockSpec(memory_space=pltpu.HBM)] * 2,
            out_specs=(vmem, vmem, vmem),
            scratch_shapes=[
                pltpu.VMEM((n_layers, N_CHUNK, rows, hid), BF16),
                pltpu.VMEM((n_layers, N_CHUNK, rows, hid), BF16),
                pltpu.VMEM((n_layers, N_CHUNK, rows, dim), BF16),
                pltpu.VMEM((n_layers, dim, hid), BF16),
                pltpu.VMEM((n_layers, hid, dim), BF16),
                pltpu.VMEM((2, rows, dim), BF16),
                pltpu.VMEM((rows, hid), F32),
                pltpu.VMEM((N_CHUNK, rows, dim), BF16),
                pltpu.VMEM((N_CHUNK, rows // 2, dim), BF16),
                pltpu.VMEM((N_CHUNK, 2, piece, dim), BF16),
                pltpu.VMEM((N_CHUNK, 2, piece, dim), BF16),
                pltpu.VMEM((N_CHUNK, 2, piece, dim), BF16),
                pltpu.VMEM((2 * n_layers, RING, RING, grad_rows, hid), F32),
                pltpu.VMEM((2 * n_layers, 6, RING // 2, grad_rows, hid), F32),
                pltpu.VMEM((2 * n_layers, 6, grad_rows // 2, hid), F32),
                pltpu.VMEM((n_ex, 8, seq), F32),
                pltpu.VMEM((N_CHUNK, 8, 128), F32),
                pltpu.VMEM((N_CHUNK, 2 * RING - 1, 8, 128), F32),
                pltpu.VMEM((n_ex, 8, 128), F32),
                pltpu.VMEM((2, n_layers, grad_rows, hid), F32),
                pltpu.SMEM((1,), F32),
                pltpu.SMEM((1,), F32),
                dma((2, N_CHUNK)),
                dma((len(GROUP_PIECES), N_CHUNK)),
                dma((2,)),
                dma((2, 2, 2 * n_layers)),
                dma((N_CHUNK,)),
                dma((N_CHUNK,)),
                dma((n_layers, N_CHUNK)),
                dma((2, n_layers)),
                dma((N_CHUNK,)),
                dma((2,)),
                dma((4,)),
            ],
            compiler_params=pltpu.CompilerParams(
                collective_id=0, has_side_effects=True, vmem_limit_bytes=61_700_000
            ),
            cost_estimate=pl.CostEstimate(flops=flops, bytes_accessed=50_000_000, transcendentals=n_layers * tokens * hid),
            name="clipped_step",
        )(x4, u4, w_up, w_down, d4, noise_up, jnp.transpose(noise_down, (0, 2, 1)), clip_norm, noise_mult)
        results = (g_up, g_down, d_in)
        g_up, g_down, d_in = pl.pallas_call(
            hand_on,
            out_shape=[jax.ShapeDtypeStruct(v.shape, v.dtype) for v in results],
            in_specs=[vmem] * 3,
            out_specs=[pl.BlockSpec(memory_space=pltpu.HBM)] * 3,
            scratch_shapes=[dma((3,))],
            compiler_params=pltpu.CompilerParams(vmem_limit_bytes=1_000_000),
            name="hand_on",
        )(*[pltpu.with_memory_space_constraint(v, pltpu.VMEM) for v in results])
        return g_up, jnp.transpose(g_down, (0, 2, 1)), d_in.reshape(d_out.shape)

    in_specs = (P(None, None, "dp", None, None), P(None, None, "dp", None, "tp"), P(None, None, "tp"),
                P(None, "tp", None), P(None, "dp", None, None), P(None, "dp", "tp"), P(None, "tp", "dp"), P(), P())
    out_specs = (P(None, "dp", "tp"), P(None, "tp", "dp"), P(None, "dp", None, None))
    return jax.shard_map(local, mesh=mesh, in_specs=in_specs, out_specs=out_specs, check_vma=False)
```
